32 devices in a mesh: section: 2 (over core), seq: 4 (over z), head: 4 (over y, x).
Axes of the slice: x: 2, y: 2, z: 4, core: 2. Of those that a mesh axis runs over, the one named last changes fastest.
Arguments:
- inputs: bfloat16 [2, 1024, 1536], P(None, 'seq'), may hold values from -6 to 6
- segments: int32 [2, 1024], P(None, 'seq'), may hold values from 0 to 31, never falling along the last dimension, each value on 1 to 768 neighbouring positions
- norms: float32 [2, 2, 1536], P('section'), may hold values from 0.25 to 1.75
- rec_in: bfloat16 [1536, 2, 2048], P(None, None, 'head'), may hold values from -0.15625 to 0.15625
- rec_gates: bfloat16 [16, 128, 2, 128], P('head'), may hold values from -0.5 to 0.5
- rec_chan: float32 [8, 2048], P(None, 'head'), may hold values from -20 to 4
- rec_out: bfloat16 [2048, 1536], P('head'), may hold values from -0.125 to 0.125
- attn_q: bfloat16 [1536, 1536], P(None, 'head'), may hold values from -0.15625 to 0.15625
- attn_kv: bfloat16 [1536, 256], replicated, may hold values from -0.15625 to 0.15625
- attn_out: bfloat16 [1536, 1536], P('head'), may hold values from -0.4375 to 0.4375
- mlp_in: bfloat16 [2, 1536, 2, 4608], P('section', None, None, 'head'), may hold values from -0.15625 to 0.15625
- mlp_out: bfloat16 [2, 4608, 1536], P('section', 'head'), may hold values from -0.09375 to 0.09375
- cotangent: bfloat16 [2, 1024, 1536], P(None, 'seq'), may hold values from -6 to 6
Outputs:
- final_out: bfloat16 [2, 1024, 1536], P('section', 'seq')
- grad_inputs: float32 [2, 1024, 1536], P('section', 'seq')
- grad_norms: float32 [2, 2, 1536], P('section', None, 'seq')
- grad_rec_in: float32 [1536, 2, 2048], P(('section', 'seq'), None, 'head')
- grad_rec_gates: float32 [16, 128, 2, 128], P('head', ('section', 'seq'))
- grad_rec_chan: float32 [8, 2048], P('section', 'head')
- grad_rec_out: float32 [2048, 1536], P('head', ('section', 'seq'))
- grad_attn_q: float32 [1536, 1536], P(('section', 'seq'), 'head')
- grad_attn_kv: float32 [1536, 256], P(('section', 'seq'))
- grad_attn_out: float32 [1536, 1536], P('head', ('section', 'seq'))
- grad_mlp_in: float32 [2, 1536, 2, 4608], P('section', 'seq', None, 'head')
- grad_mlp_out: float32 [2, 4608, 1536], P('section', 'head', 'seq')
The draws below stay inside these ranges and needn't reach their ends.
Inputs may be any that keep to these rules, and one draw needn't show every extreme that they name: `segments`: along each stream segment numbers never fall and rise by one at each new document; a document holds 1 to 768 tokens, and one in every stream holds exactly 768.
All inputs are finite; a program needn't handle non-finite values.
Results may differ from the reference program's by a relative error of at most 0.03.
Values may be sent and summed in bfloat16 or wider, within the bound.
A program may use at most 320 MiB of HBM per device.

```python
import math
import jax
import jax.numpy as jnp
import numpy as np
from jax import lax

D = 1536
R = 2048
FF = 4608
HQ = 12
HEAD = 128
WINDOW = 1024
BLOCK = 128
MB = 2
TOKENS_MB = 1024
SEG_COUNT = 32
DOC_MAX = 768


def draw_rec_chan(key, part):
    streams = jax.random.split(key, 6)
    taps = 0.5 * jnp.clip(jax.random.normal(streams[0], (4, R), jnp.float32), -4.0, 4.0)
    conv_bias = 0.3 * jnp.clip(jax.random.normal(streams[1], (1, R), jnp.float32), -4.0, 4.0)
    gate_bias = jnp.clip(jax.random.normal(streams[2], (2, R), jnp.float32), -4.0, 4.0)
    chain = 1.0 * TOKENS_MB
    slow_rates = jnp.exp(jax.random.uniform(streams[3], (1, R), jnp.float32, jnp.log(0.05 / chain), jnp.log(0.5 / chain)))
    fast_rates = jnp.exp(jax.random.uniform(streams[4], (1, R), jnp.float32, jnp.log(0.5 / chain), jnp.log(0.03)))
    share = 0.5
    chosen = jax.random.uniform(streams[5], (1, R), jnp.float32) < share
    rates = jnp.where(chosen, slow_rates, fast_rates)
    lam_row = jnp.log(jnp.expm1(rates))
    return jnp.concatenate([taps, conv_bias, gate_bias, lam_row], axis=0)


def level_of(rng, dims, pieces, low, top_value):
    def one(dim, shards_of):
        draws = jax.random.uniform(jax.random.fold_in(jax.random.fold_in(rng, 6), dim), (shards_of,), jnp.float32, low / len(pieces), top_value / len(pieces))
        return jnp.repeat(jnp.exp(draws), dims[dim] // shards_of).reshape((-1,) + (1,) * (len(dims) - dim - 1))

    gain = one(*pieces[0])
    for cut in pieces[1:]:
        gain = gain * one(*cut)
    return gain


def profile(count, total, bound, slope):
    loads = [(1 << 20) // math.isqrt(grade ** slope) + 1 for grade in range(2, count + 1)]
    spare, counts = total - bound - (count - 1), [1] * (count - 1)
    while spare > 0:
        free = [i for i in range(count - 1) if counts[i] < bound]
        pool, left = sum([loads[i] for i in free]), spare
        for i in free:
            more = min(bound - counts[i], max(1, left * loads[i] // pool), spare)
            counts[i] = counts[i] + more
            spare = spare - more
    return np.array([bound] + counts)


def ragged_sizes(stream_key, number_of, total, most, slope):
    if number_of == 2:
        one = jax.random.randint(stream_key, (), max(1, total - most), min(most, total - 1) + 1)
        return jnp.stack([one, total - one])
    tallies = jnp.asarray(profile(number_of, total, most, slope), jnp.int32)
    pairs = (number_of - 1) // 2
    donor, sink = tallies[1:1 + 2 * pairs:2], tallies[2:2 + 2 * pairs:2]
    margin = jnp.minimum(donor - 1, most - sink)
    shifted = jax.random.randint(jax.random.fold_in(stream_key, 1), (pairs,), 0, 1 << 20) % (margin + 1)
    tallies = tallies.at[1:1 + 2 * pairs:2].set(donor - shifted).at[2:2 + 2 * pairs:2].set(sink + shifted)
    return tallies[jax.random.permutation(jax.random.fold_in(stream_key, 2), number_of)]


def centred(rng, extent, spread, bound, cuts=(), kind=jnp.bfloat16):
    level = level_of(rng, extent, cuts, -0.22, 0.18) if cuts else 1.0
    drawn = jax.random.normal(rng, extent, jnp.float32) * spread * level
    return jnp.minimum(jnp.maximum(drawn, -bound), bound).astype(kind)


def setup_inputs(seed: int = 0) -> dict:
    keys = jax.random.split(jax.random.key(seed), 14)
    inputs = centred(keys[0], (MB, TOKENS_MB, D), 1.0, 6.0, ((1, 4),))
    segments = jax.vmap(lambda own: jnp.searchsorted(jnp.cumsum(ragged_sizes(own, SEG_COUNT, TOKENS_MB, DOC_MAX, 2)), jnp.arange(TOKENS_MB), side="right"))(jax.random.split(keys[1], MB)).reshape((MB, TOKENS_MB)).astype(jnp.int32)
    norms = jnp.clip(1.0 + 0.15 * jax.random.normal(keys[2], (2, 2, D), jnp.float32), 0.25, 1.75)
    rec_in = centred(keys[3], (D, 2, R), D ** -0.5, 0.15625, ((2, 4),))
    rec_gates = centred(keys[4], (R // BLOCK, BLOCK, 2, BLOCK), BLOCK ** -0.5, 0.5, ((0, 4),))
    rec_chan = draw_rec_chan(jax.random.fold_in(keys[13], 71), 0)
    rec_out = centred(keys[6], (R, D), R ** -0.5, 0.125, ((0, 4),))
    attn_q = centred(keys[7], (D, HQ * HEAD), D ** -0.5, 0.15625, ((1, 4),))
    attn_kv = centred(keys[8], (D, 2 * HEAD), D ** -0.5, 0.15625)
    attn_out = centred(keys[9], (HQ * HEAD, D), (HQ * HEAD // 8) ** -0.5, 0.4375, ((0, 4),))
    mlp_in = centred(keys[10], (2, D, 2, FF), D ** -0.5, 0.15625, ((0, 2), (3, 4)))
    mlp_out = centred(keys[11], (2, FF, D), FF ** -0.5, 0.09375, ((0, 2), (1, 4)))
    cotangent = centred(keys[12], (MB, TOKENS_MB, D), 1.0, 6.0, ((1, 4),))
    return {"inputs": inputs, "segments": segments, "norms": norms, "rec_in": rec_in, "rec_gates": rec_gates, "rec_chan": rec_chan, "rec_out": rec_out, "attn_q": attn_q, "attn_kv": attn_kv, "attn_out": attn_out, "mlp_in": mlp_in, "mlp_out": mlp_out, "cotangent": cotangent}


@jax.custom_vjp
def low(v):
    return lax.optimization_barrier(v.astype(jnp.bfloat16)).astype(jnp.float32)

@jax.custom_vjp
def low_back(v):
    return v

def low_keep(v):
    return (low(v), None)

def low_pass(kept, grad):
    return (grad,)

def back_keep(v):
    return (v, None)

def back_low(kept, grad):
    return (low(grad),)
low.defvjp(low_keep, low_pass)
low_back.defvjp(back_keep, back_low)
epsilon = 1e-06
highest = lax.Precision.HIGHEST

def root_norm(tensor, scale_gain):
    return tensor * lax.rsqrt(lax.optimization_barrier(jnp.mean(tensor * tensor, axis=-1, keepdims=True)) + epsilon) * scale_gain

def lagged(tensor, offset):
    return jnp.concatenate([jnp.zeros((offset,) + tensor.shape[1:], tensor.dtype), tensor[:-offset]], axis=0)

def same_doc(doc_ids, offset):
    before = jnp.concatenate([jnp.full((offset,), -1, jnp.int32), doc_ids[:-offset]])
    return (before == doc_ids).astype(jnp.float32)[:, None]

def gate_math(pre_rate, pre_input, conv_in, lam_param):
    log_decay = -8.0 * jax.nn.sigmoid(pre_rate) * jax.nn.softplus(lam_param)
    decays = jnp.exp(log_decay)
    drive = jnp.sqrt(-jnp.expm1(2.0 * log_decay)) * jax.nn.sigmoid(pre_input) * conv_in
    return (decays, drive)

def feed_forward(residual, scale_gain, w_in, w_out):
    normed = low(root_norm(residual, scale_gain))
    gate_up = low_back(jnp.einsum('td,dkf->tkf', normed, w_in, precision=highest))
    hidden = low(jax.nn.gelu(gate_up[:, 0]) * gate_up[:, 1])
    return residual + low_back(jnp.dot(hidden, w_out, precision=highest))

def recurrent_layer(stream, doc_ids, gains_pair, rec_in, rec_gates, rec_chan, rec_out, w_in, w_out):
    length = stream.shape[0]
    normed = low(root_norm(stream, gains_pair[0]))
    branches = low_back(jnp.einsum('td,dkr->tkr', normed, rec_in, precision=highest))
    values = low(branches[:, 0])
    gate_act = jax.nn.gelu(branches[:, 1])
    conv_out = rec_chan[4] + rec_chan[0] * values
    for offset in range(1, 4):
        conv_out = conv_out + rec_chan[offset] * lagged(values, offset) * same_doc(doc_ids, offset)
    conv_out = low(conv_out)
    blocks = conv_out.reshape(length, R // BLOCK, BLOCK)
    pre_gates = low_back(jnp.einsum('tnb,nbkc->tknc', blocks, rec_gates, precision=highest)).reshape(length, 2, R)
    decays, drive = gate_math(pre_gates[:, 0] + rec_chan[5], pre_gates[:, 1] + rec_chan[6], conv_out, rec_chan[7])
    decays = decays * same_doc(doc_ids, 1)

    def advance(carry_state, step_pair):
        carry_state = step_pair[0] * carry_state + step_pair[1]
        return (carry_state, carry_state)
    _, hidden = lax.scan(advance, jnp.zeros((R,), jnp.float32), (decays, drive))
    mixed_out = low(hidden * gate_act)
    residual = stream + low_back(jnp.dot(mixed_out, rec_out, precision=highest))
    return feed_forward(residual, gains_pair[1], w_in, w_out)

def attention_layer(stream, doc_ids, gains_pair, attn_q, attn_kv, attn_out, w_in, w_out):
    length = stream.shape[0]
    normed = low(root_norm(stream, gains_pair[0]))
    queries = low(low_back(jnp.dot(normed, attn_q, precision=highest))).reshape(length, HQ, HEAD)
    keyval = low(low_back(jnp.dot(normed, attn_kv, precision=highest)))
    block_rows = min(512, length)
    padded = jnp.concatenate([jnp.zeros((WINDOW, 2 * HEAD), jnp.float32), keyval], axis=0)
    seg_pad = jnp.concatenate([jnp.full((WINDOW,), -1, jnp.int32), doc_ids])
    key_spots = jnp.arange(block_rows + WINDOW, dtype=jnp.int32)

    def attend(start_row):
        query_rows = lax.dynamic_slice_in_dim(queries, start_row, block_rows, 0)
        near_kv = lax.dynamic_slice_in_dim(padded, start_row, block_rows + WINDOW, 0)
        near_seg = lax.dynamic_slice_in_dim(seg_pad, start_row, block_rows + WINDOW, 0)
        own_seg = lax.dynamic_slice_in_dim(doc_ids, start_row, block_rows, 0)
        distance = jnp.arange(block_rows, dtype=jnp.int32)[:, None] + WINDOW - key_spots[None, :]
        allowed = (distance >= 0) & (distance < WINDOW) & (own_seg[:, None] == near_seg[None, :])
        scores = low_back(jnp.einsum('qhd,kd->hqk', query_rows, near_kv[:, :HEAD], precision=highest) * HEAD ** (-0.5))
        weights = low(jax.nn.softmax(jnp.where(allowed[None], scores, -1e+30), axis=-1))
        return low(low_back(jnp.einsum('hqk,kd->qhd', weights, near_kv[:, HEAD:], precision=highest)))
    starts = jnp.arange(0, length, block_rows, dtype=jnp.int32)
    attended = lax.map(jax.checkpoint(attend), starts).reshape(length, HQ * HEAD)
    residual = stream + low_back(jnp.dot(attended, attn_out, precision=highest))
    return feed_forward(residual, gains_pair[1], w_in, w_out)

def forward(stream, doc_ids, norms, rec_in, rec_gates, rec_chan, rec_out, attn_q, attn_kv, attn_out, mlp_in, mlp_out):
    first_out = recurrent_layer(stream, doc_ids, norms[0], rec_in, rec_gates, rec_chan, rec_out, mlp_in[0], mlp_out[0])
    passed = low_back(low(first_out))
    return attention_layer(passed, doc_ids, norms[1], attn_q, attn_kv, attn_out, mlp_in[1], mlp_out[1])

def reference(inputs, segments, norms, rec_in, rec_gates, rec_chan, rec_out, attn_q, attn_kv, attn_out, mlp_in, mlp_out, cotangent):
    parameters = tuple((weight.astype(jnp.float32) for weight in (norms, rec_in, rec_gates, rec_chan, rec_out, attn_q, attn_kv, attn_out, mlp_in, mlp_out)))
    outputs, input_grads, totals = ([], [], None)
    for micro_index in range(MB):
        doc_ids = segments[micro_index]

        def run_layers(stream, *weights):
            return forward(stream, doc_ids, *weights)
        result, pull_back = jax.vjp(run_layers, inputs[micro_index].astype(jnp.float32), *parameters)
        gradients = pull_back(cotangent[micro_index].astype(jnp.float32))
        outputs.append(result.astype(jnp.bfloat16))
        input_grads.append(gradients[0])
        if totals is None:
            totals = gradients[1:]
        else:
            totals = tuple((first_sum + second_sum for first_sum, second_sum in zip(totals, gradients[1:])))
    grad_norms, grad_rec_in, grad_rec_gates, grad_rec_chan, grad_rec_out, grad_attn_q, grad_attn_kv, grad_attn_out, grad_mlp_in, grad_mlp_out = totals
    return (jnp.stack(outputs), jnp.stack(input_grads), grad_norms, grad_rec_in, grad_rec_gates, grad_rec_chan, grad_rec_out, grad_attn_q, grad_attn_kv, grad_attn_out, grad_mlp_in, grad_mlp_out)
```

```python
import functools

import jax
import jax.numpy as jnp
from jax import lax
from jax.experimental import pallas as pl
from jax.experimental.pallas import tpu as pltpu
from jax.sharding import PartitionSpec as P

WINDOW = 1024
EPSILON = 1e-06
MESH = pl.DeviceIdType.MESH
F32 = jnp.float32
BF16 = jnp.bfloat16
SWAP = [(0, 1), (1, 0)]


def dot(a, b, dims, out=F32):
    return lax.dot_general(a, b, ((dims[:1], dims[1:]), ((), ())), preferred_element_type=F32).astype(
        out
    )


def vmem():
    return pl.BlockSpec(memory_space=pltpu.VMEM)


def meet(axis, me, n):
    barrier = pltpu.get_barrier_semaphore()
    for k in range(1, n):
        peer = lax.rem(me + k, n)
        pl.semaphore_signal(barrier, inc=1, device_id={axis: peer}, device_id_type=MESH)
    pl.semaphore_wait(barrier, n - 1)


def remote(src, dst, send, recv, axis, peer):
    return pltpu.make_async_remote_copy(
        src_ref=src,
        dst_ref=dst,
        send_sem=send,
        recv_sem=recv,
        device_id={axis: peer},
        device_id_type=MESH,
    )


def scatter_sum(n, me, rows, part, recv, send_sem, recv_sem):
    copies = []
    for k in range(1, n):
        peer = lax.rem(me + k, n)
        start = pl.multiple_of(peer * rows, rows)
        copies.append(
            remote(
                part.at[pl.ds(start, rows)],
                recv.at[k - 1],
                send_sem.at[k - 1],
                recv_sem.at[k - 1],
                "head",
                peer,
            )
        )
    for copy in copies:
        copy.start()
    total = part[pl.ds(pl.multiple_of(me * rows, rows), rows)].astype(F32)
    for k, copy in enumerate(copies):
        copy.wait_recv()
        total = total + recv[k].astype(F32)
    for copy in copies:
        copy.wait_send()
    return total


def spread(n, me, rows, value, full, send_sem, recv_sem):
    mine = pl.ds(pl.multiple_of(me * rows, rows), rows)
    full[mine] = value
    copies = []
    for k in range(1, n):
        peer = lax.rem(me + k, n)
        copies.append(
            remote(
                full.at[mine], full.at[mine], send_sem.at[k - 1], recv_sem.at[k - 1], "head", peer
            )
        )
    for copy in copies:
        copy.start()
    for copy in copies:
        copy.wait()


def forward_body(n, kind, part, base, gain, new, full, recv, s1, r1, s2, r2):
    me = lax.axis_index("head")
    rows = base.shape[0]
    meet("head", me, n)
    fresh = base[...] + scatter_sum(n, me, rows, part, recv, s1, r1)
    if kind == "last":
        new[...] = fresh
        out = fresh
    else:
        if kind == "round":
            fresh = fresh.astype(BF16).astype(F32)
        new[...] = fresh
        out = fresh * lax.rsqrt(jnp.mean(fresh * fresh, axis=-1, keepdims=True) + EPSILON)
        out = out * gain[...]
    spread(n, me, rows, out.astype(BF16), full, s2, r2)


def backward_body(n, kind, part, base, gain, up, res, gain_grad, full, recv, s1, r1, s2, r2):
    me = lax.axis_index("head")
    rows = base.shape[0]
    meet("head", me, n)
    grad = scatter_sum(n, me, rows, part, recv, s1, r1)
    v = base[...]
    scale = lax.rsqrt(jnp.mean(v * v, axis=-1, keepdims=True) + EPSILON)
    gain_grad[...] = jnp.sum(grad * v * scale, axis=0, keepdims=True)
    inner = grad * gain[...]
    out = up[...] + scale * inner - v * (
        scale * scale * scale * jnp.mean(inner * v, axis=-1, keepdims=True)
    )
    if kind == "round":
        out = out.astype(BF16).astype(F32)
    res[...] = out
    spread(n, me, rows, out.astype(BF16), full, s2, r2)


def boundary_scratch(n, rows, width):
    return [pltpu.VMEM((n - 1, rows, width), BF16)] + [pltpu.SemaphoreType.DMA((n - 1,))] * 4


def join_forward(kind, part, base, gain, ident):
    n = lax.axis_size("head")
    count, width = part.shape
    rows = base.shape[0]
    return pl.pallas_call(
        functools.partial(forward_body, n, kind),
        name=f"join_forward_{ident}",
        out_shape=(
            jax.ShapeDtypeStruct((rows, width), F32),
            jax.ShapeDtypeStruct((count, width), BF16),
        ),
        in_specs=[vmem()] * 3,
        out_specs=(vmem(), vmem()),
        scratch_shapes=boundary_scratch(n, rows, width),
        compiler_params=pltpu.CompilerParams(collective_id=ident, has_side_effects=True),
    )(part, base, gain)


def join_backward(kind, part, base, gain, up, ident):
    n = lax.axis_size("head")
    count, width = part.shape
    rows = base.shape[0]
    return pl.pallas_call(
        functools.partial(backward_body, n, kind),
        name=f"join_backward_{ident}",
        out_shape=(
            jax.ShapeDtypeStruct((rows, width), F32),
            jax.ShapeDtypeStruct((1, width), F32),
            jax.ShapeDtypeStruct((count, width), BF16),
        ),
        in_specs=[vmem()] * 4,
        out_specs=(vmem(), vmem(), vmem()),
        scratch_shapes=boundary_scratch(n, rows, width),
        compiler_params=pltpu.CompilerParams(collective_id=ident, has_side_effects=True),
    )(part, base, gain, up)


def carry_body(n, reverse, edge, out, every, send_sem, recv_sem):
    me = lax.axis_index("seq")
    meet("seq", me, n)
    copies = []
    for k in range(1, n):
        peer = lax.rem(me + k, n)
        copies.append(
            remote(edge, every.at[k - 1], send_sem.at[k - 1], recv_sem.at[k - 1], "seq", peer)
        )
    for copy in copies:
        copy.start()
    for copy in copies:
        copy.wait()
    state = jnp.zeros((1, edge.shape[1]), F32)
    order = range(1, n) if reverse else range(n - 1, 0, -1)
    for k in order:
        sender = me - k if not reverse else me + n - k
        inside = sender >= 0 if not reverse else sender < n
        if reverse:
            inside = jnp.logical_and(inside, sender > me)
        slot = every[k - 1]
        state = jnp.where(inside, slot[0:1] * state + slot[1:2], state)
    out[...] = jnp.broadcast_to(state, out.shape)


def carry(edge, reverse, ident):
    n = lax.axis_size("seq")
    return pl.pallas_call(
        functools.partial(carry_body, n, reverse),
        name=f"carry_{ident}",
        out_shape=jax.ShapeDtypeStruct(edge.shape, F32),
        in_specs=[vmem()],
        out_specs=vmem(),
        scratch_shapes=[
            pltpu.VMEM((n - 1,) + edge.shape, F32),
            pltpu.SemaphoreType.DMA((n - 1,)),
            pltpu.SemaphoreType.DMA((n - 1,)),
        ],
        compiler_params=pltpu.CompilerParams(collective_id=ident, has_side_effects=True),
    )(edge)


def shifted(x, by, row, fill):
    count = x.shape[0]
    if by > 0:
        return jnp.where(row >= by, pltpu.roll(x, by, 0), fill)
    return jnp.where(row < count + by, pltpu.roll(x, count + by, 0), fill)


def scan_rows(a, b, row, sign):
    step = 1
    while step < a.shape[0]:
        b = b + a * shifted(b, sign * step, row, 0.0)
        a = a * shifted(a, sign * step, row, 1.0)
        step *= 2
    return a, b


def minus_expm1(y):
    series = jnp.full_like(y, 1.0)
    for k in range(9, 1, -1):
        series = 1.0 + y * series * (1.0 / k)
    return jnp.where(y > -0.5, -y * series, 1.0 - jnp.exp(y))


def gelu_parts(x):
    c = 0.7978845608028654
    inner = c * (x + 0.044715 * x * x * x)
    t = jnp.tanh(inner)
    act = 0.5 * x * (1.0 + t)
    slope = 0.5 * (1.0 + t) + 0.5 * x * (1.0 - t * t) * c * (1.0 + 3.0 * 0.044715 * x * x)
    return act, slope


def rec_forward_body(ext, masks, chan, soft, gates, conv_out, pre_out, through, local, edge):
    count = conv_out.shape[0]
    block = conv_out.shape[1]
    wide = ext[...].astype(F32)
    total = chan[4:5] + chan[0:1] * wide[8:]
    for k in range(1, 4):
        total = total + chan[k : k + 1] * pltpu.roll(wide, k, 0)[8:] * masks[:, k : k + 1]
    low = total.astype(BF16)
    conv_out[...] = low
    pre = jnp.dot(low, gates[0], preferred_element_type=F32)
    rate = pre[:, :block] + chan[5:6]
    gate = pre[:, block:] + chan[6:7]
    pre_out[0] = rate
    pre_out[1] = gate
    log_decay = -8.0 * jax.nn.sigmoid(rate) * soft[0:1]
    decay = jnp.exp(log_decay) * masks[:, 1:2]
    drive = jnp.sqrt(minus_expm1(2.0 * log_decay)) * jax.nn.sigmoid(gate) * low.astype(F32)
    row = lax.broadcasted_iota(jnp.int32, (count, block), 0)
    a, b = scan_rows(decay, drive, row, 1)
    through[...] = a
    local[...] = b
    edge[0:1] = a[count - 1 :]
    edge[1:2] = b[count - 1 :]
    edge[2:8] = jnp.zeros((6, block), F32)


def rec_forward_local(ext, masks, chan, soft, gates):
    count, chans = ext.shape[0] - 8, ext.shape[1]
    blocks, block = gates.shape[:2]
    wide = pl.BlockSpec((count, block), lambda i: (0, i))
    row8 = pl.BlockSpec((8, block), lambda i: (0, i))
    return pl.pallas_call(
        rec_forward_body,
        name="rec_forward_local",
        grid=(blocks,),
        out_shape=(
            jax.ShapeDtypeStruct((count, chans), BF16),
            jax.ShapeDtypeStruct((2, count, chans), F32),
            jax.ShapeDtypeStruct((count, chans), F32),
            jax.ShapeDtypeStruct((count, chans), F32),
            jax.ShapeDtypeStruct((8, chans), F32),
        ),
        in_specs=[
            pl.BlockSpec((count + 8, block), lambda i: (0, i)),
            pl.BlockSpec((count, 4), lambda i: (0, 0)),
            row8,
            row8,
            pl.BlockSpec((1, block, 2 * block), lambda i: (i, 0, 0)),
        ],
        out_specs=(
            wide,
            pl.BlockSpec((2, count, block), lambda i: (0, 0, i)),
            wide,
            wide,
            row8,
        ),
    )(ext, masks, chan, soft, gates)


def rec_back_first_body(gm, gate_pre, hidden, rate, soft, masks, grad_gate, beyond, local, edge):
    count, block = gm.shape
    act, slope = gelu_parts(gate_pre[...])
    up = gm[...]
    grad_gate[...] = (up * hidden[...] * slope).astype(BF16)
    decay = jnp.exp(-8.0 * jax.nn.sigmoid(rate[0]) * soft[0:1]) * masks[:, 1:2]
    row = lax.broadcasted_iota(jnp.int32, (count, block), 0)
    a, b = scan_rows(shifted(decay, -1, row, 1.0), up * act, row, -1)
    beyond[...] = a
    local[...] = b
    edge[0:1] = decay[0:1] * a[0:1]
    edge[1:2] = decay[0:1] * b[0:1]
    edge[2:8] = jnp.zeros((6, block), F32)


def rec_back_first(gm, gate_pre, hidden, pre, soft, masks, block):
    count, chans = gm.shape
    wide = pl.BlockSpec((count, block), lambda i: (0, i))
    row8 = pl.BlockSpec((8, block), lambda i: (0, i))
    return pl.pallas_call(
        rec_back_first_body,
        name="rec_back_first",
        grid=(chans // block,),
        out_shape=(
            jax.ShapeDtypeStruct((count, chans), BF16),
            jax.ShapeDtypeStruct((count, chans), F32),
            jax.ShapeDtypeStruct((count, chans), F32),
            jax.ShapeDtypeStruct((8, chans), F32),
        ),
        in_specs=[
            wide,
            wide,
            wide,
            pl.BlockSpec((1, count, block), lambda i: (0, 0, i)),
            row8,
            pl.BlockSpec((count, 4), lambda i: (0, 0)),
        ],
        out_specs=(wide, wide, wide, row8),
    )(gm, gate_pre, hidden, pre, soft, masks)


def rec_back_second_body(
    beyond, local, arriving, hidden, entering, pre, conv, chan, soft, gates, masks, ext,
    gate_low, grad_values, edge, chan_grad,
):
    count, block = local.shape
    row = lax.broadcasted_iota(jnp.int32, (count, block), 0)
    state = local[...] + beyond[...] * arriving[0:1]
    earlier = jnp.where(row >= 1, pltpu.roll(hidden[...], 1, 0), entering[0:1])
    low = conv[...].astype(F32)
    keep_rate = jax.nn.sigmoid(pre[0])
    log_decay = -8.0 * keep_rate * soft[0:1]
    decay = jnp.exp(log_decay)
    size = jnp.sqrt(minus_expm1(2.0 * log_decay))
    gate = jax.nn.sigmoid(pre[1])
    grad_decay = state * earlier * masks[:, 1:2]
    grad_log = grad_decay * decay - state * gate * low * (decay * decay / size)
    grad_rate = grad_log * (-8.0 * soft[0:1]) * keep_rate * (1.0 - keep_rate)
    grad_gate = state * size * low * gate * (1.0 - gate)
    rate_low = grad_rate.astype(BF16)
    gate_low_part = grad_gate.astype(BF16)
    gate_low[0] = rate_low
    gate_low[1] = gate_low_part
    weights = gates[0]
    over = (((1,), (1,)), ((), ()))
    grad_conv = (
        state * size * gate
        + lax.dot_general(rate_low, weights[:, :block], over, preferred_element_type=F32)
        + lax.dot_general(gate_low_part, weights[:, block:], over, preferred_element_type=F32)
    )
    wide = ext[...].astype(F32)
    total = chan[0:1] * grad_conv
    chan_grad[0:1] = jnp.sum(grad_conv * wide[8:], axis=0, keepdims=True)
    row8 = lax.broadcasted_iota(jnp.int32, (8, block), 0)
    over_edge = jnp.zeros((8, block), F32)
    for k in range(1, 4):
        masked = grad_conv * masks[:, k : k + 1]
        chan_grad[k : k + 1] = jnp.sum(masked * pltpu.roll(wide, k, 0)[8:], axis=0, keepdims=True)
        back = chan[k : k + 1] * masked
        total = total + shifted(back, -k, row, 0.0)
        first = back[0:8]
        if k < 3:
            first = pltpu.roll(first, 3 - k, 0)
        over_edge = over_edge + jnp.where((row8 >= 3 - k) & (row8 < 3), first, 0.0)
    grad_values[...] = total
    edge[...] = over_edge
    chan_grad[4:5] = jnp.sum(grad_conv, axis=0, keepdims=True)
    chan_grad[5:6] = jnp.sum(grad_rate, axis=0, keepdims=True)
    chan_grad[6:7] = jnp.sum(grad_gate, axis=0, keepdims=True)
    chan_grad[7:8] = jnp.sum(grad_log * keep_rate, axis=0, keepdims=True) * (
        -8.0 * jax.nn.sigmoid(chan[7:8])
    )


def rec_back_second(beyond, local, arriving, hidden, entering, pre, conv, chan, soft, gates, masks, ext):
    count, chans = local.shape
    blocks, block = gates.shape[:2]
    wide = pl.BlockSpec((count, block), lambda i: (0, i))
    row8 = pl.BlockSpec((8, block), lambda i: (0, i))
    pair = pl.BlockSpec((2, count, block), lambda i: (0, 0, i))
    return pl.pallas_call(
        rec_back_second_body,
        name="rec_back_second",
        grid=(blocks,),
        out_shape=(
            jax.ShapeDtypeStruct((2, count, chans), BF16),
            jax.ShapeDtypeStruct((count, chans), F32),
            jax.ShapeDtypeStruct((8, chans), F32),
            jax.ShapeDtypeStruct((8, chans), F32),
        ),
        in_specs=[
            wide,
            wide,
            row8,
            wide,
            row8,
            pair,
            wide,
            row8,
            row8,
            pl.BlockSpec((1, block, 2 * block), lambda i: (i, 0, 0)),
            pl.BlockSpec((count, 4), lambda i: (0, 0)),
            pl.BlockSpec((count + 8, block), lambda i: (0, i)),
        ],
        out_specs=(pair, wide, row8, row8),
    )(beyond, local, arriving, hidden, entering, pre, conv, chan, soft, gates, masks, ext)


def from_behind(array, axis, by):
    devices = lax.axis_size(axis)
    pairs = [(i, i + by) for i in range(devices) if 0 <= i + by < devices]
    return lax.ppermute(array, axis, pairs)


def swapped(array):
    return lax.ppermute(array, "section", SWAP)


def attend(query_rows, key_rows, allowed):
    head_dim = query_rows.shape[2]
    scores = jnp.einsum(
        "qhd,kd->hqk", query_rows, key_rows[:, :head_dim], preferred_element_type=F32
    ) * head_dim ** (-0.5)
    masked = jnp.where(allowed[None], scores, -1e30)
    row_max = jnp.max(masked, axis=-1, keepdims=True)
    lifted = jnp.exp(masked - row_max)
    row_total = jnp.sum(lifted, axis=-1, keepdims=True)
    weights = (lifted / row_total).astype(BF16)
    attended = jnp.einsum(
        "hqk,kd->qhd", weights, key_rows[:, head_dim:], preferred_element_type=F32
    ).astype(BF16)
    return (attended, row_max[:, :, 0] + jnp.log(row_total[:, :, 0]))


def attend_back(query_rows, key_rows, allowed, log_total, grad_rows):
    head_dim = query_rows.shape[2]
    factor = head_dim ** (-0.5)
    scores = (
        jnp.einsum("qhd,kd->hqk", query_rows, key_rows[:, :head_dim], preferred_element_type=F32)
        * factor
    )
    probs = jnp.exp(jnp.where(allowed[None], scores, -1e30) - log_total[:, :, None])
    weights = probs.astype(BF16)
    grad_probs = jnp.einsum(
        "qhd,kd->hqk", grad_rows, key_rows[:, head_dim:], preferred_element_type=F32
    )
    grad_values = jnp.einsum("hqk,qhd->kd", weights, grad_rows, preferred_element_type=F32)
    grad_scores = (
        probs * (grad_probs - jnp.sum(grad_probs * probs, axis=-1, keepdims=True))
    ).astype(BF16)
    grad_query = (
        jnp.einsum("hqk,kd->qhd", grad_scores, key_rows[:, :head_dim], preferred_element_type=F32)
        * factor
    )
    grad_keys = (
        jnp.einsum("hqk,qhd->kd", grad_scores, query_rows, preferred_element_type=F32) * factor
    )
    return (grad_query, jnp.concatenate([grad_keys, grad_values], axis=-1))


def mlp_forward(normed, w_in, w_out):
    gate_up = jnp.einsum("td,dkf->tkf", normed, w_in, preferred_element_type=F32)
    hidden = (jax.nn.gelu(gate_up[:, 0]) * gate_up[:, 1]).astype(BF16)
    return gate_up, hidden, dot(hidden, w_out, (1, 0), BF16)


def mlp_backward(gate_up, w_in, w_out, out_low):
    grad_hidden = dot(out_low, w_out, (1, 1))
    act, slope = gelu_parts(gate_up[:, 0])
    grad_gate = (grad_hidden * gate_up[:, 1] * slope).astype(BF16)
    grad_up = (grad_hidden * act).astype(BF16)
    part = (
        dot(grad_gate, w_in[:, 0], (1, 1)) + dot(grad_up, w_in[:, 1], (1, 1))
    ).astype(BF16)
    return grad_gate, grad_up, part


def seq_scatter(grad):
    return lax.psum_scatter(grad, "seq", scatter_dimension=0, tiled=True)


def pair_grad(left, left_other, right, right_other):
    return (dot(left, right, (0, 0)) + dot(left_other, right_other, (0, 0))).astype(BF16)


def columns(array, start, size):
    return lax.dynamic_slice_in_dim(array, start, size, axis=1)


def on_device(
    inputs,
    segments,
    norms,
    rec_in,
    rec_gates,
    rec_chan,
    rec_out,
    attn_q,
    attn_kv,
    attn_out,
    mlp_in,
    mlp_out,
    cotangent,
):
    core = lax.axis_index("section")
    first = core == 0
    place = lax.axis_index("seq")
    rank = lax.axis_index("head")
    heads = lax.axis_size("head")
    blocks_seq = lax.axis_size("seq")
    _, count, width = inputs.shape
    rows = count // heads
    chans = rec_in.shape[2]
    blocks, block = rec_gates.shape[:2]
    half_width = width // 2

    def pick(array, index):
        return lax.dynamic_index_in_dim(array, index, 0, keepdims=False)

    def own_rows(array):
        return lax.dynamic_slice_in_dim(array, rank * rows, rows, axis=0)

    def mine_and_other(pair_zero, pair_one):
        return jnp.where(first, pair_zero, pair_one), swapped(jnp.where(first, pair_one, pair_zero))

    other_in, other_out, other_norms = swapped(mlp_in[0]), swapped(mlp_out[0]), swapped(norms[0])
    gains = [
        jnp.where(first, norms[0], other_norms),
        jnp.where(first, other_norms, norms[0]),
    ]
    gain = [[gains[l][k][None] for k in range(2)] for l in range(2)]
    w_in = [jnp.where(first, mlp_in[0], other_in), jnp.where(first, other_in, mlp_in[0])]
    w_out = [jnp.where(first, mlp_out[0], other_out), jnp.where(first, other_out, mlp_out[0])]

    stream_low = pick(inputs, core)
    stream = stream_low.astype(F32)
    top_low = pick(cotangent, core)
    ids = pick(segments, core)
    every_id = lax.all_gather(ids, "seq")

    def rooted(x):
        return x * lax.rsqrt(jnp.mean(x * x, axis=-1, keepdims=True) + EPSILON) * gain[0][0]

    normed_one = rooted(stream).astype(BF16)
    branches = jnp.einsum("td,dkr->ktr", normed_one, rec_in, preferred_element_type=F32)
    values = branches[0].astype(BF16)
    gate_pre = branches[1]
    before = from_behind(values[-8:], "seq", 1)
    ext = jnp.concatenate([before, values], axis=0)
    before_ids = pick(every_id, jnp.maximum(place - 1, 0))[-3:]
    ext_ids = jnp.concatenate([jnp.where(place == 0, -1, before_ids), ids])
    masks = jnp.stack(
        [(ext_ids[3 - k : 3 - k + count] == ids).astype(F32) for k in range(4)], axis=1
    )
    soft = jnp.broadcast_to(jax.nn.softplus(rec_chan[7:8]), rec_chan.shape)
    gates_flat = rec_gates.reshape(blocks, block, 2 * block)
    conv_low, pre, through, local, edge = rec_forward_local(ext, masks, rec_chan, soft, gates_flat)
    entering = carry(edge, False, 0)
    hidden_state = local + through * entering[0:1]
    mixed = (hidden_state * jax.nn.gelu(gate_pre)).astype(BF16)
    part = dot(mixed, rec_out, (1, 0), BF16)
    res_one, normed_a = join_forward("keep", part, own_rows(stream), gain[0][1], 1)

    gate_up_a, hidden_a, part = mlp_forward(normed_a, w_in[0], w_out[0])
    passed, normed_two = join_forward("round", part, res_one, gain[1][0], 2)

    head_dim = attn_kv.shape[1] // 2
    heads_here = attn_q.shape[1] // head_dim
    queries = dot(normed_two, attn_q, (1, 0), BF16).reshape(count, heads_here, head_dim)
    keyval = dot(normed_two, attn_kv, (1, 0), BF16)
    reach = min(max(1, WINDOW // count), blocks_seq - 1)
    window_kv = [from_behind(keyval, "seq", distance) for distance in range(reach, 0, -1)]
    all_keys = jnp.concatenate(window_kv + [keyval], axis=0)
    key_ids = jnp.concatenate(
        [pick(every_id, jnp.maximum(place - distance, 0)) for distance in range(reach, 0, -1)]
        + [ids]
    )
    key_spots = (place - reach) * count + jnp.arange((reach + 1) * count, dtype=jnp.int32)
    query_spots = place * count + jnp.arange(count, dtype=jnp.int32)
    distance_q = query_spots[:, None] - key_spots[None, :]
    inside = (distance_q >= 0) & (distance_q < WINDOW) & (key_spots >= 0)[None, :]
    allowed = inside & (ids[:, None] == key_ids[None, :])
    attended, log_totals = attend(queries, all_keys, allowed)
    attended = attended.reshape(count, heads_here * head_dim)
    part = dot(attended, attn_out, (1, 0), BF16)
    res_two, normed_b = join_forward("keep", part, passed, gain[1][1], 3)

    gate_up_b, hidden_b, part = mlp_forward(normed_b, w_in[1], w_out[1])
    _, final = join_forward("last", part, res_two, gain[1][1], 4)

    def mlp_grads(normed, hidden, grad_gate, grad_up, out_low, out_other):
        side, side_other = mine_and_other(grad_gate, grad_up)
        units = hidden.shape[1] // 2
        kept = columns(hidden, core * units, units)
        kept_other = swapped(columns(hidden, (1 - core) * units, units))
        grad_in = pair_grad(normed, swapped(normed), side, side_other)
        grad_out = pair_grad(out_low, out_other, kept, kept_other)
        return seq_scatter(grad_in), seq_scatter(grad_out)

    def half_columns(array):
        own = columns(array, core * half_width, half_width)
        return own, swapped(columns(array, (1 - core) * half_width, half_width))

    def half_grad(array_pair, right):
        return seq_scatter(pair_grad(array_pair[0], array_pair[1], right, swapped(right)))

    grad_gate_b, grad_up_b, part = mlp_backward(gate_up_b, w_in[1], w_out[1], top_low)
    grads_b = mlp_grads(
        normed_b, hidden_b, grad_gate_b, grad_up_b, top_low, pick(cotangent, 1 - core)
    )
    grad_res_two, gain_b, low_two = join_backward(
        "keep", part, res_two, gain[1][1], own_rows(top_low.astype(F32)), 5
    )

    grad_att = dot(low_two, attn_out, (1, 1), BF16)
    grad_query, grad_kv = attend_back(
        queries, all_keys, allowed, log_totals, grad_att.reshape(count, heads_here, head_dim)
    )
    own_kv = grad_kv[reach * count :]
    for distance in range(1, reach + 1):
        start = (reach - distance) * count
        own_kv = own_kv + from_behind(
            grad_kv[start : start + count].astype(BF16), "seq", -distance
        ).astype(F32)
    query_low = grad_query.reshape(count, heads_here * head_dim).astype(BF16)
    kv_part = own_kv.astype(BF16)
    part = (dot(query_low, attn_q, (1, 1)) + dot(kv_part, attn_kv, (1, 1))).astype(BF16)
    grad_passed, gain_two, low_passed = join_backward(
        "round", part, passed, gain[1][0], grad_res_two, 6
    )
    kv_low = lax.psum(kv_part.astype(F32), "head").astype(BF16)

    grad_gate_a, grad_up_a, part = mlp_backward(gate_up_a, w_in[0], w_out[0], low_passed)
    grads_a = mlp_grads(
        normed_a, hidden_a, grad_gate_a, grad_up_a, low_passed, swapped(low_passed)
    )
    grad_res_one, gain_a, mix_low = join_backward(
        "keep", part, res_one, gain[0][1], grad_passed, 7
    )

    grad_mixed = dot(mix_low, rec_out, (1, 1))
    grad_branch, beyond, local_grad, edge = rec_back_first(
        grad_mixed, gate_pre, hidden_state, pre, soft, masks, block
    )
    arriving = carry(edge, True, 9)
    gate_low, grad_values, over_edge, chan_grad = rec_back_second(
        beyond, local_grad, arriving, hidden_state, entering, pre, conv_low, rec_chan, soft,
        gates_flat, masks, ext,
    )
    from_next = from_behind(over_edge[:3], "seq", -1)
    grad_values = jnp.concatenate([grad_values[:-3], grad_values[-3:] + from_next]).astype(BF16)
    part = (dot(grad_values, rec_in[:, 0], (1, 1)) + dot(grad_branch, rec_in[:, 1], (1, 1))).astype(
        BF16
    )
    _, gain_one, grad_inputs = join_backward(
        "keep", part, own_rows(stream), gain[0][0], grad_res_one, 8
    )

    two_halves = half_columns(normed_two)
    grad_q = half_grad(two_halves, query_low).astype(F32)
    grad_kv_out = half_grad(two_halves, kv_low).astype(F32)
    grad_attn_out = half_grad(half_columns(low_two), attended).astype(F32).T

    one_halves = half_columns(normed_one)
    grad_in = jnp.stack(
        [half_grad(one_halves, grad_values), half_grad(one_halves, grad_branch)], axis=1
    ).astype(F32)
    grad_rec_out = half_grad(half_columns(mix_low), mixed).astype(F32).T
    gate_parts = jnp.einsum(
        "tnb,ktnc->bnkc",
        conv_low.reshape(count, blocks, block),
        gate_low.reshape(2, count, blocks, block),
        preferred_element_type=F32,
    ).reshape(block, blocks * 2 * block)
    gate_sum = lax.psum_scatter(
        gate_parts.astype(BF16), ("section", "seq"), scatter_dimension=0, tiled=True
    )
    grad_gates = jnp.swapaxes(gate_sum.astype(F32).reshape(-1, blocks, 2, block), 0, 1)
    chan_total = lax.psum(chan_grad, ("section", "seq"))
    grad_chan = jnp.where(first, chan_total[:4], chan_total[4:])

    own_part_in = jnp.where(first, grads_a[0], grads_b[0])
    other_part_in = swapped(jnp.where(first, grads_b[0], grads_a[0]))
    grad_mlp_in = jnp.stack(
        [
            jnp.where(first, own_part_in, other_part_in),
            jnp.where(first, other_part_in, own_part_in),
        ],
        axis=1,
    ).astype(F32)
    own_part_out = jnp.where(first, grads_a[1], grads_b[1])
    other_part_out = swapped(jnp.where(first, grads_b[1], grads_a[1]))
    grad_mlp_out = jnp.concatenate(
        [
            jnp.where(first, own_part_out, other_part_out).T,
            jnp.where(first, other_part_out, own_part_out).T,
        ],
        axis=0,
    ).astype(F32)

    gain_rows = jnp.concatenate([gain_one, gain_a, gain_two, gain_b], axis=0)
    gain_total = lax.psum(gain_rows, ("section", "seq", "head")).reshape(2, 2, width)
    share = width // blocks_seq
    grad_norms = lax.dynamic_slice_in_dim(pick(gain_total, core), place * share, share, axis=1)

    return (
        final[None],
        grad_inputs.astype(F32)[None],
        grad_norms[None],
        grad_in,
        grad_gates,
        grad_chan,
        grad_rec_out,
        grad_q,
        grad_kv_out,
        grad_attn_out,
        grad_mlp_in[None],
        grad_mlp_out[None],
    )


def solution(mesh):
    in_specs = (
        P(None, "seq", None),
        P(None, "seq"),
        P("section", None, None),
        P(None, None, "head"),
        P("head", None, None, None),
        P(None, "head"),
        P("head", None),
        P(None, "head"),
        P(),
        P("head", None),
        P("section", None, None, "head"),
        P("section", "head", None),
        P(None, "seq", None),
    )
    out_specs = (
        P("section", "seq", None),
        P("section", "seq", None),
        P("section", None, "seq"),
        P(("section", "seq"), None, "head"),
        P("head", ("section", "seq"), None, None),
        P("section", "head"),
        P("head", ("section", "seq")),
        P(("section", "seq"), "head"),
        P(("section", "seq"), None),
        P("head", ("section", "seq")),
        P("section", "seq", None, "head"),
        P("section", "head", "seq"),
    )
    return jax.shard_map(
        on_device, mesh=mesh, in_specs=in_specs, out_specs=out_specs, check_vma=False
    )
```

```python
import functools

import jax
import jax.numpy as jnp
from jax import lax
from jax.experimental import pallas as pl
from jax.experimental.pallas import tpu as pltpu
from jax.sharding import PartitionSpec as P

WINDOW = 1024
EPSILON = 1e-06
MESH = pl.DeviceIdType.MESH
F32 = jnp.float32
BF16 = jnp.bfloat16
SWAP = [(0, 1), (1, 0)]


def dot(a, b, dims, out=F32):
    return lax.dot_general(a, b, ((dims[:1], dims[1:]), ((), ())), preferred_element_type=F32).astype(
        out
    )


def vmem():
    return pl.BlockSpec(memory_space=pltpu.VMEM)


def meet(axis, me, n):
    barrier = pltpu.get_barrier_semaphore()
    for k in range(1, n):
        peer = lax.rem(me + k, n)
        pl.semaphore_signal(barrier, inc=1, device_id={axis: peer}, device_id_type=MESH)
    pl.semaphore_wait(barrier, n - 1)


def remote(src, dst, send, recv, axis, peer):
    return pltpu.make_async_remote_copy(
        src_ref=src,
        dst_ref=dst,
        send_sem=send,
        recv_sem=recv,
        device_id={axis: peer},
        device_id_type=MESH,
    )


def scatter_start(n, me, rows, part, recv, send_sem, recv_sem):
    copies = []
    for k in range(1, n):
        peer = lax.rem(me + k, n)
        start = pl.multiple_of(peer * rows, rows)
        copies.append(
            remote(
                part.at[pl.ds(start, rows)],
                recv.at[k - 1],
                send_sem.at[k - 1],
                recv_sem.at[k - 1],
                "head",
                peer,
            )
        )
    for copy in copies:
        copy.start()
    return copies


def scatter_sum(me, rows, part, recv, copies):
    total = part[pl.ds(pl.multiple_of(me * rows, rows), rows)].astype(F32)
    for k, copy in enumerate(copies):
        copy.wait_recv()
        total = total + recv[k].astype(F32)
    return total


def drain(copies):
    for copy in copies:
        copy.wait_send()


def spread(n, me, rows, value, full, send_sem, recv_sem):
    mine = pl.ds(pl.multiple_of(me * rows, rows), rows)
    full[mine] = value
    copies = []
    for k in range(1, n):
        peer = lax.rem(me + k, n)
        copies.append(
            remote(
                full.at[mine], full.at[mine], send_sem.at[k - 1], recv_sem.at[k - 1], "head", peer
            )
        )
    for copy in copies:
        copy.start()
    return copies


def finish(copies):
    for copy in copies:
        copy.wait()


def forward_body(n, kind, part, base, gain, new, full, recv, s1, r1, s2, r2):
    me = lax.axis_index("head")
    rows = base.shape[0]
    meet("head", me, n)
    sent = scatter_start(n, me, rows, part, recv, s1, r1)
    fresh = base[...] + scatter_sum(me, rows, part, recv, sent)
    if kind == "last":
        new[...] = fresh
        out = fresh
    else:
        if kind == "round":
            fresh = fresh.astype(BF16).astype(F32)
        new[...] = fresh
        out = fresh * lax.rsqrt(jnp.mean(fresh * fresh, axis=-1, keepdims=True) + EPSILON)
        out = out * gain[...]
    finish(spread(n, me, rows, out.astype(BF16), full, s2, r2))
    drain(sent)


def backward_body(n, kind, part, base, gain, up, *refs):
    extra = None
    if kind == "round":
        extra, res, gain_grad, full, extra_full, recv, s1, r1, s2, r2, extra_recv, s3, r3, s4, r4 = refs
    else:
        res, gain_grad, full, recv, s1, r1, s2, r2 = refs
    me = lax.axis_index("head")
    rows = base.shape[0]
    meet("head", me, n)
    if extra is not None:
        sent_extra = scatter_start(n, me, rows, extra, extra_recv, s3, r3)
    sent = scatter_start(n, me, rows, part, recv, s1, r1)
    if extra is not None:
        joined = scatter_sum(me, rows, extra, extra_recv, sent_extra)
        done = spread(n, me, rows, joined.astype(BF16), extra_full, s4, r4)
    grad = scatter_sum(me, rows, part, recv, sent)
    v = base[...]
    scale = lax.rsqrt(jnp.mean(v * v, axis=-1, keepdims=True) + EPSILON)
    gain_grad[...] = jnp.sum(grad * v * scale, axis=0, keepdims=True)
    inner = grad * gain[...]
    out = up[...] + scale * inner - v * (
        scale * scale * scale * jnp.mean(inner * v, axis=-1, keepdims=True)
    )
    if kind == "round":
        out = out.astype(BF16).astype(F32)
    res[...] = out
    finish(spread(n, me, rows, out.astype(BF16), full, s2, r2))
    drain(sent)
    if extra is not None:
        finish(done)
        drain(sent_extra)


def boundary_scratch(n, rows, width):
    return [pltpu.VMEM((n - 1, rows, width), BF16)] + [pltpu.SemaphoreType.DMA((n - 1,))] * 4


def join_forward(kind, part, base, gain, ident):
    n = lax.axis_size("head")
    count, width = part.shape
    rows = base.shape[0]
    return pl.pallas_call(
        functools.partial(forward_body, n, kind),
        name=f"join_forward_{ident}",
        out_shape=(
            jax.ShapeDtypeStruct((rows, width), F32),
            jax.ShapeDtypeStruct((count, width), BF16),
        ),
        in_specs=[vmem()] * 3,
        out_specs=(vmem(), vmem()),
        scratch_shapes=boundary_scratch(n, rows, width),
        compiler_params=pltpu.CompilerParams(collective_id=ident, has_side_effects=True),
    )(part, base, gain)


def join_backward(kind, part, base, gain, up, ident, extra=None):
    n = lax.axis_size("head")
    count, width = part.shape
    rows = base.shape[0]
    outs = [
        jax.ShapeDtypeStruct((rows, width), F32),
        jax.ShapeDtypeStruct((1, width), F32),
        jax.ShapeDtypeStruct((count, width), BF16),
    ]
    scratch = boundary_scratch(n, rows, width)
    operands = [part, base, gain, up]
    if extra is not None:
        outs.append(jax.ShapeDtypeStruct(extra.shape, BF16))
        scratch += boundary_scratch(n, rows, extra.shape[1])
        operands.append(extra)
    return pl.pallas_call(
        functools.partial(backward_body, n, kind),
        name=f"join_backward_{ident}",
        out_shape=tuple(outs),
        in_specs=[vmem()] * len(operands),
        out_specs=tuple(vmem() for _ in outs),
        scratch_shapes=scratch,
        compiler_params=pltpu.CompilerParams(collective_id=ident, has_side_effects=True),
    )(*operands)


def start_body(n, tail, ids, before, every, s0, r0, send_sem, recv_sem):
    me = lax.axis_index("seq")
    meet("seq", me, n)
    copies = [remote(tail, before, s0, r0, "seq", lax.rem(me + 1, n))]
    every[me] = ids[...]
    for k in range(1, n):
        peer = lax.rem(me + k, n)
        copies.append(
            remote(ids, every.at[me], send_sem.at[k - 1], recv_sem.at[k - 1], "seq", peer)
        )
    for copy in copies:
        copy.start()
    finish(copies)


def start_exchange(tail, ids, ident):
    n = lax.axis_size("seq")
    return pl.pallas_call(
        functools.partial(start_body, n),
        name="start_exchange",
        out_shape=(
            jax.ShapeDtypeStruct(tail.shape, BF16),
            jax.ShapeDtypeStruct((n,) + ids.shape, jnp.int32),
        ),
        in_specs=[vmem(), vmem()],
        out_specs=(vmem(), vmem()),
        scratch_shapes=[
            pltpu.SemaphoreType.DMA,
            pltpu.SemaphoreType.DMA,
            pltpu.SemaphoreType.DMA((n - 1,)),
            pltpu.SemaphoreType.DMA((n - 1,)),
        ],
        compiler_params=pltpu.CompilerParams(collective_id=ident, has_side_effects=True),
    )(tail, ids)


def totals_body(heads, blocks, gains, chan, gain_out, chan_out, *scratch):
    g1, g2, g3, sum_one, sum_two, c2, c3, csum, sems = scratch
    head, place, core = lax.axis_index("head"), lax.axis_index("seq"), lax.axis_index("section")
    barrier = pltpu.get_barrier_semaphore()
    for axis, me, n in (("head", head, heads), ("seq", place, blocks), ("section", core, 2)):
        for k in range(1, n):
            pl.semaphore_signal(
                barrier, inc=1, device_id={axis: lax.rem(me + k, n)}, device_id_type=MESH
            )
    pl.semaphore_wait(barrier, heads + blocks - 1)
    used = 0

    def exchange(src, slots, axis, me, n):
        nonlocal used
        copies = []
        for k in range(1, n):
            copies.append(
                remote(
                    src, slots.at[k - 1], sems.at[0, used], sems.at[1, used], axis, lax.rem(me + k, n)
                )
            )
            used += 1
        for copy in copies:
            copy.start()
        return copies

    def collect(copies, src, slots):
        total = src[...]
        for k, copy in enumerate(copies):
            copy.wait_recv()
            total = total + slots[k]
        return total

    by_head = exchange(gains, g1, "head", head, heads)
    chan_seq = exchange(chan, c2, "seq", place, blocks)
    sum_one[...] = collect(by_head, gains, g1)
    gain_seq = exchange(sum_one, g2, "seq", place, blocks)
    csum[...] = collect(chan_seq, chan, c2)
    chan_core = exchange(csum, c3, "section", core, 2)
    sum_two[...] = collect(gain_seq, sum_one, g2)
    gain_core = exchange(sum_two, g3, "section", core, 2)
    chan_out[...] = collect(chan_core, csum, c3)
    gain_out[...] = collect(gain_core, sum_two, g3)
    for copy in by_head + chan_seq + gain_seq + chan_core + gain_core:
        copy.wait_send()


def totals(gains, chan, ident):
    heads, blocks = lax.axis_size("head"), lax.axis_size("seq")
    gs, cs = gains.shape, chan.shape
    return pl.pallas_call(
        functools.partial(totals_body, heads, blocks),
        name="totals",
        out_shape=(jax.ShapeDtypeStruct(gs, F32), jax.ShapeDtypeStruct(cs, F32)),
        in_specs=[vmem(), vmem()],
        out_specs=(vmem(), vmem()),
        scratch_shapes=[
            pltpu.VMEM((heads - 1,) + gs, F32),
            pltpu.VMEM((blocks - 1,) + gs, F32),
            pltpu.VMEM((1,) + gs, F32),
            pltpu.VMEM(gs, F32),
            pltpu.VMEM(gs, F32),
            pltpu.VMEM((blocks - 1,) + cs, F32),
            pltpu.VMEM((1,) + cs, F32),
            pltpu.VMEM(cs, F32),
            pltpu.SemaphoreType.DMA((2, heads + 2 * blocks)),
        ],
        compiler_params=pltpu.CompilerParams(collective_id=ident, has_side_effects=True),
    )(gains, chan)


def either(core, layer, own, other, run):
    @pl.when(core[0] == layer)
    def _():
        run(*own)

    @pl.when(core[0] != layer)
    def _():
        run(*other)


def weight_specs(layer, width, units, tile):
    def at_own(i, core):
        return jnp.where(core[0] == layer, i, 0)

    def at_other(i, core):
        return jnp.where(core[0] == layer, 0, i)

    return [
        pl.BlockSpec((2, width, tile), lambda i, core: (0, 0, at_own(i, core))),
        pl.BlockSpec((2, width, tile), lambda i, core: (0, 0, at_other(i, core))),
        pl.BlockSpec((tile, width), lambda i, core: (at_own(i, core), 0)),
        pl.BlockSpec((tile, width), lambda i, core: (at_other(i, core), 0)),
    ]


def mlp_forward_body(layer, steps, core, x, own_in, other_in, own_out, other_out, gate_up, hidden, part, acc):
    step = pl.program_id(0)

    @pl.when(step == 0)
    def _():
        acc[...] = jnp.zeros_like(acc)

    def run(w_in, w_out):
        gate = jnp.dot(x[...], w_in[0], preferred_element_type=F32)
        up = jnp.dot(x[...], w_in[1], preferred_element_type=F32)
        gate_up[0] = gate
        gate_up[1] = up
        low = (gelu_parts(gate)[0] * up).astype(BF16)
        hidden[...] = low
        acc[...] += jnp.dot(low, w_out[...], preferred_element_type=F32)

    either(core, layer, (own_in, own_out), (other_in, other_out), run)

    @pl.when(step == steps - 1)
    def _():
        part[...] = acc[...].astype(BF16)


def mlp_forward(layer, core, x, own_in, other_in, own_out, other_out):
    count, width = x.shape
    units = own_out.shape[0]
    tile = units // 3
    return pl.pallas_call(
        functools.partial(mlp_forward_body, layer, 3),
        name=f"mlp_forward_{layer}",
        grid_spec=pltpu.PrefetchScalarGridSpec(
            num_scalar_prefetch=1,
            grid=(3,),
            in_specs=[pl.BlockSpec((count, width), lambda i, core: (0, 0))]
            + weight_specs(layer, width, units, tile),
            out_specs=(
                pl.BlockSpec((2, count, tile), lambda i, core: (0, 0, i)),
                pl.BlockSpec((count, tile), lambda i, core: (0, i)),
                pl.BlockSpec((count, width), lambda i, core: (0, 0)),
            ),
            scratch_shapes=[pltpu.VMEM((count, width), F32)],
        ),
        out_shape=(
            jax.ShapeDtypeStruct((2, count, units), F32),
            jax.ShapeDtypeStruct((count, units), BF16),
            jax.ShapeDtypeStruct((count, width), BF16),
        ),
    )(core, x, own_in, other_in, own_out, other_out)


def mlp_backward_body(layer, steps, core, low, gate_up, own_in, other_in, own_out, other_out, pair, part, acc):
    step = pl.program_id(0)

    @pl.when(step == 0)
    def _():
        acc[...] = jnp.zeros_like(acc)

    over = (((1,), (1,)), ((), ()))

    def run(w_in, w_out):
        grad_hidden = lax.dot_general(low[...], w_out[...], over, preferred_element_type=F32)
        act, slope = gelu_parts(gate_up[0])
        grad_gate = (grad_hidden * gate_up[1] * slope).astype(BF16)
        grad_up = (grad_hidden * act).astype(BF16)
        pair[0] = grad_gate
        pair[1] = grad_up
        acc[...] += lax.dot_general(grad_gate, w_in[0], over, preferred_element_type=F32)
        acc[...] += lax.dot_general(grad_up, w_in[1], over, preferred_element_type=F32)

    either(core, layer, (own_in, own_out), (other_in, other_out), run)

    @pl.when(step == steps - 1)
    def _():
        part[...] = acc[...].astype(BF16)


def mlp_backward(layer, core, low, gate_up, own_in, other_in, own_out, other_out):
    count, width = low.shape
    units = own_out.shape[0]
    tile = units // 3
    return pl.pallas_call(
        functools.partial(mlp_backward_body, layer, 3),
        name=f"mlp_backward_{layer}",
        grid_spec=pltpu.PrefetchScalarGridSpec(
            num_scalar_prefetch=1,
            grid=(3,),
            in_specs=[
                pl.BlockSpec((count, width), lambda i, core: (0, 0)),
                pl.BlockSpec((2, count, tile), lambda i, core: (0, 0, i)),
            ]
            + weight_specs(layer, width, units, tile),
            out_specs=(
                pl.BlockSpec((2, count, tile), lambda i, core: (0, 0, i)),
                pl.BlockSpec((count, width), lambda i, core: (0, 0)),
            ),
            scratch_shapes=[pltpu.VMEM((count, width), F32)],
        ),
        out_shape=(
            jax.ShapeDtypeStruct((2, count, units), BF16),
            jax.ShapeDtypeStruct((count, width), BF16),
        ),
    )(core, low, gate_up, own_in, other_in, own_out, other_out)


def weight_grad_body(sizes, core, *refs):
    out = refs[-1]
    over = (((0,), (0,)), ((), ()))
    start = 0
    for t, size in enumerate(sizes):
        left, left_other, right, right_other = refs[4 * t : 4 * t + 4]
        total = lax.dot_general(left[...], right[...], over, preferred_element_type=F32)
        total += lax.dot_general(left_other[...], right_other[...], over, preferred_element_type=F32)
        out[:, start : start + size] = total.astype(BF16)
        start += size


def weight_grad(name, core, terms, half):
    count, width = terms[0][0].shape
    tile = 256
    steps = width // tile // (2 if half else 1)
    sizes = [term[2].shape[1] for term in terms]
    in_specs, operands = [], []
    for left, left_other, right, right_other in terms:
        if half:
            rows = pl.BlockSpec((count, tile), lambda i, core: (0, core[0] * steps + i))
        else:
            rows = pl.BlockSpec((count, tile), lambda i, core: (0, i))
        full = pl.BlockSpec(right.shape, lambda i, core: (0, 0))
        in_specs += [rows, rows, full, full]
        operands += [left, left_other, right, right_other]
    return pl.pallas_call(
        functools.partial(weight_grad_body, sizes),
        name=f"weight_grad_{name}",
        grid_spec=pltpu.PrefetchScalarGridSpec(
            num_scalar_prefetch=1,
            grid=(steps,),
            in_specs=in_specs,
            out_specs=pl.BlockSpec((tile, sum(sizes)), lambda i, core: (i, 0)),
        ),
        out_shape=jax.ShapeDtypeStruct((steps * tile, sum(sizes)), BF16),
    )(core, *operands)


def carry_body(n, reverse, edge, out, every, send_sem, recv_sem):
    me = lax.axis_index("seq")
    meet("seq", me, n)
    copies = []
    for k in range(1, n):
        peer = lax.rem(me + k, n)
        copies.append(
            remote(edge, every.at[k - 1], send_sem.at[k - 1], recv_sem.at[k - 1], "seq", peer)
        )
    for copy in copies:
        copy.start()
    for copy in copies:
        copy.wait()
    state = jnp.zeros((1, edge.shape[1]), F32)
    order = range(1, n) if reverse else range(n - 1, 0, -1)
    for k in order:
        sender = me - k if not reverse else me + n - k
        inside = sender >= 0 if not reverse else sender < n
        if reverse:
            inside = jnp.logical_and(inside, sender > me)
        slot = every[k - 1]
        state = jnp.where(inside, slot[0:1] * state + slot[1:2], state)
    out[...] = jnp.broadcast_to(state, out.shape)


def carry(edge, reverse, ident):
    n = lax.axis_size("seq")
    return pl.pallas_call(
        functools.partial(carry_body, n, reverse),
        name=f"carry_{ident}",
        out_shape=jax.ShapeDtypeStruct(edge.shape, F32),
        in_specs=[vmem()],
        out_specs=vmem(),
        scratch_shapes=[
            pltpu.VMEM((n - 1,) + edge.shape, F32),
            pltpu.SemaphoreType.DMA((n - 1,)),
            pltpu.SemaphoreType.DMA((n - 1,)),
        ],
        compiler_params=pltpu.CompilerParams(collective_id=ident, has_side_effects=True),
    )(edge)


def shifted(x, by, row, fill):
    count = x.shape[0]
    if by > 0:
        return jnp.where(row >= by, pltpu.roll(x, by, 0), fill)
    return jnp.where(row < count + by, pltpu.roll(x, count + by, 0), fill)


def scan_rows(a, b, row, sign):
    step = 1
    while step < a.shape[0]:
        b = b + a * shifted(b, sign * step, row, 0.0)
        a = a * shifted(a, sign * step, row, 1.0)
        step *= 2
    return a, b


def minus_expm1(y):
    series = jnp.full_like(y, 1.0)
    for k in range(9, 1, -1):
        series = 1.0 + y * series * (1.0 / k)
    return jnp.where(y > -0.5, -y * series, 1.0 - jnp.exp(y))


def gelu_parts(x):
    c = 0.7978845608028654
    inner = c * (x + 0.044715 * x * x * x)
    t = jnp.tanh(inner)
    act = 0.5 * x * (1.0 + t)
    slope = 0.5 * (1.0 + t) + 0.5 * x * (1.0 - t * t) * c * (1.0 + 3.0 * 0.044715 * x * x)
    return act, slope


def rec_forward_body(ext, masks, chan, soft, gates, conv_out, pre_out, through, local, edge):
    count = conv_out.shape[0]
    block = conv_out.shape[1]
    wide = ext[...].astype(F32)
    total = chan[4:5] + chan[0:1] * wide[16:]
    for k in range(1, 4):
        total = total + chan[k : k + 1] * pltpu.roll(wide, k, 0)[16:] * masks[:, k : k + 1]
    low = total.astype(BF16)
    conv_out[...] = low
    pre = jnp.dot(low, gates[0], preferred_element_type=F32)
    rate = pre[:, :block] + chan[5:6]
    gate = pre[:, block:] + chan[6:7]
    pre_out[0] = rate
    pre_out[1] = gate
    log_decay = -8.0 * jax.nn.sigmoid(rate) * soft[0:1]
    decay = jnp.exp(log_decay) * masks[:, 1:2]
    drive = jnp.sqrt(minus_expm1(2.0 * log_decay)) * jax.nn.sigmoid(gate) * low.astype(F32)
    row = lax.broadcasted_iota(jnp.int32, (count, block), 0)
    a, b = scan_rows(decay, drive, row, 1)
    through[...] = a
    local[...] = b
    edge[0:1] = a[count - 1 :]
    edge[1:2] = b[count - 1 :]
    edge[2:8] = jnp.zeros((6, block), F32)


def rec_forward_local(ext, masks, chan, soft, gates):
    count, chans = ext.shape[0] - 16, ext.shape[1]
    blocks, block = gates.shape[:2]
    wide = pl.BlockSpec((count, block), lambda i: (0, i))
    row8 = pl.BlockSpec((8, block), lambda i: (0, i))
    return pl.pallas_call(
        rec_forward_body,
        name="rec_forward_local",
        grid=(blocks,),
        out_shape=(
            jax.ShapeDtypeStruct((count, chans), BF16),
            jax.ShapeDtypeStruct((2, count, chans), F32),
            jax.ShapeDtypeStruct((count, chans), F32),
            jax.ShapeDtypeStruct((count, chans), F32),
            jax.ShapeDtypeStruct((8, chans), F32),
        ),
        in_specs=[
            pl.BlockSpec((count + 16, block), lambda i: (0, i)),
            pl.BlockSpec((count, 4), lambda i: (0, 0)),
            row8,
            row8,
            pl.BlockSpec((1, block, 2 * block), lambda i: (i, 0, 0)),
        ],
        out_specs=(
            wide,
            pl.BlockSpec((2, count, block), lambda i: (0, 0, i)),
            wide,
            wide,
            row8,
        ),
    )(ext, masks, chan, soft, gates)


def rec_back_first_body(gm, gate_pre, hidden, rate, soft, masks, grad_gate, beyond, local, edge):
    count, block = gm.shape
    act, slope = gelu_parts(gate_pre[...])
    up = gm[...]
    grad_gate[...] = (up * hidden[...] * slope).astype(BF16)
    decay = jnp.exp(-8.0 * jax.nn.sigmoid(rate[0]) * soft[0:1]) * masks[:, 1:2]
    row = lax.broadcasted_iota(jnp.int32, (count, block), 0)
    a, b = scan_rows(shifted(decay, -1, row, 1.0), up * act, row, -1)
    beyond[...] = a
    local[...] = b
    edge[0:1] = decay[0:1] * a[0:1]
    edge[1:2] = decay[0:1] * b[0:1]
    edge[2:8] = jnp.zeros((6, block), F32)


def rec_back_first(gm, gate_pre, hidden, pre, soft, masks, block):
    count, chans = gm.shape
    wide = pl.BlockSpec((count, block), lambda i: (0, i))
    row8 = pl.BlockSpec((8, block), lambda i: (0, i))
    return pl.pallas_call(
        rec_back_first_body,
        name="rec_back_first",
        grid=(chans // block,),
        out_shape=(
            jax.ShapeDtypeStruct((count, chans), BF16),
            jax.ShapeDtypeStruct((count, chans), F32),
            jax.ShapeDtypeStruct((count, chans), F32),
            jax.ShapeDtypeStruct((8, chans), F32),
        ),
        in_specs=[
            wide,
            wide,
            wide,
            pl.BlockSpec((1, count, block), lambda i: (0, 0, i)),
            row8,
            pl.BlockSpec((count, 4), lambda i: (0, 0)),
        ],
        out_specs=(wide, wide, wide, row8),
    )(gm, gate_pre, hidden, pre, soft, masks)


def rec_back_second_body(
    beyond, local, arriving, hidden, entering, pre, conv, chan, soft, gates, masks, ext,
    gate_low, grad_values, edge, chan_grad,
):
    count, block = local.shape
    row = lax.broadcasted_iota(jnp.int32, (count, block), 0)
    state = local[...] + beyond[...] * arriving[0:1]
    earlier = jnp.where(row >= 1, pltpu.roll(hidden[...], 1, 0), entering[0:1])
    low = conv[...].astype(F32)
    keep_rate = jax.nn.sigmoid(pre[0])
    log_decay = -8.0 * keep_rate * soft[0:1]
    decay = jnp.exp(log_decay)
    size = jnp.sqrt(minus_expm1(2.0 * log_decay))
    gate = jax.nn.sigmoid(pre[1])
    grad_decay = state * earlier * masks[:, 1:2]
    grad_log = grad_decay * decay - state * gate * low * (decay * decay / size)
    grad_rate = grad_log * (-8.0 * soft[0:1]) * keep_rate * (1.0 - keep_rate)
    grad_gate = state * size * low * gate * (1.0 - gate)
    rate_low = grad_rate.astype(BF16)
    gate_low_part = grad_gate.astype(BF16)
    gate_low[0] = rate_low
    gate_low[1] = gate_low_part
    weights = gates[0]
    over = (((1,), (1,)), ((), ()))
    grad_conv = (
        state * size * gate
        + lax.dot_general(rate_low, weights[:, :block], over, preferred_element_type=F32)
        + lax.dot_general(gate_low_part, weights[:, block:], over, preferred_element_type=F32)
    )
    wide = ext[...].astype(F32)
    total = chan[0:1] * grad_conv
    chan_grad[0:1] = jnp.sum(grad_conv * wide[16:], axis=0, keepdims=True)
    row8 = lax.broadcasted_iota(jnp.int32, (8, block), 0)
    over_edge = jnp.zeros((8, block), F32)
    for k in range(1, 4):
        masked = grad_conv * masks[:, k : k + 1]
        chan_grad[k : k + 1] = jnp.sum(masked * pltpu.roll(wide, k, 0)[16:], axis=0, keepdims=True)
        back = chan[k : k + 1] * masked
        total = total + shifted(back, -k, row, 0.0)
        first = back[0:8]
        if k < 3:
            first = pltpu.roll(first, 3 - k, 0)
        over_edge = over_edge + jnp.where((row8 >= 3 - k) & (row8 < 3), first, 0.0)
    grad_values[...] = total
    edge[...] = over_edge
    chan_grad[4:5] = jnp.sum(grad_conv, axis=0, keepdims=True)
    chan_grad[5:6] = jnp.sum(grad_rate, axis=0, keepdims=True)
    chan_grad[6:7] = jnp.sum(grad_gate, axis=0, keepdims=True)
    chan_grad[7:8] = jnp.sum(grad_log * keep_rate, axis=0, keepdims=True) * (
        -8.0 * jax.nn.sigmoid(chan[7:8])
    )


def rec_back_second(beyond, local, arriving, hidden, entering, pre, conv, chan, soft, gates, masks, ext):
    count, chans = local.shape
    blocks, block = gates.shape[:2]
    wide = pl.BlockSpec((count, block), lambda i: (0, i))
    row8 = pl.BlockSpec((8, block), lambda i: (0, i))
    pair = pl.BlockSpec((2, count, block), lambda i: (0, 0, i))
    return pl.pallas_call(
        rec_back_second_body,
        name="rec_back_second",
        grid=(blocks,),
        out_shape=(
            jax.ShapeDtypeStruct((2, count, chans), BF16),
            jax.ShapeDtypeStruct((count, chans), F32),
            jax.ShapeDtypeStruct((8, chans), F32),
            jax.ShapeDtypeStruct((8, chans), F32),
        ),
        in_specs=[
            wide,
            wide,
            row8,
            wide,
            row8,
            pair,
            wide,
            row8,
            row8,
            pl.BlockSpec((1, block, 2 * block), lambda i: (i, 0, 0)),
            pl.BlockSpec((count, 4), lambda i: (0, 0)),
            pl.BlockSpec((count + 16, block), lambda i: (0, i)),
        ],
        out_specs=(pair, wide, row8, row8),
    )(beyond, local, arriving, hidden, entering, pre, conv, chan, soft, gates, masks, ext)


def from_behind(array, axis, by):
    devices = lax.axis_size(axis)
    pairs = [(i, i + by) for i in range(devices) if 0 <= i + by < devices]
    return lax.ppermute(array, axis, pairs)


def swapped(array):
    return lax.ppermute(array, "section", SWAP)


def attend(query_rows, key_rows, allowed):
    head_dim = query_rows.shape[2]
    scores = jnp.einsum(
        "qhd,kd->hqk", query_rows, key_rows[:, :head_dim], preferred_element_type=F32
    ) * head_dim ** (-0.5)
    masked = jnp.where(allowed[None], scores, -1e30)
    row_max = jnp.max(masked, axis=-1, keepdims=True)
    lifted = jnp.exp(masked - row_max)
    row_total = jnp.sum(lifted, axis=-1, keepdims=True)
    weights = (lifted / row_total).astype(BF16)
    attended = jnp.einsum(
        "hqk,kd->qhd", weights, key_rows[:, head_dim:], preferred_element_type=F32
    ).astype(BF16)
    return (attended, row_max[:, :, 0] + jnp.log(row_total[:, :, 0]))


def attend_back(query_rows, key_rows, allowed, log_total, grad_rows):
    head_dim = query_rows.shape[2]
    factor = head_dim ** (-0.5)
    scores = (
        jnp.einsum("qhd,kd->hqk", query_rows, key_rows[:, :head_dim], preferred_element_type=F32)
        * factor
    )
    probs = jnp.exp(jnp.where(allowed[None], scores, -1e30) - log_total[:, :, None])
    weights = probs.astype(BF16)
    grad_probs = jnp.einsum(
        "qhd,kd->hqk", grad_rows, key_rows[:, head_dim:], preferred_element_type=F32
    )
    grad_values = jnp.einsum("hqk,qhd->kd", weights, grad_rows, preferred_element_type=F32)
    grad_scores = (
        probs * (grad_probs - jnp.sum(grad_probs * probs, axis=-1, keepdims=True))
    ).astype(BF16)
    grad_query = (
        jnp.einsum("hqk,kd->qhd", grad_scores, key_rows[:, :head_dim], preferred_element_type=F32)
        * factor
    )
    grad_keys = (
        jnp.einsum("hqk,qhd->kd", grad_scores, query_rows, preferred_element_type=F32) * factor
    )
    return (grad_query, jnp.concatenate([grad_keys, grad_values], axis=-1))


def seq_scatter(grad):
    return lax.psum_scatter(grad, "seq", scatter_dimension=0, tiled=True)


def columns(array, start, size):
    return lax.dynamic_slice_in_dim(array, start, size, axis=1)


def on_device(
    inputs,
    segments,
    norms,
    rec_in,
    rec_gates,
    rec_chan,
    rec_out,
    attn_q,
    attn_kv,
    attn_out,
    mlp_in,
    mlp_out,
    cotangent,
):
    core = lax.axis_index("section")
    first = core == 0
    place = lax.axis_index("seq")
    rank = lax.axis_index("head")
    heads = lax.axis_size("head")
    blocks_seq = lax.axis_size("seq")
    _, count, width = inputs.shape
    rows = count // heads
    chans = rec_in.shape[2]
    blocks, block = rec_gates.shape[:2]

    def pick(array, index):
        return lax.dynamic_index_in_dim(array, index, 0, keepdims=False)

    def own_rows(array):
        return lax.dynamic_slice_in_dim(array, rank * rows, rows, axis=0)

    core_ref = core[None].astype(jnp.int32)
    ids = pick(segments, core)
    stream_low = pick(inputs, core)
    top_low = pick(cotangent, core)
    before, every_id = start_exchange(stream_low[-16:], ids[None], 10)
    every_id = every_id[:, 0]

    own_in = jnp.swapaxes(mlp_in[0], 0, 1)
    other_in, other_out, other_norms = swapped(own_in), swapped(mlp_out[0]), swapped(norms[0])
    gains = [
        jnp.where(first, norms[0], other_norms),
        jnp.where(first, other_norms, norms[0]),
    ]
    gain = [[gains[l][k][None] for k in range(2)] for l in range(2)]
    weights = (own_in, other_in, mlp_out[0], other_out)

    def rooted(x):
        return x * lax.rsqrt(jnp.mean(x * x, axis=-1, keepdims=True) + EPSILON) * gain[0][0]

    ext_normed = rooted(jnp.concatenate([before, stream_low]).astype(F32)).astype(BF16)
    normed_one = ext_normed[16:]
    ext = dot(ext_normed, rec_in[:, 0], (1, 0), BF16)
    gate_pre = dot(normed_one, rec_in[:, 1], (1, 0))
    before_ids = pick(every_id, jnp.maximum(place - 1, 0))[-3:]
    ext_ids = jnp.concatenate([jnp.where(place == 0, -1, before_ids), ids])
    masks = jnp.stack(
        [(ext_ids[3 - k : 3 - k + count] == ids).astype(F32) for k in range(4)], axis=1
    )
    soft = jnp.broadcast_to(jax.nn.softplus(rec_chan[7:8]), rec_chan.shape)
    gates_flat = rec_gates.reshape(blocks, block, 2 * block)
    conv_low, pre, through, local, edge = rec_forward_local(ext, masks, rec_chan, soft, gates_flat)
    entering = carry(edge, False, 0)
    hidden_state = local + through * entering[0:1]
    mixed = (hidden_state * jax.nn.gelu(gate_pre)).astype(BF16)
    part = dot(mixed, rec_out, (1, 0), BF16)
    stream_rows = own_rows(stream_low).astype(F32)
    res_one, normed_a = join_forward("keep", part, stream_rows, gain[0][1], 1)

    gate_up_a, hidden_a, part = mlp_forward(0, core_ref, normed_a, *weights)
    passed, normed_two = join_forward("round", part, res_one, gain[1][0], 2)

    head_dim = attn_kv.shape[1] // 2
    heads_here = attn_q.shape[1] // head_dim
    queries = dot(normed_two, attn_q, (1, 0), BF16).reshape(count, heads_here, head_dim)
    keyval = dot(normed_two, attn_kv, (1, 0), BF16)
    reach = min(max(1, WINDOW // count), blocks_seq - 1)
    window_kv = [from_behind(keyval, "seq", distance) for distance in range(reach, 0, -1)]
    all_keys = jnp.concatenate(window_kv + [keyval], axis=0)
    key_ids = jnp.concatenate(
        [pick(every_id, jnp.maximum(place - distance, 0)) for distance in range(reach, 0, -1)]
        + [ids]
    )
    key_spots = (place - reach) * count + jnp.arange((reach + 1) * count, dtype=jnp.int32)
    query_spots = place * count + jnp.arange(count, dtype=jnp.int32)
    distance_q = query_spots[:, None] - key_spots[None, :]
    inside = (distance_q >= 0) & (distance_q < WINDOW) & (key_spots >= 0)[None, :]
    allowed = inside & (ids[:, None] == key_ids[None, :])
    attended, log_totals = attend(queries, all_keys, allowed)
    attended = attended.reshape(count, heads_here * head_dim)
    part = dot(attended, attn_out, (1, 0), BF16)
    res_two, normed_b = join_forward("keep", part, passed, gain[1][1], 3)

    gate_up_b, hidden_b, part_last = mlp_forward(1, core_ref, normed_b, *weights)

    units = hidden_b.shape[1] // 2

    def mlp_term(pair, normed, hidden, out_low, out_other):
        side, side_other = pick(pair, core), swapped(pick(pair, 1 - core))
        kept = columns(hidden, core * units, units)
        kept_other = swapped(columns(hidden, (1 - core) * units, units))
        return [(normed, swapped(normed), side, side_other), (out_low, out_other, kept, kept_other)]

    pair_b, part = mlp_backward(1, core_ref, top_low, gate_up_b, *weights)
    terms = mlp_term(pair_b, normed_b, hidden_b, top_low, pick(cotangent, 1 - core))
    part, sum_b = lax.optimization_barrier((part, weight_grad("b", core_ref, terms, False)))
    sum_b = seq_scatter(sum_b)
    grad_res_two, gain_b, low_two = join_backward(
        "keep", part, res_two, gain[1][1], own_rows(top_low).astype(F32), 5
    )

    grad_att = dot(low_two, attn_out, (1, 1), BF16)
    grad_query, grad_kv = attend_back(
        queries, all_keys, allowed, log_totals, grad_att.reshape(count, heads_here, head_dim)
    )
    own_kv = grad_kv[reach * count :]
    for distance in range(1, reach + 1):
        start = (reach - distance) * count
        own_kv = own_kv + from_behind(
            grad_kv[start : start + count].astype(BF16), "seq", -distance
        ).astype(F32)
    query_low = grad_query.reshape(count, heads_here * head_dim).astype(BF16)
    kv_part = own_kv.astype(BF16)
    part = (dot(query_low, attn_q, (1, 1)) + dot(kv_part, attn_kv, (1, 1))).astype(BF16)
    grad_passed, gain_two, low_passed, kv_low = join_backward(
        "round", part, passed, gain[1][0], grad_res_two, 6, kv_part
    )

    pair_a, part = mlp_backward(0, core_ref, low_passed, gate_up_a, *weights)
    normed_two_other = swapped(normed_two)
    attn_sum = weight_grad(
        "attention",
        core_ref,
        [
            (normed_two, normed_two_other, query_low, swapped(query_low)),
            (normed_two, normed_two_other, kv_low, swapped(kv_low)),
            (low_two, swapped(low_two), attended, swapped(attended)),
        ],
        True,
    )
    terms = mlp_term(pair_a, normed_a, hidden_a, low_passed, swapped(low_passed))
    part, sum_a, attn_sum = lax.optimization_barrier(
        (part, weight_grad("a", core_ref, terms, False), attn_sum)
    )
    attn_sum = seq_scatter(attn_sum)
    sum_a = seq_scatter(sum_a)
    grad_res_one, gain_a, mix_low = join_backward(
        "keep", part, res_one, gain[0][1], grad_passed, 7
    )

    grad_mixed = dot(mix_low, rec_out, (1, 1))
    grad_branch, beyond, local_grad, edge = rec_back_first(
        grad_mixed, gate_pre, hidden_state, pre, soft, masks, block
    )
    arriving = carry(edge, True, 9)
    gate_low, grad_values, over_edge, chan_grad = rec_back_second(
        beyond, local_grad, arriving, hidden_state, entering, pre, conv_low, rec_chan, soft,
        gates_flat, masks, ext,
    )
    from_next = from_behind(over_edge[:3], "seq", -1)
    grad_values = jnp.concatenate([grad_values[:-3], grad_values[-3:] + from_next]).astype(BF16)
    part = (dot(grad_values, rec_in[:, 0], (1, 1)) + dot(grad_branch, rec_in[:, 1], (1, 1))).astype(
        BF16
    )
    normed_one_other = swapped(normed_one)
    rec_sum = weight_grad(
        "recurrent",
        core_ref,
        [
            (normed_one, normed_one_other, grad_values, swapped(grad_values)),
            (normed_one, normed_one_other, grad_branch, swapped(grad_branch)),
            (mix_low, swapped(mix_low), mixed, swapped(mixed)),
        ],
        True,
    )
    side = pick(gate_low, core)
    side_other = swapped(pick(gate_low, 1 - core))
    conv_other = swapped(conv_low)

    def gate_grad(left, right):
        return jnp.einsum(
            "tnb,tnc->bnc",
            left.reshape(count, blocks, block),
            right.reshape(count, blocks, block),
            preferred_element_type=F32,
        )

    gate_sum = (gate_grad(conv_low, side) + gate_grad(conv_other, side_other)).astype(BF16)
    share = block // (2 * blocks_seq)
    gate_sum = jnp.swapaxes(
        gate_sum.reshape(2, blocks_seq, share, chans), 0, 1
    ).reshape(block, chans)
    part, rec_sum, gate_sum = lax.optimization_barrier((part, rec_sum, gate_sum))
    rec_sum = seq_scatter(rec_sum)
    gate_sum = seq_scatter(gate_sum).reshape(2, share, chans)
    _, gain_one, grad_inputs = join_backward(
        "keep", part, stream_rows, gain[0][0], grad_res_one, 8
    )
    part_last, grad_inputs, gain_one = lax.optimization_barrier((part_last, grad_inputs, gain_one))
    _, final = join_forward("last", part_last, res_two, gain[1][1], 4)

    gain_rows = jnp.concatenate([gain_one, gain_a, gain_two, gain_b], axis=0)
    gain_total, chan_total = totals(gain_rows, chan_grad, 11)
    share_norm = width // blocks_seq
    grad_norms = lax.dynamic_slice_in_dim(
        pick(gain_total.reshape(2, 2, width), core), place * share_norm, share_norm, axis=1
    )
    grad_chan = jnp.where(first, chan_total[:4], chan_total[4:])

    chans_q = attn_q.shape[1]
    attn_sum = attn_sum.astype(F32)
    grad_q = attn_sum[:, :chans_q]
    grad_kv_out = attn_sum[:, chans_q : chans_q + 2 * head_dim]
    grad_attn_out = attn_sum[:, chans_q + 2 * head_dim :].T
    rec_sum = rec_sum.astype(F32)
    grad_in = rec_sum[:, : 2 * chans].reshape(-1, 2, chans)
    grad_rec_out = rec_sum[:, 2 * chans :].T
    own_gate = pick(gate_sum, core)
    other_gate = swapped(pick(gate_sum, 1 - core))
    grad_gates = jnp.transpose(
        jnp.stack([jnp.where(first, own_gate, other_gate), jnp.where(first, other_gate, own_gate)])
        .astype(F32)
        .reshape(2, share, blocks, block),
        (2, 1, 0, 3),
    )
    own_part = jnp.where(first, sum_a, sum_b)
    other_part = swapped(jnp.where(first, sum_b, sum_a))
    lower = jnp.where(first, own_part, other_part).astype(F32)
    upper = jnp.where(first, other_part, own_part).astype(F32)
    grad_mlp_in = jnp.stack([lower[:, : 2 * units], upper[:, : 2 * units]], axis=1)
    grad_mlp_out = jnp.concatenate([lower[:, 2 * units :].T, upper[:, 2 * units :].T], axis=0)

    return (
        final[None],
        grad_inputs.astype(F32)[None],
        grad_norms[None],
        grad_in,
        grad_gates,
        grad_chan,
        grad_rec_out,
        grad_q,
        grad_kv_out,
        grad_attn_out,
        grad_mlp_in[None],
        grad_mlp_out[None],
    )


def solution(mesh):
    in_specs = (
        P(None, "seq", None),
        P(None, "seq"),
        P("section", None, None),
        P(None, None, "head"),
        P("head", None, None, None),
        P(None, "head"),
        P("head", None),
        P(None, "head"),
        P(),
        P("head", None),
        P("section", None, None, "head"),
        P("section", "head", None),
        P(None, "seq", None),
    )
    out_specs = (
        P("section", "seq", None),
        P("section", "seq", None),
        P("section", None, "seq"),
        P(("section", "seq"), None, "head"),
        P("head", ("section", "seq"), None, None),
        P("section", "head"),
        P("head", ("section", "seq")),
        P(("section", "seq"), "head"),
        P(("section", "seq"), None),
        P("head", ("section", "seq")),
        P("section", "seq", None, "head"),
        P("section", "head", "seq"),
    )
    return jax.shard_map(
        on_device, mesh=mesh, in_specs=in_specs, out_specs=out_specs, check_vma=False
    )
```

```python
import functools

import jax
import jax.numpy as jnp
from jax import lax
from jax.experimental import pallas as pl
from jax.experimental.pallas import tpu as pltpu
from jax.sharding import PartitionSpec as P

WINDOW = 1024
EPSILON = 1e-06
MESH = pl.DeviceIdType.MESH
F32 = jnp.float32
BF16 = jnp.bfloat16
SWAP = [(0, 1), (1, 0)]


def dot(a, b, dims, out=F32):
    return lax.dot_general(a, b, ((dims[:1], dims[1:]), ((), ())), preferred_element_type=F32).astype(
        out
    )


def vmem():
    return pl.BlockSpec(memory_space=pltpu.VMEM)


def meet(axis, me, n):
    barrier = pltpu.get_barrier_semaphore()
    for k in range(1, n):
        peer = lax.rem(me + k, n)
        pl.semaphore_signal(barrier, inc=1, device_id={axis: peer}, device_id_type=MESH)
    pl.semaphore_wait(barrier, n - 1)


def remote(src, dst, send, recv, axis, peer):
    return pltpu.make_async_remote_copy(
        src_ref=src,
        dst_ref=dst,
        send_sem=send,
        recv_sem=recv,
        device_id={axis: peer},
        device_id_type=MESH,
    )


def scatter_start(n, me, rows, part, recv, send_sem, recv_sem):
    copies = []
    for k in range(1, n):
        peer = lax.rem(me + k, n)
        start = pl.multiple_of(peer * rows, rows)
        copies.append(
            remote(
                part.at[pl.ds(start, rows)],
                recv.at[k - 1],
                send_sem.at[k - 1],
                recv_sem.at[k - 1],
                "head",
                peer,
            )
        )
    for copy in copies:
        copy.start()
    return copies


def scatter_sum(me, rows, part, recv, copies):
    total = part[pl.ds(pl.multiple_of(me * rows, rows), rows)].astype(F32)
    for k, copy in enumerate(copies):
        copy.wait_recv()
        total = total + recv[k].astype(F32)
    return total


def drain(copies):
    for copy in copies:
        copy.wait_send()


def spread(n, me, rows, value, full, send_sem, recv_sem):
    mine = pl.ds(pl.multiple_of(me * rows, rows), rows)
    full[mine] = value
    copies = []
    for k in range(1, n):
        peer = lax.rem(me + k, n)
        copies.append(
            remote(
                full.at[mine], full.at[mine], send_sem.at[k - 1], recv_sem.at[k - 1], "head", peer
            )
        )
    for copy in copies:
        copy.start()
    return copies


def finish(copies):
    for copy in copies:
        copy.wait()


def forward_body(n, kind, part, base, gain, new, full, recv, s1, r1, s2, r2):
    me = lax.axis_index("head")
    rows = base.shape[0]
    meet("head", me, n)
    sent = scatter_start(n, me, rows, part, recv, s1, r1)
    fresh = base[...] + scatter_sum(me, rows, part, recv, sent)
    new[...] = fresh
    out = fresh
    if kind != "last":
        out = fresh * lax.rsqrt(jnp.mean(fresh * fresh, axis=-1, keepdims=True) + EPSILON)
        out = out * gain[...]
    finish(spread(n, me, rows, out.astype(BF16), full, s2, r2))
    drain(sent)


def meet_around(n, me, blocks, place, pairs):
    barrier = pltpu.get_barrier_semaphore()
    for d, k in pairs:
        device = {
            "seq": lax.rem(place - d + blocks, blocks),
            "head": lax.rem(me - k + n, n),
        }
        pl.semaphore_signal(barrier, inc=1, device_id=device, device_id_type=MESH)
    pl.semaphore_wait(barrier, len(pairs))


def keys_body(n, blocks, reach, part, base, gain, w_kv, new, full, keys, recv, s1, r1, s2, r2, own, s3, r3):
    me, place = lax.axis_index("head"), lax.axis_index("seq")
    rows = base.shape[0]
    count = part.shape[0]
    pairs = [(d, k) for d in range(reach + 1) for k in range(n) if (d, k) != (0, 0)]
    meet_around(n, me, blocks, place, pairs)
    sent = scatter_start(n, me, rows, part, recv, s1, r1)
    fresh = base[...] + scatter_sum(me, rows, part, recv, sent)
    fresh = fresh.astype(BF16).astype(F32)
    new[...] = fresh
    out = fresh * lax.rsqrt(jnp.mean(fresh * fresh, axis=-1, keepdims=True) + EPSILON)
    low = (out * gain[...]).astype(BF16)
    spreading = spread(n, me, rows, low, full, s2, r2)
    value = jnp.dot(low, w_kv[...], preferred_element_type=F32).astype(BF16)
    own[...] = value
    mine = pl.multiple_of(me * rows, rows)
    keys[pl.ds(reach * count + mine, rows)] = value
    copies = []
    for d, k in pairs:
        copies.append(
            pltpu.make_async_remote_copy(
                src_ref=own,
                dst_ref=keys.at[pl.ds((reach - d) * count + mine, rows)],
                send_sem=s3.at[d * n + k],
                recv_sem=r3.at[d * n + k],
                device_id={
                    "seq": lax.rem(place + d, blocks),
                    "head": lax.rem(me + k, n),
                },
                device_id_type=MESH,
            )
        )
    for copy in copies:
        copy.start()
    finish(spreading)
    finish(copies)
    drain(sent)


def norm_back_rows(grad, v, gain, up):
    scale = lax.rsqrt(jnp.mean(v * v, axis=-1, keepdims=True) + EPSILON)
    gain_grad = jnp.sum(grad * v * scale, axis=0, keepdims=True)
    inner = grad * gain
    out = up + scale * inner - v * (
        scale * scale * scale * jnp.mean(inner * v, axis=-1, keepdims=True)
    )
    return out, gain_grad


def backward_body(n, part, base, gain, up, res, gain_grad, full, recv, s1, r1, s2, r2):
    me = lax.axis_index("head")
    rows = base.shape[0]
    meet("head", me, n)
    sent = scatter_start(n, me, rows, part, recv, s1, r1)
    grad = scatter_sum(me, rows, part, recv, sent)
    out, gain_grad[...] = norm_back_rows(grad, base[...], gain[...], up[...])
    res[...] = out
    finish(spread(n, me, rows, out.astype(BF16), full, s2, r2))
    drain(sent)


def keys_back_body(
    n, blocks, reach, part, base, gain, up, grad_kv, w_kv, res, gain_grad, full, kv_full,
    recv, s1, r1, s2, r2, recv_kv, s3, r3, send_z, recv_z, s4, r4, s5, r5,
):
    me, place = lax.axis_index("head"), lax.axis_index("seq")
    rows = base.shape[0]
    meet_around(
        n,
        me,
        blocks,
        place,
        [(0, k) for k in range(1, n)] + [(-d, 0) for d in range(1, reach + 1)],
    )
    mine = pl.ds(pl.multiple_of(me * rows, rows), rows)
    kv_sent = []
    for k in range(1, n):
        peer = lax.rem(me + k, n)
        there = pl.ds(pl.multiple_of(peer * rows, rows), rows)
        kv_sent.append(
            remote(
                grad_kv.at[:, there], recv_kv.at[k - 1], s3.at[k - 1], r3.at[k - 1], "head", peer
            )
        )
    for copy in kv_sent:
        copy.start()
    sent = scatter_start(n, me, rows, part, recv, s1, r1)
    total = grad_kv[:, mine].astype(F32)
    for k, copy in enumerate(kv_sent):
        copy.wait_recv()
        total = total + recv_kv[k].astype(F32)
    send_z[...] = total.astype(BF16)
    z_sent = []
    for d in range(1, reach + 1):
        z_sent.append(
            remote(
                send_z.at[reach - d],
                recv_z.at[d - 1],
                s4.at[d - 1],
                r4.at[d - 1],
                "seq",
                lax.rem(place - d + blocks, blocks),
            )
        )
    for copy in z_sent:
        copy.start()
    grad = scatter_sum(me, rows, part, recv, sent)
    own_kv = total[reach]
    for d, copy in enumerate(z_sent):
        copy.wait_recv()
        own_kv = own_kv + recv_z[d].astype(F32)
    kv_low = own_kv.astype(BF16)
    kv_spread = spread(n, me, rows, kv_low, kv_full, s5, r5)
    grad = grad + lax.dot_general(
        kv_low, w_kv[...], (((1,), (1,)), ((), ())), preferred_element_type=F32
    )
    out, gain_grad[...] = norm_back_rows(grad, base[...], gain[...], up[...])
    low = out.astype(BF16)
    res[...] = low.astype(F32)
    finish(spread(n, me, rows, low, full, s2, r2))
    finish(kv_spread)
    drain(sent + kv_sent + z_sent)


def boundary_scratch(n, rows, width):
    return [pltpu.VMEM((n - 1, rows, width), BF16)] + [pltpu.SemaphoreType.DMA((n - 1,))] * 4


def join_forward(kind, part, base, gain, ident):
    n = lax.axis_size("head")
    count, width = part.shape
    rows = base.shape[0]
    return pl.pallas_call(
        functools.partial(forward_body, n, kind),
        name=f"join_forward_{ident}",
        out_shape=(
            jax.ShapeDtypeStruct((rows, width), F32),
            jax.ShapeDtypeStruct((count, width), BF16),
        ),
        in_specs=[vmem()] * 3,
        out_specs=(vmem(), vmem()),
        scratch_shapes=boundary_scratch(n, rows, width),
        compiler_params=pltpu.CompilerParams(collective_id=ident, has_side_effects=True),
    )(part, base, gain)


def join_keys(part, base, gain, w_kv, reach, ident):
    n, blocks = lax.axis_size("head"), lax.axis_size("seq")
    count, width = part.shape
    rows = base.shape[0]
    both = w_kv.shape[1]
    slots = (reach + 1) * n
    return pl.pallas_call(
        functools.partial(keys_body, n, blocks, reach),
        name="join_keys",
        out_shape=(
            jax.ShapeDtypeStruct((rows, width), F32),
            jax.ShapeDtypeStruct((count, width), BF16),
            jax.ShapeDtypeStruct(((reach + 1) * count, both), BF16),
        ),
        in_specs=[vmem()] * 4,
        out_specs=(vmem(), vmem(), vmem()),
        scratch_shapes=boundary_scratch(n, rows, width)
        + [
            pltpu.VMEM((rows, both), BF16),
            pltpu.SemaphoreType.DMA((slots,)),
            pltpu.SemaphoreType.DMA((slots,)),
        ],
        compiler_params=pltpu.CompilerParams(collective_id=ident, has_side_effects=True),
    )(part, base, gain, w_kv)


def join_backward(part, base, gain, up, ident):
    n = lax.axis_size("head")
    count, width = part.shape
    rows = base.shape[0]
    return pl.pallas_call(
        functools.partial(backward_body, n),
        name=f"join_backward_{ident}",
        out_shape=(
            jax.ShapeDtypeStruct((rows, width), F32),
            jax.ShapeDtypeStruct((1, width), F32),
            jax.ShapeDtypeStruct((count, width), BF16),
        ),
        in_specs=[vmem()] * 4,
        out_specs=(vmem(), vmem(), vmem()),
        scratch_shapes=boundary_scratch(n, rows, width),
        compiler_params=pltpu.CompilerParams(collective_id=ident, has_side_effects=True),
    )(part, base, gain, up)


def join_keys_back(part, base, gain, up, grad_kv, w_kv, ident):
    n, blocks = lax.axis_size("head"), lax.axis_size("seq")
    count, width = part.shape
    rows = base.shape[0]
    reach, both = grad_kv.shape[0] - 1, grad_kv.shape[2]
    dma = pltpu.SemaphoreType.DMA
    return pl.pallas_call(
        functools.partial(keys_back_body, n, blocks, reach),
        name="join_keys_back",
        out_shape=(
            jax.ShapeDtypeStruct((rows, width), F32),
            jax.ShapeDtypeStruct((1, width), F32),
            jax.ShapeDtypeStruct((count, width), BF16),
            jax.ShapeDtypeStruct((count, both), BF16),
        ),
        in_specs=[vmem()] * 6,
        out_specs=tuple([vmem()] * 4),
        scratch_shapes=boundary_scratch(n, rows, width)
        + [
            pltpu.VMEM((n - 1, reach + 1, rows, both), BF16),
            dma((n - 1,)),
            dma((n - 1,)),
            pltpu.VMEM((reach + 1, rows, both), BF16),
            pltpu.VMEM((reach, rows, both), BF16),
            dma((reach,)),
            dma((reach,)),
            dma((n - 1,)),
            dma((n - 1,)),
        ],
        compiler_params=pltpu.CompilerParams(collective_id=ident, has_side_effects=True),
    )(part, base, gain, up, grad_kv, w_kv)


def totals_body(heads, blocks, gains, chan, gates, gain_out, chan_out, gate_out, *scratch):
    g1, g2, g3, sum_one, sum_two, c2, c3, csum, w2, sems = scratch
    head, place, core = lax.axis_index("head"), lax.axis_index("seq"), lax.axis_index("section")
    barrier = pltpu.get_barrier_semaphore()
    for axis, me, n in (("head", head, heads), ("seq", place, blocks), ("section", core, 2)):
        for k in range(1, n):
            pl.semaphore_signal(
                barrier, inc=1, device_id={axis: lax.rem(me + k, n)}, device_id_type=MESH
            )
    pl.semaphore_wait(barrier, heads + blocks - 1)
    used = 0

    def exchange(src, slots, axis, me, n, split=False):
        nonlocal used
        copies = []
        for k in range(1, n):
            peer = lax.rem(me + k, n)
            copies.append(
                remote(
                    src.at[peer] if split else src,
                    slots.at[k - 1],
                    sems.at[0, used],
                    sems.at[1, used],
                    axis,
                    peer,
                )
            )
            used += 1
        for copy in copies:
            copy.start()
        return copies

    def collect(copies, src, slots):
        total = src[...]
        for k, copy in enumerate(copies):
            copy.wait_recv()
            total = total + slots[k]
        return total

    by_head = exchange(gains, g1, "head", head, heads)
    chan_seq = exchange(chan, c2, "seq", place, blocks)
    gate_seq = exchange(gates, w2, "seq", place, blocks, True)
    sum_one[...] = collect(by_head, gains, g1)
    gain_seq = exchange(sum_one, g2, "seq", place, blocks)
    csum[...] = collect(chan_seq, chan, c2)
    chan_core = exchange(csum, c3, "section", core, 2)
    sum_two[...] = collect(gain_seq, sum_one, g2)
    gain_core = exchange(sum_two, g3, "section", core, 2)
    chan_out[...] = collect(chan_core, csum, c3)
    gain_out[...] = collect(gain_core, sum_two, g3)
    gate_total = gates[place].astype(F32)
    for k, copy in enumerate(gate_seq):
        copy.wait_recv()
        gate_total = gate_total + w2[k].astype(F32)
    gate_out[...] = gate_total.astype(BF16)
    for copy in by_head + chan_seq + gate_seq + gain_seq + chan_core + gain_core:
        copy.wait_send()


def totals(gains, chan, gates, ident):
    heads, blocks = lax.axis_size("head"), lax.axis_size("seq")
    gs, cs, ws = gains.shape, chan.shape, gates.shape[1:]
    return pl.pallas_call(
        functools.partial(totals_body, heads, blocks),
        name="totals",
        out_shape=(
            jax.ShapeDtypeStruct(gs, F32),
            jax.ShapeDtypeStruct(cs, F32),
            jax.ShapeDtypeStruct(ws, BF16),
        ),
        in_specs=[vmem(), vmem(), vmem()],
        out_specs=(vmem(), vmem(), vmem()),
        scratch_shapes=[
            pltpu.VMEM((heads - 1,) + gs, F32),
            pltpu.VMEM((blocks - 1,) + gs, F32),
            pltpu.VMEM((1,) + gs, F32),
            pltpu.VMEM(gs, F32),
            pltpu.VMEM(gs, F32),
            pltpu.VMEM((blocks - 1,) + cs, F32),
            pltpu.VMEM((1,) + cs, F32),
            pltpu.VMEM(cs, F32),
            pltpu.VMEM((blocks - 1,) + ws, BF16),
            pltpu.SemaphoreType.DMA((2, heads + 3 * blocks)),
        ],
        compiler_params=pltpu.CompilerParams(collective_id=ident, has_side_effects=True),
    )(gains, chan, gates)


def either(core, layer, own, other, run):
    @pl.when(core[0] == layer)
    def _():
        run(*own)

    @pl.when(core[0] != layer)
    def _():
        run(*other)


def weight_specs(layer, width, units, tile):
    def at_own(i, core):
        return jnp.where(core[0] == layer, i, 0)

    def at_other(i, core):
        return jnp.where(core[0] == layer, 0, i)

    return [
        pl.BlockSpec((2, width, tile), lambda i, core: (0, 0, at_own(i, core))),
        pl.BlockSpec((2, width, tile), lambda i, core: (0, 0, at_other(i, core))),
        pl.BlockSpec((tile, width), lambda i, core: (at_own(i, core), 0)),
        pl.BlockSpec((tile, width), lambda i, core: (at_other(i, core), 0)),
    ]


def mlp_forward_body(layer, steps, core, x, own_in, other_in, own_out, other_out, gate_up, hidden, part, acc):
    step = pl.program_id(0)

    @pl.when(step == 0)
    def _():
        acc[...] = jnp.zeros_like(acc)

    def run(w_in, w_out):
        gate = jnp.dot(x[...], w_in[0], preferred_element_type=F32)
        up = jnp.dot(x[...], w_in[1], preferred_element_type=F32)
        gate_up[0] = gate
        gate_up[1] = up
        low = (gelu_parts(gate)[0] * up).astype(BF16)
        hidden[...] = low
        acc[...] += jnp.dot(low, w_out[...], preferred_element_type=F32)

    either(core, layer, (own_in, own_out), (other_in, other_out), run)

    @pl.when(step == steps - 1)
    def _():
        part[...] = acc[...].astype(BF16)


def mlp_forward(layer, core, x, own_in, other_in, own_out, other_out):
    count, width = x.shape
    units = own_out.shape[0]
    tile = units // 3
    return pl.pallas_call(
        functools.partial(mlp_forward_body, layer, 3),
        name=f"mlp_forward_{layer}",
        grid_spec=pltpu.PrefetchScalarGridSpec(
            num_scalar_prefetch=1,
            grid=(3,),
            in_specs=[pl.BlockSpec((count, width), lambda i, core: (0, 0))]
            + weight_specs(layer, width, units, tile),
            out_specs=(
                pl.BlockSpec((2, count, tile), lambda i, core: (0, 0, i)),
                pl.BlockSpec((count, tile), lambda i, core: (0, i)),
                pl.BlockSpec((count, width), lambda i, core: (0, 0)),
            ),
            scratch_shapes=[pltpu.VMEM((count, width), F32)],
        ),
        out_shape=(
            jax.ShapeDtypeStruct((2, count, units), F32),
            jax.ShapeDtypeStruct((count, units), BF16),
            jax.ShapeDtypeStruct((count, width), BF16),
        ),
    )(core, x, own_in, other_in, own_out, other_out)


OVER_LAST = (((1,), (1,)), ((), ()))


def mlp_grad_tile(core, low, gate, up, w_in, w_out, mine, theirs, acc):
    grad_hidden = lax.dot_general(low[...], w_out[...], OVER_LAST, preferred_element_type=F32)
    act, slope = gelu_parts(gate)
    grad_gate = (grad_hidden * up * slope).astype(BF16)
    grad_up = (grad_hidden * act).astype(BF16)
    swap = core[0] == 0
    mine[...] = jnp.where(swap, grad_gate, grad_up)
    theirs[...] = jnp.where(swap, grad_up, grad_gate)
    acc[...] += lax.dot_general(grad_gate, w_in[0], OVER_LAST, preferred_element_type=F32)
    acc[...] += lax.dot_general(grad_up, w_in[1], OVER_LAST, preferred_element_type=F32)
    return act


def mlp_backward_body(
    layer, steps, core, low, gate_up, own_in, other_in, own_out, other_out, mine, theirs, part, acc
):
    step = pl.program_id(0)

    @pl.when(step == 0)
    def _():
        acc[...] = jnp.zeros_like(acc)

    def run(w_in, w_out):
        mlp_grad_tile(core, low, gate_up[0], gate_up[1], w_in, w_out, mine, theirs, acc)

    either(core, layer, (own_in, own_out), (other_in, other_out), run)

    @pl.when(step == steps - 1)
    def _():
        part[...] = acc[...].astype(BF16)


def mlp_backward(layer, core, low, gate_up, own_in, other_in, own_out, other_out):
    count, width = low.shape
    units = own_out.shape[0]
    tile = units // 3
    column = pl.BlockSpec((count, tile), lambda i, core: (0, i))
    return pl.pallas_call(
        functools.partial(mlp_backward_body, layer, 3),
        name=f"mlp_backward_{layer}",
        grid_spec=pltpu.PrefetchScalarGridSpec(
            num_scalar_prefetch=1,
            grid=(3,),
            in_specs=[
                pl.BlockSpec((count, width), lambda i, core: (0, 0)),
                pl.BlockSpec((2, count, tile), lambda i, core: (0, 0, i)),
            ]
            + weight_specs(layer, width, units, tile),
            out_specs=(column, column, pl.BlockSpec((count, width), lambda i, core: (0, 0))),
            scratch_shapes=[pltpu.VMEM((count, width), F32)],
        ),
        out_shape=(
            jax.ShapeDtypeStruct((count, units), BF16),
            jax.ShapeDtypeStruct((count, units), BF16),
            jax.ShapeDtypeStruct((count, width), BF16),
        ),
    )(core, low, gate_up, own_in, other_in, own_out, other_out)


def mlp_both_body(
    layer, steps, core, x, low, own_in, other_in, own_out, other_out,
    hidden, mine, theirs, part, part_back, acc, acc_back,
):
    step = pl.program_id(0)

    @pl.when(step == 0)
    def _():
        acc[...] = jnp.zeros_like(acc)
        acc_back[...] = jnp.zeros_like(acc_back)

    def run(w_in, w_out):
        gate = jnp.dot(x[...], w_in[0], preferred_element_type=F32)
        up = jnp.dot(x[...], w_in[1], preferred_element_type=F32)
        act = mlp_grad_tile(core, low, gate, up, w_in, w_out, mine, theirs, acc_back)
        value = (act * up).astype(BF16)
        hidden[...] = value
        acc[...] += jnp.dot(value, w_out[...], preferred_element_type=F32)

    either(core, layer, (own_in, own_out), (other_in, other_out), run)

    @pl.when(step == steps - 1)
    def _():
        part[...] = acc[...].astype(BF16)
        part_back[...] = acc_back[...].astype(BF16)


def mlp_both(layer, core, x, low, own_in, other_in, own_out, other_out):
    count, width = x.shape
    units = own_out.shape[0]
    tile = units // 3
    column = pl.BlockSpec((count, tile), lambda i, core: (0, i))
    whole = pl.BlockSpec((count, width), lambda i, core: (0, 0))
    narrow = jax.ShapeDtypeStruct((count, units), BF16)
    wide = jax.ShapeDtypeStruct((count, width), BF16)
    return pl.pallas_call(
        functools.partial(mlp_both_body, layer, 3),
        name=f"mlp_both_{layer}",
        grid_spec=pltpu.PrefetchScalarGridSpec(
            num_scalar_prefetch=1,
            grid=(3,),
            in_specs=[whole, whole] + weight_specs(layer, width, units, tile),
            out_specs=(column, column, column, whole, whole),
            scratch_shapes=[pltpu.VMEM((count, width), F32)] * 2,
        ),
        out_shape=(narrow, narrow, narrow, wide, wide),
    )(core, x, low, own_in, other_in, own_out, other_out)


def weight_grad_body(sizes, core, *refs):
    out = refs[-1]
    over = (((0,), (0,)), ((), ()))
    start = 0
    for t, size in enumerate(sizes):
        left, left_other, right, right_other = refs[4 * t : 4 * t + 4]
        spare = right.shape[1] - size
        if spare:
            window = pl.ds(pl.multiple_of(core[0] * spare, 128), size)
            near, far = right[:, window], right_other[:, window]
        else:
            near, far = right[...], right_other[...]
        total = lax.dot_general(left[...], near, over, preferred_element_type=F32)
        total += lax.dot_general(left_other[...], far, over, preferred_element_type=F32)
        out[:, start : start + size] = total.astype(BF16)
        start += size


def weight_grad(name, core, terms, half):
    count, width = terms[0][0].shape
    tile = 256
    steps = width // tile // (2 if half else 1)
    sizes = [term[4] for term in terms]
    in_specs, operands = [], []
    for left, left_other, right, right_other, _ in terms:
        if half:
            rows = pl.BlockSpec((count, tile), lambda i, core: (0, core[0] * steps + i))
        else:
            rows = pl.BlockSpec((count, tile), lambda i, core: (0, i))
        full = pl.BlockSpec(right.shape, lambda i, core: (0, 0))
        in_specs += [rows, rows, full, full]
        operands += [left, left_other, right, right_other]
    return pl.pallas_call(
        functools.partial(weight_grad_body, sizes),
        name=f"weight_grad_{name}",
        grid_spec=pltpu.PrefetchScalarGridSpec(
            num_scalar_prefetch=1,
            grid=(steps,),
            in_specs=in_specs,
            out_specs=pl.BlockSpec((tile, sum(sizes)), lambda i, core: (i, 0)),
        ),
        out_shape=jax.ShapeDtypeStruct((steps * tile, sum(sizes)), BF16),
    )(core, *operands)


def carry_body(n, reverse, edge, out, every, send_sem, recv_sem):
    me = lax.axis_index("seq")
    meet("seq", me, n)
    copies = []
    for k in range(1, n):
        peer = lax.rem(me + k, n)
        copies.append(
            remote(edge, every.at[k - 1], send_sem.at[k - 1], recv_sem.at[k - 1], "seq", peer)
        )
    for copy in copies:
        copy.start()
    for copy in copies:
        copy.wait()
    state = jnp.zeros((1, edge.shape[1]), F32)
    order = range(1, n) if reverse else range(n - 1, 0, -1)
    for k in order:
        sender = me - k if not reverse else me + n - k
        inside = sender >= 0 if not reverse else sender < n
        if reverse:
            inside = jnp.logical_and(inside, sender > me)
        slot = every[k - 1]
        state = jnp.where(inside, slot[0:1] * state + slot[1:2], state)
    out[...] = jnp.broadcast_to(state, out.shape)


def carry(edge, reverse, ident):
    n = lax.axis_size("seq")
    return pl.pallas_call(
        functools.partial(carry_body, n, reverse),
        name=f"carry_{ident}",
        out_shape=jax.ShapeDtypeStruct(edge.shape, F32),
        in_specs=[vmem()],
        out_specs=vmem(),
        scratch_shapes=[
            pltpu.VMEM((n - 1,) + edge.shape, F32),
            pltpu.SemaphoreType.DMA((n - 1,)),
            pltpu.SemaphoreType.DMA((n - 1,)),
        ],
        compiler_params=pltpu.CompilerParams(collective_id=ident, has_side_effects=True),
    )(edge)


def shifted(x, by, row, fill):
    count = x.shape[0]
    if by > 0:
        return jnp.where(row >= by, pltpu.roll(x, by, 0), fill)
    return jnp.where(row < count + by, pltpu.roll(x, count + by, 0), fill)


def scan_rows(a, b, row, sign):
    step = 1
    while step < a.shape[0]:
        b = b + a * shifted(b, sign * step, row, 0.0)
        a = a * shifted(a, sign * step, row, 1.0)
        step *= 2
    return a, b


def minus_expm1(y):
    series = jnp.full_like(y, 1.0)
    for k in range(9, 1, -1):
        series = 1.0 + y * series * (1.0 / k)
    return jnp.where(y > -0.5, -y * series, 1.0 - jnp.exp(y))


def gelu_parts(x):
    c = 0.7978845608028654
    inner = c * (x + 0.044715 * x * x * x)
    t = jnp.tanh(inner)
    act = 0.5 * x * (1.0 + t)
    slope = 0.5 * (1.0 + t) + 0.5 * x * (1.0 - t * t) * c * (1.0 + 3.0 * 0.044715 * x * x)
    return act, slope


def same_rows(ids, k):
    return (pltpu.roll(ids, k, 0)[16:] == ids[16:]).astype(F32)


def rec_forward_body(
    x, gain, w_in, ids, chan, soft, gates,
    normed, gate_pre, ext, conv_out, pre_out, through, local, edge, low_x,
):
    count, block = conv_out.shape

    @pl.when(pl.program_id(0) == 0)
    def _():
        v = x[...].astype(F32)
        out = v * lax.rsqrt(jnp.mean(v * v, axis=-1, keepdims=True) + EPSILON) * gain[...]
        low = out.astype(BF16)
        low_x[...] = low
        normed[...] = low[16:]

    values = jnp.dot(low_x[...], w_in[0], preferred_element_type=F32).astype(BF16)
    gate_pre[...] = jnp.dot(low_x[16:], w_in[1], preferred_element_type=F32)
    ext[...] = values
    wide = values.astype(F32)
    total = chan[4:5] + chan[0:1] * wide[16:]
    for k in range(1, 4):
        total = total + chan[k : k + 1] * pltpu.roll(wide, k, 0)[16:] * same_rows(ids[...], k)
    low = total.astype(BF16)
    conv_out[...] = low
    pre = jnp.dot(low, gates[0], preferred_element_type=F32)
    rate = pre[:, :block] + chan[5:6]
    gate = pre[:, block:] + chan[6:7]
    pre_out[0] = rate
    pre_out[1] = gate
    log_decay = -8.0 * jax.nn.sigmoid(rate) * soft[...]
    decay = jnp.exp(log_decay) * same_rows(ids[...], 1)
    drive = jnp.sqrt(minus_expm1(2.0 * log_decay)) * jax.nn.sigmoid(gate) * low.astype(F32)
    row = lax.broadcasted_iota(jnp.int32, (count, block), 0)
    a, b = scan_rows(decay, drive, row, 1)
    through[...] = a
    local[...] = b
    edge[0:1] = a[count - 1 :]
    edge[1:2] = b[count - 1 :]
    edge[2:8] = jnp.zeros((6, block), F32)


def rec_forward(x, gain, w_in, ids, chan, soft, gates):
    count, width = x.shape[0] - 16, x.shape[1]
    chans = w_in.shape[2]
    blocks, block = gates.shape[:2]
    wide = pl.BlockSpec((count, block), lambda i: (0, i))
    row8 = pl.BlockSpec((8, block), lambda i: (0, i))
    tall = pl.BlockSpec((count + 16, block), lambda i: (0, i))
    f32 = jax.ShapeDtypeStruct((count, chans), F32)
    return pl.pallas_call(
        rec_forward_body,
        name="rec_forward",
        grid=(blocks,),
        out_shape=(
            jax.ShapeDtypeStruct((count, width), BF16),
            f32,
            jax.ShapeDtypeStruct((count + 16, chans), BF16),
            jax.ShapeDtypeStruct((count, chans), BF16),
            jax.ShapeDtypeStruct((2, count, chans), F32),
            f32,
            f32,
            jax.ShapeDtypeStruct((8, chans), F32),
        ),
        in_specs=[
            pl.BlockSpec((count + 16, width), lambda i: (0, 0)),
            pl.BlockSpec((1, width), lambda i: (0, 0)),
            pl.BlockSpec((2, width, block), lambda i: (0, 0, i)),
            pl.BlockSpec((count + 16, 128), lambda i: (0, 0)),
            row8,
            pl.BlockSpec((1, block), lambda i: (0, i)),
            pl.BlockSpec((1, block, 2 * block), lambda i: (i, 0, 0)),
        ],
        out_specs=(
            pl.BlockSpec((count, width), lambda i: (0, 0)),
            wide,
            tall,
            wide,
            pl.BlockSpec((2, count, block), lambda i: (0, 0, i)),
            wide,
            wide,
            row8,
        ),
        scratch_shapes=[pltpu.VMEM((count + 16, width), BF16)],
    )(x, gain, w_in, ids, chan, soft, gates)


def rec_finish_body(steps, local, through, entering, gate_pre, w_out, hidden, mixed, part, acc):
    step = pl.program_id(0)

    @pl.when(step == 0)
    def _():
        acc[...] = jnp.zeros_like(acc)

    state = local[...] + through[...] * entering[0:1]
    hidden[...] = state
    low = (state * gelu_parts(gate_pre[...])[0]).astype(BF16)
    mixed[...] = low
    acc[...] += jnp.dot(low, w_out[...], preferred_element_type=F32)

    @pl.when(step == steps - 1)
    def _():
        part[...] = acc[...].astype(BF16)


def rec_finish(local, through, entering, gate_pre, w_out):
    count, chans = local.shape
    width = w_out.shape[1]
    tile = chans // 2
    wide = pl.BlockSpec((count, tile), lambda i: (0, i))
    return pl.pallas_call(
        functools.partial(rec_finish_body, 2),
        name="rec_finish",
        grid=(2,),
        out_shape=(
            jax.ShapeDtypeStruct((count, chans), F32),
            jax.ShapeDtypeStruct((count, chans), BF16),
            jax.ShapeDtypeStruct((count, width), BF16),
        ),
        in_specs=[
            wide,
            wide,
            pl.BlockSpec((8, tile), lambda i: (0, i)),
            wide,
            pl.BlockSpec((tile, width), lambda i: (i, 0)),
        ],
        out_specs=(wide, wide, pl.BlockSpec((count, width), lambda i: (0, 0))),
        scratch_shapes=[pltpu.VMEM((count, width), F32)],
    )(local, through, entering, gate_pre, w_out)


def rec_back_first_body(gm, gate_pre, hidden, rate, soft, ids, grad_gate, beyond, local, edge):
    count, block = gm.shape
    act, slope = gelu_parts(gate_pre[...])
    up = gm[...]
    grad_gate[...] = (up * hidden[...] * slope).astype(BF16)
    decay = jnp.exp(-8.0 * jax.nn.sigmoid(rate[0]) * soft[...]) * same_rows(ids[...], 1)
    row = lax.broadcasted_iota(jnp.int32, (count, block), 0)
    a, b = scan_rows(shifted(decay, -1, row, 1.0), up * act, row, -1)
    beyond[...] = a
    local[...] = b
    edge[0:1] = decay[0:1] * a[0:1]
    edge[1:2] = decay[0:1] * b[0:1]
    edge[2:8] = jnp.zeros((6, block), F32)


def rec_back_first(gm, gate_pre, hidden, pre, soft, ids, block):
    count, chans = gm.shape
    wide = pl.BlockSpec((count, block), lambda i: (0, i))
    row8 = pl.BlockSpec((8, block), lambda i: (0, i))
    return pl.pallas_call(
        rec_back_first_body,
        name="rec_back_first",
        grid=(chans // block,),
        out_shape=(
            jax.ShapeDtypeStruct((count, chans), BF16),
            jax.ShapeDtypeStruct((count, chans), F32),
            jax.ShapeDtypeStruct((count, chans), F32),
            jax.ShapeDtypeStruct((8, chans), F32),
        ),
        in_specs=[
            wide,
            wide,
            wide,
            pl.BlockSpec((1, count, block), lambda i: (0, 0, i)),
            pl.BlockSpec((1, block), lambda i: (0, i)),
            pl.BlockSpec((count + 16, 128), lambda i: (0, 0)),
        ],
        out_specs=(wide, wide, wide, row8),
    )(gm, gate_pre, hidden, pre, soft, ids)


def rec_back_second_body(
    core, beyond, local, arriving, hidden, entering, pre, conv, chan, soft, gates, ids, ext,
    mine, theirs, grad_values, edge, chan_grad,
):
    count, block = local.shape
    row = lax.broadcasted_iota(jnp.int32, (count, block), 0)
    state = local[...] + beyond[...] * arriving[0:1]
    earlier = jnp.where(row >= 1, pltpu.roll(hidden[...], 1, 0), entering[0:1])
    low = conv[...].astype(F32)
    keep_rate = jax.nn.sigmoid(pre[0])
    log_decay = -8.0 * keep_rate * soft[...]
    decay = jnp.exp(log_decay)
    size = jnp.sqrt(minus_expm1(2.0 * log_decay))
    gate = jax.nn.sigmoid(pre[1])
    grad_decay = state * earlier * same_rows(ids[...], 1)
    grad_log = grad_decay * decay - state * gate * low * (decay * decay / size)
    grad_rate = grad_log * (-8.0 * soft[...]) * keep_rate * (1.0 - keep_rate)
    grad_gate = state * size * low * gate * (1.0 - gate)
    rate_low = grad_rate.astype(BF16)
    gate_low_part = grad_gate.astype(BF16)
    swap = core[0] == 0
    mine[...] = jnp.where(swap, rate_low, gate_low_part)
    theirs[...] = jnp.where(swap, gate_low_part, rate_low)
    weights = gates[0]
    over = (((1,), (1,)), ((), ()))
    grad_conv = (
        state * size * gate
        + lax.dot_general(rate_low, weights[:, :block], over, preferred_element_type=F32)
        + lax.dot_general(gate_low_part, weights[:, block:], over, preferred_element_type=F32)
    )
    wide = ext[...].astype(F32)
    total = chan[0:1] * grad_conv
    chan_grad[0:1] = jnp.sum(grad_conv * wide[16:], axis=0, keepdims=True)
    row8 = lax.broadcasted_iota(jnp.int32, (8, block), 0)
    over_edge = jnp.zeros((8, block), F32)
    for k in range(1, 4):
        masked = grad_conv * same_rows(ids[...], k)
        chan_grad[k : k + 1] = jnp.sum(masked * pltpu.roll(wide, k, 0)[16:], axis=0, keepdims=True)
        back = chan[k : k + 1] * masked
        total = total + shifted(back, -k, row, 0.0)
        first = back[0:8]
        if k < 3:
            first = pltpu.roll(first, 3 - k, 0)
        over_edge = over_edge + jnp.where((row8 >= 3 - k) & (row8 < 3), first, 0.0)
    grad_values[...] = total
    edge[...] = over_edge
    chan_grad[4:5] = jnp.sum(grad_conv, axis=0, keepdims=True)
    chan_grad[5:6] = jnp.sum(grad_rate, axis=0, keepdims=True)
    chan_grad[6:7] = jnp.sum(grad_gate, axis=0, keepdims=True)
    chan_grad[7:8] = jnp.sum(grad_log * keep_rate, axis=0, keepdims=True) * (
        -8.0 * jax.nn.sigmoid(chan[7:8])
    )


def rec_back_second(core, beyond, local, arriving, hidden, entering, pre, conv, chan, soft, gates, ids, ext):
    count, chans = local.shape
    blocks, block = gates.shape[:2]
    wide = pl.BlockSpec((count, block), lambda i, core: (0, i))
    row8 = pl.BlockSpec((8, block), lambda i, core: (0, i))
    pair = pl.BlockSpec((2, count, block), lambda i, core: (0, 0, i))
    low = jax.ShapeDtypeStruct((count, chans), BF16)
    return pl.pallas_call(
        rec_back_second_body,
        name="rec_back_second",
        grid_spec=pltpu.PrefetchScalarGridSpec(
            num_scalar_prefetch=1,
            grid=(blocks,),
            in_specs=[
                wide,
                wide,
                row8,
                wide,
                row8,
                pair,
                wide,
                row8,
                pl.BlockSpec((1, block), lambda i, core: (0, i)),
                pl.BlockSpec((1, block, 2 * block), lambda i, core: (i, 0, 0)),
                pl.BlockSpec((count + 16, 128), lambda i, core: (0, 0)),
                pl.BlockSpec((count + 16, block), lambda i, core: (0, i)),
            ],
            out_specs=(wide, wide, wide, row8, row8),
        ),
        out_shape=(
            low,
            low,
            jax.ShapeDtypeStruct((count, chans), F32),
            jax.ShapeDtypeStruct((8, chans), F32),
            jax.ShapeDtypeStruct((8, chans), F32),
        ),
    )(core, beyond, local, arriving, hidden, entering, pre, conv, chan, soft, gates, ids, ext)


def from_behind(array, axis, by):
    devices = lax.axis_size(axis)
    pairs = [(i, i + by) for i in range(devices) if 0 <= i + by < devices]
    return lax.ppermute(array, axis, pairs)


def swapped(array):
    return lax.ppermute(array, "section", SWAP)


def attend(query_rows, key_rows, allowed):
    head_dim = query_rows.shape[2]
    scores = jnp.einsum(
        "qhd,kd->hqk", query_rows, key_rows[:, :head_dim], preferred_element_type=F32
    ) * head_dim ** (-0.5)
    masked = jnp.where(allowed[None], scores, -1e30)
    row_max = jnp.max(masked, axis=-1, keepdims=True)
    lifted = jnp.exp(masked - row_max)
    row_total = jnp.sum(lifted, axis=-1, keepdims=True)
    weights = (lifted / row_total).astype(BF16)
    attended = jnp.einsum(
        "hqk,kd->qhd", weights, key_rows[:, head_dim:], preferred_element_type=F32
    ).astype(BF16)
    return (attended, row_max[:, :, 0] + jnp.log(row_total[:, :, 0]))


def attend_back(query_rows, key_rows, allowed, log_total, grad_rows):
    head_dim = query_rows.shape[2]
    factor = head_dim ** (-0.5)
    scores = (
        jnp.einsum("qhd,kd->hqk", query_rows, key_rows[:, :head_dim], preferred_element_type=F32)
        * factor
    )
    probs = jnp.exp(jnp.where(allowed[None], scores, -1e30) - log_total[:, :, None])
    weights = probs.astype(BF16)
    grad_probs = jnp.einsum(
        "qhd,kd->hqk", grad_rows, key_rows[:, head_dim:], preferred_element_type=F32
    )
    grad_values = jnp.einsum("hqk,qhd->kd", weights, grad_rows, preferred_element_type=F32)
    grad_scores = (
        probs * (grad_probs - jnp.sum(grad_probs * probs, axis=-1, keepdims=True))
    ).astype(BF16)
    grad_query = (
        jnp.einsum("hqk,kd->qhd", grad_scores, key_rows[:, :head_dim], preferred_element_type=F32)
        * factor
    )
    grad_keys = (
        jnp.einsum("hqk,qhd->kd", grad_scores, query_rows, preferred_element_type=F32) * factor
    )
    return (grad_query, jnp.concatenate([grad_keys, grad_values], axis=-1))


def seq_scatter(grad):
    return lax.psum_scatter(grad, "seq", scatter_dimension=0, tiled=True)


def columns(array, start, size):
    return lax.dynamic_slice_in_dim(array, start, size, axis=1)


def on_device(
    inputs,
    segments,
    norms,
    rec_in,
    rec_gates,
    rec_chan,
    rec_out,
    attn_q,
    attn_kv,
    attn_out,
    mlp_in,
    mlp_out,
    cotangent,
):
    core = lax.axis_index("section")
    first = core == 0
    place = lax.axis_index("seq")
    rank = lax.axis_index("head")
    heads = lax.axis_size("head")
    blocks_seq = lax.axis_size("seq")
    _, count, width = inputs.shape
    rows = count // heads
    chans = rec_in.shape[2]
    blocks, block = rec_gates.shape[:2]

    def pick(array, index):
        return lax.dynamic_index_in_dim(array, index, 0, keepdims=False)

    def own_rows(array):
        return lax.dynamic_slice_in_dim(array, rank * rows, rows, axis=0)

    core_ref = core[None].astype(jnp.int32)
    ids = pick(segments, core)
    stream_low = pick(inputs, core)
    top_low = pick(cotangent, core)
    before = from_behind(stream_low[-16:], "seq", 1)
    reach = min(max(1, WINDOW // count), blocks_seq - 1)
    earlier_ids = [from_behind(ids, "seq", distance) for distance in range(reach, 0, -1)]

    own_in = jnp.swapaxes(mlp_in[0], 0, 1)
    other_in, other_out, other_norms = swapped(own_in), swapped(mlp_out[0]), swapped(norms[0])
    gains = [
        jnp.where(first, norms[0], other_norms),
        jnp.where(first, other_norms, norms[0]),
    ]
    gain = [[gains[l][k][None] for k in range(2)] for l in range(2)]
    weights = (own_in, other_in, mlp_out[0], other_out)
    rec_in_wide = jnp.swapaxes(rec_in, 0, 1)

    before_ids = jnp.where(place == 0, -1, earlier_ids[-1][-16:])
    ext_ids = jnp.broadcast_to(jnp.concatenate([before_ids, ids])[:, None], (count + 16, 128))
    soft = jax.nn.softplus(rec_chan[7:8])
    gates_flat = rec_gates.reshape(blocks, block, 2 * block)
    normed_one, gate_pre, ext, conv_low, pre, through, local, edge = rec_forward(
        jnp.concatenate([before, stream_low]),
        gain[0][0],
        rec_in_wide,
        ext_ids,
        rec_chan,
        soft,
        gates_flat,
    )
    entering = carry(edge, False, 0)
    hidden_state, mixed, part = rec_finish(local, through, entering, gate_pre, rec_out)
    stream_rows = own_rows(stream_low).astype(F32)
    res_one, normed_a = join_forward("keep", part, stream_rows, gain[0][1], 1)

    gate_up_a, hidden_a, part = mlp_forward(0, core_ref, normed_a, *weights)
    passed, normed_two, all_keys = join_keys(part, res_one, gain[1][0], attn_kv, reach, 2)

    head_dim = attn_kv.shape[1] // 2
    heads_here = attn_q.shape[1] // head_dim
    queries = dot(normed_two, attn_q, (1, 0), BF16).reshape(count, heads_here, head_dim)
    key_ids = jnp.concatenate(earlier_ids + [ids])
    key_spots = (place - reach) * count + jnp.arange((reach + 1) * count, dtype=jnp.int32)
    query_spots = place * count + jnp.arange(count, dtype=jnp.int32)
    distance_q = query_spots[:, None] - key_spots[None, :]
    inside = (distance_q >= 0) & (distance_q < WINDOW) & (key_spots >= 0)[None, :]
    allowed = inside & (ids[:, None] == key_ids[None, :])
    attended, log_totals = attend(queries, all_keys, allowed)
    attended = attended.reshape(count, heads_here * head_dim)
    part = dot(attended, attn_out, (1, 0), BF16)
    res_two, normed_b = join_forward("keep", part, passed, gain[1][1], 3)

    hidden_b, mine_b, theirs_b, part_last, part = mlp_both(
        1, core_ref, normed_b, top_low, *weights
    )

    units = hidden_b.shape[1]
    window = (units // 2 + 127) // 128 * 128

    def mlp_term(mine, theirs, normed, hidden, out_low, out_other):
        return [
            (normed, swapped(normed), mine, swapped(theirs), units),
            (out_low, out_other, hidden, swapped(hidden), window),
        ]

    terms = mlp_term(mine_b, theirs_b, normed_b, hidden_b, top_low, pick(cotangent, 1 - core))
    part, sum_b = lax.optimization_barrier((part, weight_grad("b", core_ref, terms, False)))
    sum_b = seq_scatter(sum_b)
    grad_res_two, gain_b, low_two = join_backward(
        part, res_two, gain[1][1], own_rows(top_low).astype(F32), 5
    )

    grad_att = dot(low_two, attn_out, (1, 1), BF16)
    grad_query, grad_kv = attend_back(
        queries, all_keys, allowed, log_totals, grad_att.reshape(count, heads_here, head_dim)
    )
    query_low = grad_query.reshape(count, heads_here * head_dim).astype(BF16)
    part = dot(query_low, attn_q, (1, 1), BF16)
    grad_passed, gain_two, low_passed, kv_low = join_keys_back(
        part,
        passed,
        gain[1][0],
        grad_res_two,
        grad_kv.astype(BF16).reshape(reach + 1, count, 2 * head_dim),
        attn_kv,
        6,
    )

    mine_a, theirs_a, part = mlp_backward(0, core_ref, low_passed, gate_up_a, *weights)
    normed_two_other = swapped(normed_two)
    width_q, width_kv = query_low.shape[1], kv_low.shape[1]
    attn_sum = weight_grad(
        "attention",
        core_ref,
        [
            (normed_two, normed_two_other, query_low, swapped(query_low), width_q),
            (normed_two, normed_two_other, kv_low, swapped(kv_low), width_kv),
            (low_two, swapped(low_two), attended, swapped(attended), width_q),
        ],
        True,
    )
    terms = mlp_term(mine_a, theirs_a, normed_a, hidden_a, low_passed, swapped(low_passed))
    part, sum_a, attn_sum = lax.optimization_barrier(
        (part, weight_grad("a", core_ref, terms, False), attn_sum)
    )
    attn_sum = seq_scatter(attn_sum)
    sum_a = seq_scatter(sum_a)
    grad_res_one, gain_a, mix_low = join_backward(part, res_one, gain[0][1], grad_passed, 7)

    grad_mixed = dot(mix_low, rec_out, (1, 1))
    grad_branch, beyond, local_grad, edge = rec_back_first(
        grad_mixed, gate_pre, hidden_state, pre, soft, ext_ids, block
    )
    arriving = carry(edge, True, 9)
    gate_mine, gate_theirs, grad_values, over_edge, chan_grad = rec_back_second(
        core_ref, beyond, local_grad, arriving, hidden_state, entering, pre, conv_low, rec_chan,
        soft, gates_flat, ext_ids, ext,
    )
    from_next = from_behind(over_edge[:3], "seq", -1)
    grad_values = jnp.concatenate([grad_values[:-3], grad_values[-3:] + from_next]).astype(BF16)
    part = (
        dot(grad_values, rec_in_wide[0], (1, 1)) + dot(grad_branch, rec_in_wide[1], (1, 1))
    ).astype(BF16)
    normed_one_other = swapped(normed_one)
    rec_sum = weight_grad(
        "recurrent",
        core_ref,
        [
            (normed_one, normed_one_other, grad_values, swapped(grad_values), chans),
            (normed_one, normed_one_other, grad_branch, swapped(grad_branch), chans),
            (mix_low, swapped(mix_low), mixed, swapped(mixed), chans),
        ],
        True,
    )
    part, rec_sum = lax.optimization_barrier((part, rec_sum))
    rec_sum = seq_scatter(rec_sum)
    _, gain_one, grad_inputs = join_backward(part, stream_rows, gain[0][0], grad_res_one, 8)
    part_last, grad_inputs, gain_one = lax.optimization_barrier((part_last, grad_inputs, gain_one))
    _, final = join_forward("last", part_last, res_two, gain[1][1], 4)

    def gate_grad(left, right):
        return jnp.einsum(
            "tnb,tnc->bnc",
            left.reshape(count, blocks, block),
            right.reshape(count, blocks, block),
            preferred_element_type=F32,
        )

    gate_sum = gate_grad(conv_low, gate_mine) + gate_grad(swapped(conv_low), swapped(gate_theirs))
    share = block // (2 * blocks_seq)
    gate_sum = jnp.swapaxes(
        gate_sum.astype(BF16).reshape(2, blocks_seq, share, chans), 0, 1
    ).reshape(blocks_seq, 2 * share, chans)
    gain_rows = jnp.concatenate([gain_one, gain_a, gain_two, gain_b], axis=0)
    gain_total, chan_total, gate_sum = totals(gain_rows, chan_grad, gate_sum, 11)
    gate_sum = gate_sum.reshape(2, share, chans)
    share_norm = width // blocks_seq
    grad_norms = lax.dynamic_slice_in_dim(
        pick(gain_total.reshape(2, 2, width), core), place * share_norm, share_norm, axis=1
    )
    grad_chan = jnp.where(first, chan_total[:4], chan_total[4:])

    chans_q = attn_q.shape[1]
    attn_sum = attn_sum.astype(F32)
    grad_q = attn_sum[:, :chans_q]
    grad_kv_out = attn_sum[:, chans_q : chans_q + 2 * head_dim]
    grad_attn_out = attn_sum[:, chans_q + 2 * head_dim :].T
    rec_sum = rec_sum.astype(F32)
    grad_in = rec_sum[:, : 2 * chans].reshape(-1, 2, chans)
    grad_rec_out = rec_sum[:, 2 * chans :].T
    own_gate = pick(gate_sum, core)
    other_gate = swapped(pick(gate_sum, 1 - core))
    grad_gates = jnp.transpose(
        jnp.stack([jnp.where(first, own_gate, other_gate), jnp.where(first, other_gate, own_gate)])
        .astype(F32)
        .reshape(2, share, blocks, block),
        (2, 1, 0, 3),
    )
    own_part = jnp.where(first, sum_a, sum_b)
    other_part = swapped(jnp.where(first, sum_b, sum_a))
    lower = jnp.where(first, own_part, other_part).astype(F32)
    upper = jnp.where(first, other_part, own_part).astype(F32)
    grad_mlp_in = jnp.stack([lower[:, :units], upper[:, :units]], axis=1)
    grad_mlp_out = jnp.concatenate(
        [lower[:, units:].T, upper[:, 2 * window :].T], axis=0
    )

    return (
        final[None],
        grad_inputs.astype(F32)[None],
        grad_norms[None],
        grad_in,
        grad_gates,
        grad_chan,
        grad_rec_out,
        grad_q,
        grad_kv_out,
        grad_attn_out,
        grad_mlp_in[None],
        grad_mlp_out[None],
    )


def solution(mesh):
    in_specs = (
        P(None, "seq", None),
        P(None, "seq"),
        P("section", None, None),
        P(None, None, "head"),
        P("head", None, None, None),
        P(None, "head"),
        P("head", None),
        P(None, "head"),
        P(),
        P("head", None),
        P("section", None, None, "head"),
        P("section", "head", None),
        P(None, "seq", None),
    )
    out_specs = (
        P("section", "seq", None),
        P("section", "seq", None),
        P("section", None, "seq"),
        P(("section", "seq"), None, "head"),
        P("head", ("section", "seq"), None, None),
        P("section", "head"),
        P("head", ("section", "seq")),
        P(("section", "seq"), "head"),
        P(("section", "seq"), None),
        P("head", ("section", "seq")),
        P("section", "seq", None, "head"),
        P("section", "head", "seq"),
    )
    return jax.shard_map(
        on_device, mesh=mesh, in_specs=in_specs, out_specs=out_specs, check_vma=False
    )
```

```python
import functools

import jax
import jax.numpy as jnp
from jax import lax
from jax.experimental import pallas as pl
from jax.experimental.pallas import tpu as pltpu
from jax.sharding import PartitionSpec as P

WINDOW = 1024
EPSILON = 1e-06
MESH = pl.DeviceIdType.MESH
F32 = jnp.float32
BF16 = jnp.bfloat16
SWAP = [(0, 1), (1, 0)]


def dot(a, b, dims, out=F32):
    return lax.dot_general(a, b, ((dims[:1], dims[1:]), ((), ())), preferred_element_type=F32).astype(
        out
    )


def vmem():
    return pl.BlockSpec(memory_space=pltpu.VMEM)


def meet(axis, me, n):
    barrier = pltpu.get_barrier_semaphore()
    for k in range(1, n):
        peer = lax.rem(me + k, n)
        pl.semaphore_signal(barrier, inc=1, device_id={axis: peer}, device_id_type=MESH)
    pl.semaphore_wait(barrier, n - 1)


def remote(src, dst, send, recv, axis, peer):
    return pltpu.make_async_remote_copy(
        src_ref=src,
        dst_ref=dst,
        send_sem=send,
        recv_sem=recv,
        device_id={axis: peer},
        device_id_type=MESH,
    )


def scatter_start(n, me, rows, part, recv, send_sem, recv_sem):
    copies = []
    for k in range(1, n):
        peer = lax.rem(me + k, n)
        start = pl.multiple_of(peer * rows, rows)
        copies.append(
            remote(
                part.at[pl.ds(start, rows)],
                recv.at[k - 1],
                send_sem.at[k - 1],
                recv_sem.at[k - 1],
                "head",
                peer,
            )
        )
    for copy in copies:
        copy.start()
    return copies


def scatter_sum(me, rows, part, recv, copies):
    total = part[pl.ds(pl.multiple_of(me * rows, rows), rows)].astype(F32)
    for k, copy in enumerate(copies):
        copy.wait_recv()
        total = total + recv[k].astype(F32)
    return total


def drain(copies):
    for copy in copies:
        copy.wait_send()


def spread(n, me, rows, value, full, send_sem, recv_sem):
    mine = pl.ds(pl.multiple_of(me * rows, rows), rows)
    full[mine] = value
    copies = []
    for k in range(1, n):
        peer = lax.rem(me + k, n)
        copies.append(
            remote(
                full.at[mine], full.at[mine], send_sem.at[k - 1], recv_sem.at[k - 1], "head", peer
            )
        )
    for copy in copies:
        copy.start()
    return copies


def finish(copies):
    for copy in copies:
        copy.wait()


def forward_body(n, kind, part, base, gain, new, full, recv, s1, r1, s2, r2):
    me = lax.axis_index("head")
    rows = base.shape[0]
    meet("head", me, n)
    sent = scatter_start(n, me, rows, part, recv, s1, r1)
    fresh = base[...] + scatter_sum(me, rows, part, recv, sent)
    new[...] = fresh
    out = fresh
    if kind != "last":
        out = fresh * lax.rsqrt(jnp.mean(fresh * fresh, axis=-1, keepdims=True) + EPSILON)
        out = out * gain[...]
    finish(spread(n, me, rows, out.astype(BF16), full, s2, r2))
    drain(sent)


def forward_mlp_body(n, part, base, gain, own_in, own_out, other_in, other_out, *refs):
    new, full, gate_up, hidden, part_next, recv, s1, r1, s2, r2, acc, b_in, b_out, sems = refs
    own, other = (own_in, own_out), (other_in, other_out)
    fetch_weights(0, own, other, (b_in, b_out), sems)
    forward_body(n, "keep", part, base, gain, new, full, recv, s1, r1, s2, r2)
    wait_weights(own, (b_in, b_out), sems)
    mlp_forward_part(full, (b_in, b_out), gate_up, hidden, part_next, acc)


def forward_both_body(n, part, base, gain, low, own_in, own_out, other_in, other_out, *refs):
    new, full, hidden, mine, theirs, part_last, part_back = refs[:7]
    recv, s1, r1, s2, r2, acc, acc_back, b_in, b_out, sems = refs[7:]
    own, other = (own_in, own_out), (other_in, other_out)
    fetch_weights(1, own, other, (b_in, b_out), sems)
    forward_body(n, "keep", part, base, gain, new, full, recv, s1, r1, s2, r2)
    wait_weights(own, (b_in, b_out), sems)
    mlp_both_part(
        full, low, (b_in, b_out), hidden, mine, theirs, part_last, part_back, acc, acc_back
    )


def meet_around(n, me, blocks, place, pairs):
    barrier = pltpu.get_barrier_semaphore()
    for d, k in pairs:
        device = {
            "seq": lax.rem(place - d + blocks, blocks),
            "head": lax.rem(me - k + n, n),
        }
        pl.semaphore_signal(barrier, inc=1, device_id=device, device_id_type=MESH)
    pl.semaphore_wait(barrier, len(pairs))


def keys_body(n, blocks, reach, part, base, gain, w_kv, new, full, keys, recv, s1, r1, s2, r2, own, s3, r3):
    me, place = lax.axis_index("head"), lax.axis_index("seq")
    rows = base.shape[0]
    count = part.shape[0]
    pairs = [(d, k) for d in range(reach + 1) for k in range(n) if (d, k) != (0, 0)]
    meet_around(n, me, blocks, place, pairs)
    sent = scatter_start(n, me, rows, part, recv, s1, r1)
    fresh = base[...] + scatter_sum(me, rows, part, recv, sent)
    fresh = fresh.astype(BF16).astype(F32)
    new[...] = fresh
    out = fresh * lax.rsqrt(jnp.mean(fresh * fresh, axis=-1, keepdims=True) + EPSILON)
    low = (out * gain[...]).astype(BF16)
    value = jnp.dot(low, w_kv[...], preferred_element_type=F32).astype(BF16)
    own[...] = value
    mine = pl.multiple_of(me * rows, rows)
    keys[pl.ds(reach * count + mine, rows)] = value
    copies = []
    for d, k in pairs:
        copies.append(
            pltpu.make_async_remote_copy(
                src_ref=own,
                dst_ref=keys.at[pl.ds((reach - d) * count + mine, rows)],
                send_sem=s3.at[d * n + k],
                recv_sem=r3.at[d * n + k],
                device_id={
                    "seq": lax.rem(place + d, blocks),
                    "head": lax.rem(me + k, n),
                },
                device_id_type=MESH,
            )
        )
    for copy in copies:
        copy.start()
    finish(spread(n, me, rows, low, full, s2, r2))
    finish(copies)
    drain(sent)


def norm_back_rows(grad, v, gain, up):
    scale = lax.rsqrt(jnp.mean(v * v, axis=-1, keepdims=True) + EPSILON)
    gain_grad = jnp.sum(grad * v * scale, axis=0, keepdims=True)
    inner = grad * gain
    out = up + scale * inner - v * (
        scale * scale * scale * jnp.mean(inner * v, axis=-1, keepdims=True)
    )
    return out, gain_grad


def backward_body(n, part, base, gain, up, res, gain_grad, full, recv, s1, r1, s2, r2):
    me = lax.axis_index("head")
    rows = base.shape[0]
    meet("head", me, n)
    sent = scatter_start(n, me, rows, part, recv, s1, r1)
    grad = scatter_sum(me, rows, part, recv, sent)
    out, gain_grad[...] = norm_back_rows(grad, base[...], gain[...], up[...])
    res[...] = out
    finish(spread(n, me, rows, out.astype(BF16), full, s2, r2))
    drain(sent)


def keys_back_body(
    n, blocks, reach, part, base, gain, up, grad_kv, w_kv, gate_up, own_in, own_out, other_in, other_out,
    res, gain_grad, full, kv_full, mine_out, theirs_out, part_next,
    recv, s1, r1, s2, r2, recv_kv, s3, r3, send_z, recv_z, s4, r4, s5, r5, acc, b_in, b_out, sems,
):
    own, other = (own_in, own_out), (other_in, other_out)
    fetch_weights(0, own, other, (b_in, b_out), sems)
    me, place = lax.axis_index("head"), lax.axis_index("seq")
    rows = base.shape[0]
    meet_around(
        n,
        me,
        blocks,
        place,
        [(0, k) for k in range(1, n)] + [(-d, 0) for d in range(1, reach + 1)],
    )
    mine = pl.ds(pl.multiple_of(me * rows, rows), rows)
    kv_sent = []
    for k in range(1, n):
        peer = lax.rem(me + k, n)
        there = pl.ds(pl.multiple_of(peer * rows, rows), rows)
        kv_sent.append(
            remote(
                grad_kv.at[:, there], recv_kv.at[k - 1], s3.at[k - 1], r3.at[k - 1], "head", peer
            )
        )
    for copy in kv_sent:
        copy.start()
    sent = scatter_start(n, me, rows, part, recv, s1, r1)
    total = grad_kv[:, mine].astype(F32)
    for k, copy in enumerate(kv_sent):
        copy.wait_recv()
        total = total + recv_kv[k].astype(F32)
    send_z[...] = total.astype(BF16)
    z_sent = []
    for d in range(1, reach + 1):
        z_sent.append(
            remote(
                send_z.at[reach - d],
                recv_z.at[d - 1],
                s4.at[d - 1],
                r4.at[d - 1],
                "seq",
                lax.rem(place - d + blocks, blocks),
            )
        )
    for copy in z_sent:
        copy.start()
    grad = scatter_sum(me, rows, part, recv, sent)
    own_kv = total[reach]
    for d, copy in enumerate(z_sent):
        copy.wait_recv()
        own_kv = own_kv + recv_z[d].astype(F32)
    kv_low = own_kv.astype(BF16)
    kv_spread = spread(n, me, rows, kv_low, kv_full, s5, r5)
    grad = grad + lax.dot_general(
        kv_low, w_kv[...], (((1,), (1,)), ((), ())), preferred_element_type=F32
    )
    out, gain_grad[...] = norm_back_rows(grad, base[...], gain[...], up[...])
    low = out.astype(BF16)
    res[...] = low.astype(F32)
    finish(spread(n, me, rows, low, full, s2, r2))
    finish(kv_spread)
    drain(sent + kv_sent + z_sent)
    wait_weights(own, (b_in, b_out), sems)
    mlp_backward_part(full, gate_up, (b_in, b_out), mine_out, theirs_out, part_next, acc)


def boundary_scratch(n, rows, width):
    return [pltpu.VMEM((n - 1, rows, width), BF16)] + [pltpu.SemaphoreType.DMA((n - 1,))] * 4


def join_forward(kind, part, base, gain, ident):
    n = lax.axis_size("head")
    count, width = part.shape
    rows = base.shape[0]
    return pl.pallas_call(
        functools.partial(forward_body, n, kind),
        out_shape=(
            jax.ShapeDtypeStruct((rows, width), F32),
            jax.ShapeDtypeStruct((count, width), BF16),
        ),
        in_specs=[vmem()] * 3,
        out_specs=(vmem(), vmem()),
        scratch_shapes=boundary_scratch(n, rows, width),
        compiler_params=pltpu.CompilerParams(collective_id=ident, has_side_effects=True),
    )(part, base, gain)


def join_mlp(part, base, gain, weights, ident, low=None):
    n = lax.axis_size("head")
    count, width = part.shape
    rows = base.shape[0]
    units = weights[1].shape[0]
    whole = jax.ShapeDtypeStruct((count, width), BF16)
    narrow = jax.ShapeDtypeStruct((count, units), BF16)
    outs = [jax.ShapeDtypeStruct((rows, width), F32), whole]
    if low is None:
        body, operands = forward_mlp_body, [part, base, gain]
        outs += [jax.ShapeDtypeStruct((TILES, count, 2 * units // TILES), F32), narrow, whole]
    else:
        body, operands = forward_both_body, [part, base, gain, low]
        outs += [narrow, narrow, narrow, whole, whole]
    return pl.pallas_call(
        functools.partial(body, n),
        out_shape=tuple(outs),
        in_specs=[vmem()] * len(operands) + [pl.BlockSpec(memory_space=pl.ANY)] * 4,
        out_specs=tuple(vmem() for _ in outs),
        scratch_shapes=boundary_scratch(n, rows, width)
        + mlp_scratch(count, width, units, 1 if low is None else 2),
        compiler_params=pltpu.CompilerParams(collective_id=ident, has_side_effects=True),
    )(*operands, *weights)


def join_keys(part, base, gain, w_kv, reach, ident):
    n, blocks = lax.axis_size("head"), lax.axis_size("seq")
    count, width = part.shape
    rows = base.shape[0]
    both = w_kv.shape[1]
    slots = (reach + 1) * n
    return pl.pallas_call(
        functools.partial(keys_body, n, blocks, reach),
        name="join_keys",
        out_shape=(
            jax.ShapeDtypeStruct((rows, width), F32),
            jax.ShapeDtypeStruct((count, width), BF16),
            jax.ShapeDtypeStruct(((reach + 1) * count, both), BF16),
        ),
        in_specs=[vmem()] * 4,
        out_specs=(vmem(), vmem(), vmem()),
        scratch_shapes=boundary_scratch(n, rows, width)
        + [
            pltpu.VMEM((rows, both), BF16),
            pltpu.SemaphoreType.DMA((slots,)),
            pltpu.SemaphoreType.DMA((slots,)),
        ],
        compiler_params=pltpu.CompilerParams(collective_id=ident, has_side_effects=True),
    )(part, base, gain, w_kv)


def join_backward(part, base, gain, up, ident):
    n = lax.axis_size("head")
    count, width = part.shape
    rows = base.shape[0]
    return pl.pallas_call(
        functools.partial(backward_body, n),
        out_shape=(
            jax.ShapeDtypeStruct((rows, width), F32),
            jax.ShapeDtypeStruct((1, width), F32),
            jax.ShapeDtypeStruct((count, width), BF16),
        ),
        in_specs=[vmem()] * 4,
        out_specs=(vmem(), vmem(), vmem()),
        scratch_shapes=boundary_scratch(n, rows, width),
        compiler_params=pltpu.CompilerParams(collective_id=ident, has_side_effects=True),
    )(part, base, gain, up)


def join_keys_back(part, base, gain, up, grad_kv, w_kv, gate_up, weights, ident):
    n, blocks = lax.axis_size("head"), lax.axis_size("seq")
    count, width = part.shape
    rows = base.shape[0]
    reach, both = grad_kv.shape[0] - 1, grad_kv.shape[2]
    units = weights[1].shape[0]
    dma = pltpu.SemaphoreType.DMA
    return pl.pallas_call(
        functools.partial(keys_back_body, n, blocks, reach),
        name="join_keys_back",
        out_shape=(
            jax.ShapeDtypeStruct((rows, width), F32),
            jax.ShapeDtypeStruct((1, width), F32),
            jax.ShapeDtypeStruct((count, width), BF16),
            jax.ShapeDtypeStruct((count, both), BF16),
            jax.ShapeDtypeStruct((count, units), BF16),
            jax.ShapeDtypeStruct((count, units), BF16),
            jax.ShapeDtypeStruct((count, width), BF16),
        ),
        in_specs=[vmem()] * 7 + [pl.BlockSpec(memory_space=pl.ANY)] * 4,
        out_specs=tuple([vmem()] * 7),
        scratch_shapes=boundary_scratch(n, rows, width)
        + [
            pltpu.VMEM((n - 1, reach + 1, rows, both), BF16),
            dma((n - 1,)),
            dma((n - 1,)),
            pltpu.VMEM((reach + 1, rows, both), BF16),
            pltpu.VMEM((reach, rows, both), BF16),
            dma((reach,)),
            dma((reach,)),
            dma((n - 1,)),
            dma((n - 1,)),
        ]
        + mlp_scratch(count, width, units, 1),
        compiler_params=pltpu.CompilerParams(collective_id=ident, has_side_effects=True),
    )(part, base, gain, up, grad_kv, w_kv, gate_up, *weights)


def totals_body(heads, blocks, gains, chan, gates, gain_out, chan_out, gate_out, *scratch):
    g1, g2, g3, sum_one, sum_two, c2, c3, csum, w2, sems = scratch
    head, place, core = lax.axis_index("head"), lax.axis_index("seq"), lax.axis_index("section")
    barrier = pltpu.get_barrier_semaphore()
    for axis, me, n in (("head", head, heads), ("seq", place, blocks), ("section", core, 2)):
        for k in range(1, n):
            pl.semaphore_signal(
                barrier, inc=1, device_id={axis: lax.rem(me + k, n)}, device_id_type=MESH
            )
    pl.semaphore_wait(barrier, heads + blocks - 1)
    used = 0

    def exchange(src, slots, axis, me, n, split=False):
        nonlocal used
        copies = []
        for k in range(1, n):
            peer = lax.rem(me + k, n)
            copies.append(
                remote(
                    src.at[peer] if split else src,
                    slots.at[k - 1],
                    sems.at[0, used],
                    sems.at[1, used],
                    axis,
                    peer,
                )
            )
            used += 1
        for copy in copies:
            copy.start()
        return copies

    def collect(copies, src, slots):
        total = src[...]
        for k, copy in enumerate(copies):
            copy.wait_recv()
            total = total + slots[k]
        return total

    by_head = exchange(gains, g1, "head", head, heads)
    chan_seq = exchange(chan, c2, "seq", place, blocks)
    gate_seq = exchange(gates, w2, "seq", place, blocks, True)
    sum_one[...] = collect(by_head, gains, g1)
    gain_seq = exchange(sum_one, g2, "seq", place, blocks)
    csum[...] = collect(chan_seq, chan, c2)
    chan_core = exchange(csum, c3, "section", core, 2)
    sum_two[...] = collect(gain_seq, sum_one, g2)
    gain_core = exchange(sum_two, g3, "section", core, 2)
    chan_out[...] = collect(chan_core, csum, c3)
    gain_out[...] = collect(gain_core, sum_two, g3)
    gate_total = gates[place].astype(F32)
    for k, copy in enumerate(gate_seq):
        copy.wait_recv()
        gate_total = gate_total + w2[k].astype(F32)
    gate_out[...] = gate_total.astype(BF16)
    for copy in by_head + chan_seq + gate_seq + gain_seq + chan_core + gain_core:
        copy.wait_send()


def totals(gains, chan, gates, ident):
    heads, blocks = lax.axis_size("head"), lax.axis_size("seq")
    gs, cs, ws = gains.shape, chan.shape, gates.shape[1:]
    return pl.pallas_call(
        functools.partial(totals_body, heads, blocks),
        name="totals",
        out_shape=(
            jax.ShapeDtypeStruct(gs, F32),
            jax.ShapeDtypeStruct(cs, F32),
            jax.ShapeDtypeStruct(ws, BF16),
        ),
        in_specs=[vmem(), vmem(), vmem()],
        out_specs=(vmem(), vmem(), vmem()),
        scratch_shapes=[
            pltpu.VMEM((heads - 1,) + gs, F32),
            pltpu.VMEM((blocks - 1,) + gs, F32),
            pltpu.VMEM((1,) + gs, F32),
            pltpu.VMEM(gs, F32),
            pltpu.VMEM(gs, F32),
            pltpu.VMEM((blocks - 1,) + cs, F32),
            pltpu.VMEM((1,) + cs, F32),
            pltpu.VMEM(cs, F32),
            pltpu.VMEM((blocks - 1,) + ws, BF16),
            pltpu.SemaphoreType.DMA((2, heads + 3 * blocks)),
        ],
        compiler_params=pltpu.CompilerParams(collective_id=ident, has_side_effects=True),
    )(gains, chan, gates)


OVER_LAST = (((1,), (1,)), ((), ()))
TILES = 3


def weight_copies(own, buffers, sems):
    tile = buffers[1].shape[1]
    copies = []
    for t in range(TILES):
        units = pl.ds(t * tile, tile)
        for k in range(2):
            copies.append(
                pltpu.make_async_copy(
                    own[0].at[k, :, units],
                    buffers[0].at[t, :, pl.ds(k * tile, tile)],
                    sems.at[k, t],
                )
            )
        copies.append(pltpu.make_async_copy(own[1].at[units], buffers[1].at[t], sems.at[2, t]))
    return copies


def fetch_weights(layer, own, other, buffers, sems):
    core = lax.axis_index("section")
    for near, use in ((own, core == layer), (other, core != layer)):

        @pl.when(use)
        def _(near=near):
            for copy in weight_copies(near, buffers, sems):
                copy.start()


def wait_weights(own, buffers, sems):
    for copy in weight_copies(own, buffers, sems):
        copy.wait()


def tile_columns(t, tile):
    return pl.ds(pl.multiple_of(t * tile, 128), tile)


def grad_tile(low, gate, up, w_in, w_out, mine, theirs, columns_at, acc):
    grad_hidden = lax.dot_general(low, w_out, OVER_LAST, preferred_element_type=F32)
    act, slope = gelu_parts(gate)
    grad_gate = (grad_hidden * up * slope).astype(BF16)
    grad_up = (grad_hidden * act).astype(BF16)
    swap = lax.axis_index("section") == 0
    mine[:, columns_at] = jnp.where(swap, grad_gate, grad_up)
    theirs[:, columns_at] = jnp.where(swap, grad_up, grad_gate)
    both = jnp.concatenate([grad_gate, grad_up], axis=1)
    acc[...] += lax.dot_general(both, w_in, OVER_LAST, preferred_element_type=F32)
    return act


def mlp_forward_part(x, buffers, gate_up, hidden, part, acc):
    tile = buffers[1].shape[1]
    acc[...] = jnp.zeros_like(acc)

    @pl.loop(0, TILES)
    def _(t):
        both = jnp.dot(x[...], buffers[0][t], preferred_element_type=F32)
        gate_up[t] = both
        low = (gelu_parts(both[:, :tile])[0] * both[:, tile:]).astype(BF16)
        hidden[:, tile_columns(t, tile)] = low
        acc[...] += jnp.dot(low, buffers[1][t], preferred_element_type=F32)

    part[...] = acc[...].astype(BF16)


def mlp_backward_part(low, gate_up, buffers, mine, theirs, part, acc):
    tile = buffers[1].shape[1]
    acc[...] = jnp.zeros_like(acc)

    @pl.loop(0, TILES)
    def _(t):
        grad_tile(
            low[...], gate_up[t, :, :tile], gate_up[t, :, tile:], buffers[0][t], buffers[1][t],
            mine, theirs, tile_columns(t, tile), acc,
        )

    part[...] = acc[...].astype(BF16)


def mlp_both_part(x, low, buffers, hidden, mine, theirs, part, part_back, acc, acc_back):
    tile = buffers[1].shape[1]
    acc[...] = jnp.zeros_like(acc)
    acc_back[...] = jnp.zeros_like(acc_back)

    @pl.loop(0, TILES)
    def _(t):
        both = jnp.dot(x[...], buffers[0][t], preferred_element_type=F32)
        gate, up = both[:, :tile], both[:, tile:]
        at = tile_columns(t, tile)
        act = grad_tile(low[...], gate, up, buffers[0][t], buffers[1][t], mine, theirs, at, acc_back)
        value = (act * up).astype(BF16)
        hidden[:, at] = value
        acc[...] += jnp.dot(value, buffers[1][t], preferred_element_type=F32)

    part[...] = acc[...].astype(BF16)
    part_back[...] = acc_back[...].astype(BF16)


def mlp_scratch(count, width, units, accs):
    tile = units // TILES
    return [pltpu.VMEM((count, width), F32)] * accs + [
        pltpu.VMEM((TILES, width, 2 * tile), BF16),
        pltpu.VMEM((TILES, tile, width), BF16),
        pltpu.SemaphoreType.DMA((3, TILES)),
    ]


def weight_grad_body(sizes, core, *refs):
    out = refs[-1]
    over = (((0,), (0,)), ((), ()))
    start = 0
    for t, size in enumerate(sizes):
        left, left_other, right, right_other = refs[4 * t : 4 * t + 4]
        spare = right.shape[1] - size
        if spare:
            window = pl.ds(pl.multiple_of(core[0] * spare, 128), size)
            near, far = right[:, window], right_other[:, window]
        else:
            near, far = right[...], right_other[...]
        total = lax.dot_general(left[...], near, over, preferred_element_type=F32)
        total += lax.dot_general(left_other[...], far, over, preferred_element_type=F32)
        out[:, start : start + size] = total.astype(BF16)
        start += size


def weight_grad(core, terms, half):
    count, width = terms[0][0].shape
    tile = 256
    steps = width // tile // (2 if half else 1)
    sizes = [term[4] for term in terms]
    in_specs, operands = [], []
    for left, left_other, right, right_other, _ in terms:
        if half:
            rows = pl.BlockSpec((count, tile), lambda i, core: (0, core[0] * steps + i))
        else:
            rows = pl.BlockSpec((count, tile), lambda i, core: (0, i))
        full = pl.BlockSpec(right.shape, lambda i, core: (0, 0))
        in_specs += [rows, rows, full, full]
        operands += [left, left_other, right, right_other]
    return pl.pallas_call(
        functools.partial(weight_grad_body, sizes),
        grid_spec=pltpu.PrefetchScalarGridSpec(
            num_scalar_prefetch=1,
            grid=(steps,),
            in_specs=in_specs,
            out_specs=pl.BlockSpec((tile, sum(sizes)), lambda i, core: (i, 0)),
        ),
        out_shape=jax.ShapeDtypeStruct((steps * tile, sum(sizes)), BF16),
    )(core, *operands)


def carry_body(n, reverse, edge, *refs):
    me = lax.axis_index("seq")
    if reverse:
        out, every, send_sem, recv_sem = refs
    else:
        ids, out, all_ids, every, send_sem, recv_sem, send_ids, recv_ids = refs
        all_ids[me] = ids[...]
    meet("seq", me, n)
    copies = []
    for k in range(1, n):
        peer = lax.rem(me + k, n)
        copies.append(
            remote(edge, every.at[k - 1], send_sem.at[k - 1], recv_sem.at[k - 1], "seq", peer)
        )
        if not reverse:
            copies.append(
                remote(ids, all_ids.at[me], send_ids.at[k - 1], recv_ids.at[k - 1], "seq", peer)
            )
    for copy in copies:
        copy.start()
    finish(copies)
    state = jnp.zeros((1, edge.shape[1]), F32)
    order = range(1, n) if reverse else range(n - 1, 0, -1)
    for k in order:
        sender = me - k if not reverse else me + n - k
        inside = sender >= 0 if not reverse else sender < n
        if reverse:
            inside = jnp.logical_and(inside, sender > me)
        slot = every[k - 1]
        state = jnp.where(inside, slot[0:1] * state + slot[1:2], state)
    out[...] = jnp.broadcast_to(state, out.shape)


def carry(edge, ident, ids=None):
    n = lax.axis_size("seq")
    dma = pltpu.SemaphoreType.DMA((n - 1,))
    scratch = [pltpu.VMEM((n - 1,) + edge.shape, F32), dma, dma]
    shapes = [jax.ShapeDtypeStruct(edge.shape, F32)]
    operands = [edge]
    if ids is not None:
        scratch += [dma, dma]
        shapes.append(jax.ShapeDtypeStruct((n,) + ids.shape, jnp.int32))
        operands.append(ids)
    return pl.pallas_call(
        functools.partial(carry_body, n, ids is None),
        out_shape=tuple(shapes),
        in_specs=[vmem() for _ in operands],
        out_specs=tuple(vmem() for _ in shapes),
        scratch_shapes=scratch,
        compiler_params=pltpu.CompilerParams(collective_id=ident, has_side_effects=True),
    )(*operands)


def shifted(x, by, row, fill):
    count = x.shape[0]
    if by > 0:
        return jnp.where(row >= by, pltpu.roll(x, by, 0), fill)
    return jnp.where(row < count + by, pltpu.roll(x, count + by, 0), fill)


def scan_rows(a, b, row, sign):
    step = 1
    while step < a.shape[0]:
        b = b + a * shifted(b, sign * step, row, 0.0)
        a = a * shifted(a, sign * step, row, 1.0)
        step *= 2
    return a, b


def minus_expm1(y):
    series = jnp.full_like(y, 1.0)
    for k in range(9, 1, -1):
        series = 1.0 + y * series * (1.0 / k)
    return jnp.where(y > -0.5, -y * series, 1.0 - jnp.exp(y))


def gelu_parts(x):
    c = 0.7978845608028654
    inner = c * (x + 0.044715 * x * x * x)
    t = jnp.tanh(inner)
    act = 0.5 * x * (1.0 + t)
    slope = 0.5 * (1.0 + t) + 0.5 * x * (1.0 - t * t) * c * (1.0 + 3.0 * 0.044715 * x * x)
    return act, slope


def same_rows(ids, k):
    return (pltpu.roll(ids, k, 0)[16:] == ids[16:]).astype(F32)


def rec_forward_body(
    x, gain, w_in, ids, chan, soft, gates,
    normed, gate_pre, ext, conv_out, pre_out, through, local, edge, low_x,
):
    count, block = conv_out.shape

    @pl.when(pl.program_id(0) == 0)
    def _():
        v = x[...].astype(F32)
        out = v * lax.rsqrt(jnp.mean(v * v, axis=-1, keepdims=True) + EPSILON) * gain[...]
        low = out.astype(BF16)
        low_x[...] = low
        normed[...] = low[16:]

    values = jnp.dot(low_x[...], w_in[0], preferred_element_type=F32).astype(BF16)
    gate_pre[...] = jnp.dot(low_x[16:], w_in[1], preferred_element_type=F32)
    ext[...] = values
    wide = values.astype(F32)
    total = chan[4:5] + chan[0:1] * wide[16:]
    for k in range(1, 4):
        total = total + chan[k : k + 1] * pltpu.roll(wide, k, 0)[16:] * same_rows(ids[...], k)
    low = total.astype(BF16)
    conv_out[...] = low
    pre = jnp.dot(low, gates[0], preferred_element_type=F32)
    rate = pre[:, :block] + chan[5:6]
    gate = pre[:, block:] + chan[6:7]
    pre_out[0] = rate
    pre_out[1] = gate
    log_decay = -8.0 * jax.nn.sigmoid(rate) * soft[...]
    decay = jnp.exp(log_decay) * same_rows(ids[...], 1)
    drive = jnp.sqrt(minus_expm1(2.0 * log_decay)) * jax.nn.sigmoid(gate) * low.astype(F32)
    row = lax.broadcasted_iota(jnp.int32, (count, block), 0)
    a, b = scan_rows(decay, drive, row, 1)
    through[...] = a
    local[...] = b
    edge[0:1] = a[count - 1 :]
    edge[1:2] = b[count - 1 :]
    edge[2:8] = jnp.zeros((6, block), F32)


def rec_forward(x, gain, w_in, ids, chan, soft, gates):
    count, width = x.shape[0] - 16, x.shape[1]
    chans = w_in.shape[2]
    blocks, block = gates.shape[:2]
    wide = pl.BlockSpec((count, block), lambda i: (0, i))
    row8 = pl.BlockSpec((8, block), lambda i: (0, i))
    tall = pl.BlockSpec((count + 16, block), lambda i: (0, i))
    f32 = jax.ShapeDtypeStruct((count, chans), F32)
    return pl.pallas_call(
        rec_forward_body,
        name="rec_forward",
        grid=(blocks,),
        out_shape=(
            jax.ShapeDtypeStruct((count, width), BF16),
            f32,
            jax.ShapeDtypeStruct((count + 16, chans), BF16),
            jax.ShapeDtypeStruct((count, chans), BF16),
            jax.ShapeDtypeStruct((2, count, chans), F32),
            f32,
            f32,
            jax.ShapeDtypeStruct((8, chans), F32),
        ),
        in_specs=[
            pl.BlockSpec((count + 16, width), lambda i: (0, 0)),
            pl.BlockSpec((1, width), lambda i: (0, 0)),
            pl.BlockSpec((2, width, block), lambda i: (0, 0, i)),
            pl.BlockSpec((count + 16, 128), lambda i: (0, 0)),
            row8,
            pl.BlockSpec((1, block), lambda i: (0, i)),
            pl.BlockSpec((1, block, 2 * block), lambda i: (i, 0, 0)),
        ],
        out_specs=(
            pl.BlockSpec((count, width), lambda i: (0, 0)),
            wide,
            tall,
            wide,
            pl.BlockSpec((2, count, block), lambda i: (0, 0, i)),
            wide,
            wide,
            row8,
        ),
        scratch_shapes=[pltpu.VMEM((count + 16, width), BF16)],
    )(x, gain, w_in, ids, chan, soft, gates)


def rec_finish_body(steps, local, through, entering, gate_pre, w_out, hidden, mixed, part, acc):
    step = pl.program_id(0)

    @pl.when(step == 0)
    def _():
        acc[...] = jnp.zeros_like(acc)

    state = local[...] + through[...] * entering[0:1]
    hidden[...] = state
    low = (state * gelu_parts(gate_pre[...])[0]).astype(BF16)
    mixed[...] = low
    acc[...] += jnp.dot(low, w_out[...], preferred_element_type=F32)

    @pl.when(step == steps - 1)
    def _():
        part[...] = acc[...].astype(BF16)


def rec_finish(local, through, entering, gate_pre, w_out):
    count, chans = local.shape
    width = w_out.shape[1]
    tile = chans // 2
    wide = pl.BlockSpec((count, tile), lambda i: (0, i))
    return pl.pallas_call(
        functools.partial(rec_finish_body, 2),
        name="rec_finish",
        grid=(2,),
        out_shape=(
            jax.ShapeDtypeStruct((count, chans), F32),
            jax.ShapeDtypeStruct((count, chans), BF16),
            jax.ShapeDtypeStruct((count, width), BF16),
        ),
        in_specs=[
            wide,
            wide,
            pl.BlockSpec((8, tile), lambda i: (0, i)),
            wide,
            pl.BlockSpec((tile, width), lambda i: (i, 0)),
        ],
        out_specs=(wide, wide, pl.BlockSpec((count, width), lambda i: (0, 0))),
        scratch_shapes=[pltpu.VMEM((count, width), F32)],
    )(local, through, entering, gate_pre, w_out)


def rec_back_first_body(gm, gate_pre, hidden, rate, soft, ids, grad_gate, beyond, local, edge):
    count, block = gm.shape
    act, slope = gelu_parts(gate_pre[...])
    up = gm[...]
    grad_gate[...] = (up * hidden[...] * slope).astype(BF16)
    decay = jnp.exp(-8.0 * jax.nn.sigmoid(rate[0]) * soft[...]) * same_rows(ids[...], 1)
    row = lax.broadcasted_iota(jnp.int32, (count, block), 0)
    a, b = scan_rows(shifted(decay, -1, row, 1.0), up * act, row, -1)
    beyond[...] = a
    local[...] = b
    edge[0:1] = decay[0:1] * a[0:1]
    edge[1:2] = decay[0:1] * b[0:1]
    edge[2:8] = jnp.zeros((6, block), F32)


def rec_back_first(gm, gate_pre, hidden, pre, soft, ids, block):
    count, chans = gm.shape
    wide = pl.BlockSpec((count, block), lambda i: (0, i))
    row8 = pl.BlockSpec((8, block), lambda i: (0, i))
    return pl.pallas_call(
        rec_back_first_body,
        name="rec_back_first",
        grid=(chans // block,),
        out_shape=(
            jax.ShapeDtypeStruct((count, chans), BF16),
            jax.ShapeDtypeStruct((count, chans), F32),
            jax.ShapeDtypeStruct((count, chans), F32),
            jax.ShapeDtypeStruct((8, chans), F32),
        ),
        in_specs=[
            wide,
            wide,
            wide,
            pl.BlockSpec((1, count, block), lambda i: (0, 0, i)),
            pl.BlockSpec((1, block), lambda i: (0, i)),
            pl.BlockSpec((count + 16, 128), lambda i: (0, 0)),
        ],
        out_specs=(wide, wide, wide, row8),
    )(gm, gate_pre, hidden, pre, soft, ids)


def rec_back_second_body(
    core, beyond, local, arriving, hidden, entering, pre, conv, chan, soft, gates, ids, ext,
    mine, theirs, grad_values, edge, chan_grad,
):
    count, block = local.shape
    row = lax.broadcasted_iota(jnp.int32, (count, block), 0)
    state = local[...] + beyond[...] * arriving[0:1]
    earlier = jnp.where(row >= 1, pltpu.roll(hidden[...], 1, 0), entering[0:1])
    low = conv[...].astype(F32)
    keep_rate = jax.nn.sigmoid(pre[0])
    log_decay = -8.0 * keep_rate * soft[...]
    decay = jnp.exp(log_decay)
    size = jnp.sqrt(minus_expm1(2.0 * log_decay))
    gate = jax.nn.sigmoid(pre[1])
    grad_decay = state * earlier * same_rows(ids[...], 1)
    grad_log = grad_decay * decay - state * gate * low * (decay * decay / size)
    grad_rate = grad_log * (-8.0 * soft[...]) * keep_rate * (1.0 - keep_rate)
    grad_gate = state * size * low * gate * (1.0 - gate)
    rate_low = grad_rate.astype(BF16)
    gate_low_part = grad_gate.astype(BF16)
    swap = core[0] == 0
    mine[...] = jnp.where(swap, rate_low, gate_low_part)
    theirs[...] = jnp.where(swap, gate_low_part, rate_low)
    weights = gates[0]
    over = (((1,), (1,)), ((), ()))
    grad_conv = (
        state * size * gate
        + lax.dot_general(rate_low, weights[:, :block], over, preferred_element_type=F32)
        + lax.dot_general(gate_low_part, weights[:, block:], over, preferred_element_type=F32)
    )
    wide = ext[...].astype(F32)
    total = chan[0:1] * grad_conv
    chan_grad[0:1] = jnp.sum(grad_conv * wide[16:], axis=0, keepdims=True)
    row8 = lax.broadcasted_iota(jnp.int32, (8, block), 0)
    over_edge = jnp.zeros((8, block), F32)
    for k in range(1, 4):
        masked = grad_conv * same_rows(ids[...], k)
        chan_grad[k : k + 1] = jnp.sum(masked * pltpu.roll(wide, k, 0)[16:], axis=0, keepdims=True)
        back = chan[k : k + 1] * masked
        total = total + shifted(back, -k, row, 0.0)
        first = back[0:8]
        if k < 3:
            first = pltpu.roll(first, 3 - k, 0)
        over_edge = over_edge + jnp.where((row8 >= 3 - k) & (row8 < 3), first, 0.0)
    grad_values[...] = total
    edge[...] = over_edge
    chan_grad[4:5] = jnp.sum(grad_conv, axis=0, keepdims=True)
    chan_grad[5:6] = jnp.sum(grad_rate, axis=0, keepdims=True)
    chan_grad[6:7] = jnp.sum(grad_gate, axis=0, keepdims=True)
    chan_grad[7:8] = jnp.sum(grad_log * keep_rate, axis=0, keepdims=True) * (
        -8.0 * jax.nn.sigmoid(chan[7:8])
    )


def rec_back_second(core, beyond, local, arriving, hidden, entering, pre, conv, chan, soft, gates, ids, ext):
    count, chans = local.shape
    blocks, block = gates.shape[:2]
    wide = pl.BlockSpec((count, block), lambda i, core: (0, i))
    row8 = pl.BlockSpec((8, block), lambda i, core: (0, i))
    pair = pl.BlockSpec((2, count, block), lambda i, core: (0, 0, i))
    low = jax.ShapeDtypeStruct((count, chans), BF16)
    return pl.pallas_call(
        rec_back_second_body,
        name="rec_back_second",
        grid_spec=pltpu.PrefetchScalarGridSpec(
            num_scalar_prefetch=1,
            grid=(blocks,),
            in_specs=[
                wide,
                wide,
                row8,
                wide,
                row8,
                pair,
                wide,
                row8,
                pl.BlockSpec((1, block), lambda i, core: (0, i)),
                pl.BlockSpec((1, block, 2 * block), lambda i, core: (i, 0, 0)),
                pl.BlockSpec((count + 16, 128), lambda i, core: (0, 0)),
                pl.BlockSpec((count + 16, block), lambda i, core: (0, i)),
            ],
            out_specs=(wide, wide, wide, row8, row8),
        ),
        out_shape=(
            low,
            low,
            jax.ShapeDtypeStruct((count, chans), F32),
            jax.ShapeDtypeStruct((8, chans), F32),
            jax.ShapeDtypeStruct((8, chans), F32),
        ),
    )(core, beyond, local, arriving, hidden, entering, pre, conv, chan, soft, gates, ids, ext)


def from_behind(array, axis, by):
    devices = lax.axis_size(axis)
    pairs = [(i, i + by) for i in range(devices) if 0 <= i + by < devices]
    return lax.ppermute(array, axis, pairs)


def swapped(array):
    return lax.ppermute(array, "section", SWAP)


def attend(query_rows, key_rows, allowed):
    head_dim = query_rows.shape[2]
    scores = jnp.einsum(
        "qhd,kd->hqk", query_rows, key_rows[:, :head_dim], preferred_element_type=F32
    ) * head_dim ** (-0.5)
    masked = jnp.where(allowed[None], scores, -1e30)
    row_max = jnp.max(masked, axis=-1, keepdims=True)
    lifted = jnp.exp(masked - row_max)
    row_total = jnp.sum(lifted, axis=-1, keepdims=True)
    weights = (lifted / row_total).astype(BF16)
    attended = jnp.einsum(
        "hqk,kd->qhd", weights, key_rows[:, head_dim:], preferred_element_type=F32
    ).astype(BF16)
    return (attended, row_max[:, :, 0] + jnp.log(row_total[:, :, 0]))


def attend_back(query_rows, key_rows, allowed, log_total, grad_rows):
    head_dim = query_rows.shape[2]
    factor = head_dim ** (-0.5)
    scores = (
        jnp.einsum("qhd,kd->hqk", query_rows, key_rows[:, :head_dim], preferred_element_type=F32)
        * factor
    )
    probs = jnp.exp(jnp.where(allowed[None], scores, -1e30) - log_total[:, :, None])
    weights = probs.astype(BF16)
    grad_probs = jnp.einsum(
        "qhd,kd->hqk", grad_rows, key_rows[:, head_dim:], preferred_element_type=F32
    )
    grad_values = jnp.einsum("hqk,qhd->kd", weights, grad_rows, preferred_element_type=F32)
    grad_scores = (
        probs * (grad_probs - jnp.sum(grad_probs * probs, axis=-1, keepdims=True))
    ).astype(BF16)
    grad_query = (
        jnp.einsum("hqk,kd->qhd", grad_scores, key_rows[:, :head_dim], preferred_element_type=F32)
        * factor
    )
    grad_keys = (
        jnp.einsum("hqk,qhd->kd", grad_scores, query_rows, preferred_element_type=F32) * factor
    )
    return (grad_query, jnp.concatenate([grad_keys, grad_values], axis=-1))


def seq_scatter(grad):
    return lax.psum_scatter(grad, "seq", scatter_dimension=0, tiled=True)


def on_device(
    inputs,
    segments,
    norms,
    rec_in,
    rec_gates,
    rec_chan,
    rec_out,
    attn_q,
    attn_kv,
    attn_out,
    mlp_in,
    mlp_out,
    cotangent,
):
    core = lax.axis_index("section")
    first = core == 0
    place = lax.axis_index("seq")
    rank = lax.axis_index("head")
    heads = lax.axis_size("head")
    blocks_seq = lax.axis_size("seq")
    _, count, width = inputs.shape
    rows = count // heads
    chans = rec_in.shape[2]
    blocks, block = rec_gates.shape[:2]

    def pick(array, index):
        return lax.dynamic_index_in_dim(array, index, 0, keepdims=False)

    def own_rows(array):
        return lax.dynamic_slice_in_dim(array, rank * rows, rows, axis=0)

    core_ref = core[None].astype(jnp.int32)
    ids = pick(segments, core)
    stream_low = pick(inputs, core)
    top_low = pick(cotangent, core)
    before = from_behind(stream_low[-16:], "seq", 1)
    reach = min(max(1, WINDOW // count), blocks_seq - 1)
    before_ids = from_behind(ids, "seq", 1)

    own_in = jnp.swapaxes(mlp_in[0], 0, 1)
    own_out = mlp_out[0]
    other_in, other_out, other_norms = swapped(own_in), swapped(own_out), swapped(norms[0])
    gains = [
        jnp.where(first, norms[0], other_norms),
        jnp.where(first, other_norms, norms[0]),
    ]
    gain = [[gains[l][k][None] for k in range(2)] for l in range(2)]
    weights = (own_in, own_out, other_in, other_out)
    rec_in_wide = jnp.swapaxes(rec_in, 0, 1)

    before_ids = jnp.where(place == 0, -1, before_ids[-16:])
    ext_ids = jnp.broadcast_to(jnp.concatenate([before_ids, ids])[:, None], (count + 16, 128))
    soft = jax.nn.softplus(rec_chan[7:8])
    gates_flat = rec_gates.reshape(blocks, block, 2 * block)
    normed_one, gate_pre, ext, conv_low, pre, through, local, edge = rec_forward(
        jnp.concatenate([before, stream_low]),
        gain[0][0],
        rec_in_wide,
        ext_ids,
        rec_chan,
        soft,
        gates_flat,
    )
    entering, every_id = carry(edge, 0, ids[None])
    hidden_state, mixed, part = rec_finish(local, through, entering, gate_pre, rec_out)
    stream_rows = own_rows(stream_low).astype(F32)
    res_one, normed_a, gate_up_a, hidden_a, part = join_mlp(
        part, stream_rows, gain[0][1], weights, 1
    )
    passed, normed_two, all_keys = join_keys(part, res_one, gain[1][0], attn_kv, reach, 2)

    head_dim = attn_kv.shape[1] // 2
    heads_here = attn_q.shape[1] // head_dim
    queries = dot(normed_two, attn_q, (1, 0), BF16).reshape(count, heads_here, head_dim)
    key_ids = jnp.concatenate(
        [
            pick(every_id, lax.rem(place - distance + blocks_seq, blocks_seq))[0]
            for distance in range(reach, 0, -1)
        ]
        + [ids]
    )
    key_spots = (place - reach) * count + jnp.arange((reach + 1) * count, dtype=jnp.int32)
    query_spots = place * count + jnp.arange(count, dtype=jnp.int32)
    distance_q = query_spots[:, None] - key_spots[None, :]
    inside = (distance_q >= 0) & (distance_q < WINDOW) & (key_spots >= 0)[None, :]
    allowed = inside & (ids[:, None] == key_ids[None, :])
    attended, log_totals = attend(queries, all_keys, allowed)
    attended = attended.reshape(count, heads_here * head_dim)
    part = dot(attended, attn_out, (1, 0), BF16)
    res_two, normed_b, hidden_b, mine_b, theirs_b, part_last, part_b = join_mlp(
        part, passed, gain[1][1], weights, 3, top_low
    )

    units = hidden_b.shape[1]
    window = (units // 2 + 127) // 128 * 128

    def mlp_term(mine, theirs, normed, hidden, out_low, out_other):
        return [
            (normed, swapped(normed), mine, swapped(theirs), units),
            (out_low, out_other, hidden, swapped(hidden), window),
        ]

    terms = mlp_term(mine_b, theirs_b, normed_b, hidden_b, top_low, pick(cotangent, 1 - core))
    part, sum_b = lax.optimization_barrier((part_b, weight_grad(core_ref, terms, False)))
    sum_b = seq_scatter(sum_b)
    grad_res_two, gain_b, low_two = join_backward(
        part, res_two, gain[1][1], own_rows(top_low).astype(F32), 5
    )

    grad_att = dot(low_two, attn_out, (1, 1), BF16)
    grad_query, grad_kv = attend_back(
        queries, all_keys, allowed, log_totals, grad_att.reshape(count, heads_here, head_dim)
    )
    query_low = grad_query.reshape(count, heads_here * head_dim).astype(BF16)
    part = dot(query_low, attn_q, (1, 1), BF16)
    grad_passed, gain_two, low_passed, kv_low, mine_a, theirs_a, part = join_keys_back(
        part,
        passed,
        gain[1][0],
        grad_res_two,
        grad_kv.astype(BF16).reshape(reach + 1, count, 2 * head_dim),
        attn_kv,
        gate_up_a,
        weights,
        6,
    )

    normed_two_other = swapped(normed_two)
    width_q, width_kv = query_low.shape[1], kv_low.shape[1]
    attn_terms = [
        (normed_two, normed_two_other, query_low, swapped(query_low), width_q),
        (normed_two, normed_two_other, kv_low, swapped(kv_low), width_kv),
        (low_two, swapped(low_two), attended, swapped(attended), width_q),
    ]
    terms = mlp_term(mine_a, theirs_a, normed_a, hidden_a, low_passed, swapped(low_passed))
    part, sum_a = lax.optimization_barrier((part, weight_grad(core_ref, terms, False)))
    sum_a = seq_scatter(sum_a)
    grad_res_one, gain_a, mix_low = join_backward(part, res_one, gain[0][1], grad_passed, 7)

    grad_mixed = dot(mix_low, rec_out, (1, 1))
    grad_branch, beyond, local_grad, edge = rec_back_first(
        grad_mixed, gate_pre, hidden_state, pre, soft, ext_ids, block
    )
    (arriving,) = carry(edge, 9)
    gate_mine, gate_theirs, grad_values, over_edge, chan_grad = rec_back_second(
        core_ref, beyond, local_grad, arriving, hidden_state, entering, pre, conv_low, rec_chan,
        soft, gates_flat, ext_ids, ext,
    )
    from_next = from_behind(over_edge[:3], "seq", -1)
    grad_values = jnp.concatenate([grad_values[:-3], grad_values[-3:] + from_next]).astype(BF16)
    part = (
        dot(grad_values, rec_in_wide[0], (1, 1)) + dot(grad_branch, rec_in_wide[1], (1, 1))
    ).astype(BF16)
    normed_one_other = swapped(normed_one)
    rec_sum = weight_grad(
        core_ref,
        [
            (normed_one, normed_one_other, grad_values, swapped(grad_values), chans),
            (normed_one, normed_one_other, grad_branch, swapped(grad_branch), chans),
            (mix_low, swapped(mix_low), mixed, swapped(mixed), chans),
        ]
        + attn_terms,
        True,
    )
    part, rec_sum = lax.optimization_barrier((part, rec_sum))
    rec_sum = seq_scatter(rec_sum)
    _, gain_one, grad_inputs = join_backward(part, stream_rows, gain[0][0], grad_res_one, 8)

    def gate_grad(left, right):
        return jnp.einsum(
            "tnb,tnc->bnc",
            left.reshape(count, blocks, block),
            right.reshape(count, blocks, block),
            preferred_element_type=F32,
        )

    gate_sum = gate_grad(conv_low, gate_mine) + gate_grad(swapped(conv_low), swapped(gate_theirs))
    share = block // (2 * blocks_seq)
    gate_sum = jnp.swapaxes(
        gate_sum.astype(BF16).reshape(2, blocks_seq, share, chans), 0, 1
    ).reshape(blocks_seq, 2 * share, chans)
    gain_rows = jnp.concatenate([gain_one, gain_a, gain_two, gain_b], axis=0)
    gain_total, chan_total, gate_sum = totals(gain_rows, chan_grad, gate_sum, 11)
    gate_sum = gate_sum.reshape(2, share, chans)
    share_norm = width // blocks_seq
    grad_norms = lax.dynamic_slice_in_dim(
        pick(gain_total.reshape(2, 2, width), core), place * share_norm, share_norm, axis=1
    )
    grad_chan = jnp.where(first, chan_total[:4], chan_total[4:])

    own_part = jnp.where(first, sum_a, sum_b)
    other_part = swapped(jnp.where(first, sum_b, sum_a))
    lower = jnp.where(first, own_part, other_part).astype(F32)
    upper = jnp.where(first, other_part, own_part).astype(F32)
    grad_mlp_in = jnp.stack([lower[:, :units], upper[:, :units]], axis=1)
    grad_mlp_out = jnp.concatenate(
        [lower[:, units:].T, upper[:, 2 * window :].T], axis=0
    )
    part_last, grad_mlp_in, grad_mlp_out, grad_norms = lax.optimization_barrier(
        (part_last, grad_mlp_in, grad_mlp_out, grad_norms)
    )
    _, final = join_forward("last", part_last, res_two, gain[1][1], 4)

    chans_q = attn_q.shape[1]
    rec_sum = rec_sum.astype(F32)
    attn_sum = rec_sum[:, 3 * chans :]
    grad_q = attn_sum[:, :chans_q]
    grad_kv_out = attn_sum[:, chans_q : chans_q + 2 * head_dim]
    grad_attn_out = attn_sum[:, chans_q + 2 * head_dim :].T
    grad_in = rec_sum[:, : 2 * chans].reshape(-1, 2, chans)
    grad_rec_out = rec_sum[:, 2 * chans : 3 * chans].T
    own_gate = pick(gate_sum, core)
    other_gate = swapped(pick(gate_sum, 1 - core))
    grad_gates = jnp.transpose(
        jnp.stack([jnp.where(first, own_gate, other_gate), jnp.where(first, other_gate, own_gate)])
        .astype(F32)
        .reshape(2, share, blocks, block),
        (2, 1, 0, 3),
    )
    return (
        final[None],
        grad_inputs.astype(F32)[None],
        grad_norms[None],
        grad_in,
        grad_gates,
        grad_chan,
        grad_rec_out,
        grad_q,
        grad_kv_out,
        grad_attn_out,
        grad_mlp_in[None],
        grad_mlp_out[None],
    )


def solution(mesh):
    in_specs = (
        P(None, "seq", None),
        P(None, "seq"),
        P("section", None, None),
        P(None, None, "head"),
        P("head", None, None, None),
        P(None, "head"),
        P("head", None),
        P(None, "head"),
        P(),
        P("head", None),
        P("section", None, None, "head"),
        P("section", "head", None),
        P(None, "seq", None),
    )
    out_specs = (
        P("section", "seq", None),
        P("section", "seq", None),
        P("section", None, "seq"),
        P(("section", "seq"), None, "head"),
        P("head", ("section", "seq"), None, None),
        P("section", "head"),
        P("head", ("section", "seq")),
        P(("section", "seq"), "head"),
        P(("section", "seq"), None),
        P("head", ("section", "seq")),
        P("section", "seq", None, "head"),
        P("section", "head", "seq"),
    )

    return jax.shard_map(
        on_device, mesh=mesh, in_specs=in_specs, out_specs=out_specs, check_vma=False
    )
```

```python
import functools

import jax
import jax.numpy as jnp
from jax import lax
from jax.experimental import pallas as pl
from jax.experimental.pallas import tpu as pltpu
from jax.sharding import PartitionSpec as P

WINDOW = 1024
EPSILON = 1e-06
MESH = pl.DeviceIdType.MESH
F32 = jnp.float32
BF16 = jnp.bfloat16
SWAP = [(0, 1), (1, 0)]


def dot(a, b, dims, out=F32):
    return lax.dot_general(a, b, ((dims[:1], dims[1:]), ((), ())), preferred_element_type=F32).astype(
        out
    )


def vmem():
    return pl.BlockSpec(memory_space=pltpu.VMEM)


def meet(axis, me, n):
    barrier = pltpu.get_barrier_semaphore()
    for k in range(1, n):
        peer = lax.rem(me + k, n)
        pl.semaphore_signal(barrier, inc=1, device_id={axis: peer}, device_id_type=MESH)
    pl.semaphore_wait(barrier, n - 1)


def remote(src, dst, send, recv, axis, peer):
    return pltpu.make_async_remote_copy(
        src_ref=src,
        dst_ref=dst,
        send_sem=send,
        recv_sem=recv,
        device_id={axis: peer},
        device_id_type=MESH,
    )


def scatter_start(n, me, rows, part, recv, send_sem, recv_sem):
    copies = []
    for k in range(1, n):
        peer = lax.rem(me + k, n)
        start = pl.multiple_of(peer * rows, rows)
        copies.append(
            remote(
                part.at[pl.ds(start, rows)],
                recv.at[k - 1],
                send_sem.at[k - 1],
                recv_sem.at[k - 1],
                "head",
                peer,
            )
        )
    for copy in copies:
        copy.start()
    return copies


def scatter_sum(me, rows, part, recv, copies):
    total = part[pl.ds(pl.multiple_of(me * rows, rows), rows)].astype(F32)
    for k, copy in enumerate(copies):
        copy.wait_recv()
        total = total + recv[k].astype(F32)
    return total


def drain(copies):
    for copy in copies:
        copy.wait_send()


def spread(n, me, rows, value, full, send_sem, recv_sem):
    mine = pl.ds(pl.multiple_of(me * rows, rows), rows)
    full[mine] = value
    copies = []
    for k in range(1, n):
        peer = lax.rem(me + k, n)
        copies.append(
            remote(
                full.at[mine], full.at[mine], send_sem.at[k - 1], recv_sem.at[k - 1], "head", peer
            )
        )
    for copy in copies:
        copy.start()
    return copies


def finish(copies):
    for copy in copies:
        copy.wait()


def own_part(array, me, rows):
    core = lax.axis_index("section")
    return array[core, pl.ds(pl.multiple_of(me * rows, rows), rows)].astype(F32)


def forward_rows(n, me, kind, part, base, gain, new, full, recv, s1, r1, s2, r2):
    rows = base.shape[0]
    sent = scatter_start(n, me, rows, part, recv, s1, r1)
    fresh = base + scatter_sum(me, rows, part, recv, sent)
    new[...] = fresh
    out = fresh
    if kind != "last":
        out = fresh * lax.rsqrt(jnp.mean(fresh * fresh, axis=-1, keepdims=True) + EPSILON)
        out = out * gain[...]
    finish(spread(n, me, rows, out.astype(BF16), full, s2, r2))
    drain(sent)


def forward_body(n, kind, part, base, gain, new, full, recv, s1, r1, s2, r2):
    me = lax.axis_index("head")
    meet("head", me, n)
    forward_rows(n, me, kind, part, base[...], gain, new, full, recv, s1, r1, s2, r2)


def meet_axes(axes):
    barrier = pltpu.get_barrier_semaphore()
    for axis, me, n in axes:
        for k in range(1, n):
            pl.semaphore_signal(
                barrier, inc=1, device_id={axis: lax.rem(me + k, n)}, device_id_type=MESH
            )
    pl.semaphore_wait(barrier, sum(n - 1 for _, _, n in axes))


def mixing_body(
    n, blocks, edge, ids, local, through, gate_pre, w_out, inputs, gain, own_in, own_out, other_in, other_out,
    entering, all_ids, state_out, mixed, new, full, gate_up, hidden, part_next,
    every, c1, c2, c3, c4, part, recv, s1, r1, s2, r2, acc, b_in, b_out, sems,
):
    own, other = (own_in, own_out), (other_in, other_out)
    me, place = lax.axis_index("head"), lax.axis_index("seq")
    rows = part.shape[0] // n
    all_ids[place] = ids[...]
    meet_axes((("head", me, n), ("seq", place, blocks)))
    carried = carry_start(blocks, place, edge, every, c1, c2)
    fetch_weights(0, own, other, (b_in, b_out), sems)
    id_copies = []
    for k in range(1, blocks):
        peer = lax.rem(place + k, blocks)
        id_copies.append(
            remote(ids, all_ids.at[place], c3.at[k - 1], c4.at[k - 1], "seq", peer)
        )
    for copy in id_copies:
        copy.start()
    act = gelu_parts(gate_pre[...])[0]
    finish(carried)
    state_in = carry_state(blocks, place, False, every, edge.shape[1])
    entering[...] = jnp.broadcast_to(state_in, entering.shape)
    state = local[...] + through[...] * state_in
    state_out[...] = state
    low = (state * act).astype(BF16)
    mixed[...] = low
    part[...] = jnp.dot(low, w_out[...], preferred_element_type=F32).astype(BF16)
    base = own_part(inputs, me, rows)
    forward_rows(n, me, "keep", part, base, gain, new, full, recv, s1, r1, s2, r2)
    finish(id_copies)
    wait_weights(own, (b_in, b_out), sems)
    mlp_forward_part(full, (b_in, b_out), gate_up, hidden, part_next, acc)


def mixing(edge, ids, local, through, gate_pre, w_out, inputs, gain, weights, ident):
    n, blocks = lax.axis_size("head"), lax.axis_size("seq")
    count, chans = local.shape
    width = w_out.shape[1]
    rows = count // n
    units = weights[1].shape[0]
    dma = pltpu.SemaphoreType.DMA
    f32, wide = jax.ShapeDtypeStruct((count, chans), F32), jax.ShapeDtypeStruct((count, width), BF16)
    outs = (
        jax.ShapeDtypeStruct(edge.shape, F32),
        jax.ShapeDtypeStruct((blocks,) + ids.shape, jnp.int32),
        f32,
        jax.ShapeDtypeStruct((count, chans), BF16),
        jax.ShapeDtypeStruct((rows, width), F32),
        wide,
        jax.ShapeDtypeStruct((TILES, count, 2 * units // TILES), F32),
        jax.ShapeDtypeStruct((count, units), BF16),
        wide,
    )
    return pl.pallas_call(
        functools.partial(mixing_body, n, blocks),
        name="mixing",
        out_shape=outs,
        in_specs=[vmem()] * 8 + [pl.BlockSpec(memory_space=pl.ANY)] * 4,
        out_specs=tuple(vmem() for _ in outs),
        scratch_shapes=[pltpu.VMEM((blocks - 1,) + edge.shape, F32)]
        + [dma((blocks - 1,))] * 4
        + [pltpu.VMEM((count, width), BF16)]
        + boundary_scratch(n, rows, width)
        + mlp_scratch(count, width, units, 1),
        compiler_params=pltpu.CompilerParams(collective_id=ident, has_side_effects=True),
    )(edge, ids, local, through, gate_pre, w_out, inputs, gain, *weights)


def last_layer_body(n, part, base, gain, top, own_in, own_out, other_in, other_out, *refs):
    new, full, hidden, mine, part_last, part_back, full_other, hidden_other, mine_other = refs[:9]
    recv, s1, r1, s2, r2, theirs, core_sem, acc, acc_back, b_in, b_out, sems = refs[9:]
    own, other = (own_in, own_out), (other_in, other_out)
    me, core = lax.axis_index("head"), lax.axis_index("section")
    tile = b_out.shape[1]
    fetch_weights(1, own, other, (b_in, b_out), sems)
    meet_axes((("head", me, n), ("section", core, 2)))
    forward_rows(n, me, "keep", part, base[...], gain, new, full, recv, s1, r1, s2, r2)

    def to_other(src, dst, t, j):
        return remote(src, dst, core_sem.at[0, j, t], core_sem.at[1, j, t], "section", 1 - core)

    whole = to_other(full, full_other, 0, 2)
    whole.start()
    wait_weights(own, (b_in, b_out), sems)
    acc[...] = jnp.zeros_like(acc)
    acc_back[...] = jnp.zeros_like(acc_back)

    def tile_copies(t):
        at = tile_columns(t, tile)
        return (
            to_other(theirs.at[:, at], mine_other.at[:, at], t, 0),
            to_other(hidden.at[:, at], hidden_other.at[:, at], t, 1),
        )

    @pl.loop(0, TILES)
    def _(t):
        both = jnp.dot(full[...], b_in[t], preferred_element_type=F32)
        gate, up = both[:, :tile], both[:, tile:]
        at = tile_columns(t, tile)
        act = grad_tile(top[core], gate, up, b_in[t], b_out[t], mine, theirs, at, acc_back)
        value = (act * up).astype(BF16)
        hidden[:, at] = value
        for copy in tile_copies(t):
            copy.start()
        acc[...] += jnp.dot(value, b_out[t], preferred_element_type=F32)

    part_last[...] = acc[...].astype(BF16)
    part_back[...] = acc_back[...].astype(BF16)
    whole.wait()

    @pl.loop(0, TILES)
    def _(t):
        for copy in tile_copies(t):
            copy.wait()


def last_layer(part, base, gain, top, weights, ident):
    n = lax.axis_size("head")
    count, width = part.shape
    rows = base.shape[0]
    units = weights[1].shape[0]
    wide = jax.ShapeDtypeStruct((count, width), BF16)
    narrow = jax.ShapeDtypeStruct((count, units), BF16)
    outs = (
        jax.ShapeDtypeStruct((rows, width), F32),
        wide, narrow, narrow, wide, wide, wide, narrow, narrow,
    )
    return pl.pallas_call(
        functools.partial(last_layer_body, n),
        name="last_layer",
        out_shape=outs,
        in_specs=[vmem()] * 4 + [pl.BlockSpec(memory_space=pl.ANY)] * 4,
        out_specs=tuple(vmem() for _ in outs),
        scratch_shapes=boundary_scratch(n, rows, width)
        + [pltpu.VMEM((count, units), BF16), pltpu.SemaphoreType.DMA((2, 3, TILES))]
        + mlp_scratch(count, width, units, 2),
        compiler_params=pltpu.CompilerParams(collective_id=ident, has_side_effects=True),
    )(part, base, gain, top, *weights)


def meet_around(n, me, blocks, place, pairs):
    barrier = pltpu.get_barrier_semaphore()
    for d, k in pairs:
        device = {
            "seq": lax.rem(place - d + blocks, blocks),
            "head": lax.rem(me - k + n, n),
        }
        pl.semaphore_signal(barrier, inc=1, device_id=device, device_id_type=MESH)
    pl.semaphore_wait(barrier, len(pairs))


def keys_body(n, blocks, reach, part, base, gain, w_kv, new, full, keys, recv, s1, r1, s2, r2, own, s3, r3):
    me, place = lax.axis_index("head"), lax.axis_index("seq")
    rows = base.shape[0]
    count = part.shape[0]
    pairs = [(d, k) for d in range(reach + 1) for k in range(n) if (d, k) != (0, 0)]
    meet_around(n, me, blocks, place, pairs)
    sent = scatter_start(n, me, rows, part, recv, s1, r1)
    fresh = base[...] + scatter_sum(me, rows, part, recv, sent)
    fresh = fresh.astype(BF16).astype(F32)
    new[...] = fresh
    out = fresh * lax.rsqrt(jnp.mean(fresh * fresh, axis=-1, keepdims=True) + EPSILON)
    low = (out * gain[...]).astype(BF16)
    value = jnp.dot(low, w_kv[...], preferred_element_type=F32).astype(BF16)
    own[...] = value
    mine = pl.multiple_of(me * rows, rows)
    keys[pl.ds(reach * count + mine, rows)] = value
    copies = []
    for d, k in pairs:
        copies.append(
            pltpu.make_async_remote_copy(
                src_ref=own,
                dst_ref=keys.at[pl.ds((reach - d) * count + mine, rows)],
                send_sem=s3.at[d * n + k],
                recv_sem=r3.at[d * n + k],
                device_id={
                    "seq": lax.rem(place + d, blocks),
                    "head": lax.rem(me + k, n),
                },
                device_id_type=MESH,
            )
        )
    for copy in copies:
        copy.start()
    finish(spread(n, me, rows, low, full, s2, r2))
    finish(copies)
    drain(sent)


def norm_back_rows(grad, v, gain, up):
    scale = lax.rsqrt(jnp.mean(v * v, axis=-1, keepdims=True) + EPSILON)
    gain_grad = jnp.sum(grad * v * scale, axis=0, keepdims=True)
    inner = grad * gain
    out = up + scale * inner - v * (
        scale * scale * scale * jnp.mean(inner * v, axis=-1, keepdims=True)
    )
    return out, gain_grad


def backward_body(n, part, base, gain, up, res, gain_grad, full, recv, s1, r1, s2, r2):
    me = lax.axis_index("head")
    rows = res.shape[0]
    meet("head", me, n)
    sent = scatter_start(n, me, rows, part, recv, s1, r1)
    grad = scatter_sum(me, rows, part, recv, sent)
    v = own_part(base, me, rows) if len(base.shape) == 3 else base[...]
    above = own_part(up, me, rows) if len(up.shape) == 3 else up[...]
    out, gain_grad[...] = norm_back_rows(grad, v, gain[...], above)
    res[...] = out
    finish(spread(n, me, rows, out.astype(BF16), full, s2, r2))
    drain(sent)


def keys_back_body(
    n, blocks, reach, part, base, gain, up, grad_kv, w_kv, gate_up, own_in, own_out, other_in, other_out,
    res, gain_grad, full, kv_full, mine_out, theirs_out, part_next,
    recv, s1, r1, s2, r2, recv_kv, s3, r3, send_z, recv_z, s4, r4, s5, r5, acc, b_in, b_out, sems,
):
    own, other = (own_in, own_out), (other_in, other_out)
    fetch_weights(0, own, other, (b_in, b_out), sems)
    me, place = lax.axis_index("head"), lax.axis_index("seq")
    rows = base.shape[0]
    meet_around(
        n,
        me,
        blocks,
        place,
        [(0, k) for k in range(1, n)] + [(-d, 0) for d in range(1, reach + 1)],
    )
    mine = pl.ds(pl.multiple_of(me * rows, rows), rows)
    kv_sent = []
    for k in range(1, n):
        peer = lax.rem(me + k, n)
        there = pl.ds(pl.multiple_of(peer * rows, rows), rows)
        kv_sent.append(
            remote(
                grad_kv.at[:, there], recv_kv.at[k - 1], s3.at[k - 1], r3.at[k - 1], "head", peer
            )
        )
    for copy in kv_sent:
        copy.start()
    sent = scatter_start(n, me, rows, part, recv, s1, r1)
    total = grad_kv[:, mine].astype(F32)
    for k, copy in enumerate(kv_sent):
        copy.wait_recv()
        total = total + recv_kv[k].astype(F32)
    send_z[...] = total.astype(BF16)
    z_sent = []
    for d in range(1, reach + 1):
        z_sent.append(
            remote(
                send_z.at[reach - d],
                recv_z.at[d - 1],
                s4.at[d - 1],
                r4.at[d - 1],
                "seq",
                lax.rem(place - d + blocks, blocks),
            )
        )
    for copy in z_sent:
        copy.start()
    grad = scatter_sum(me, rows, part, recv, sent)
    own_kv = total[reach]
    for d, copy in enumerate(z_sent):
        copy.wait_recv()
        own_kv = own_kv + recv_z[d].astype(F32)
    kv_low = own_kv.astype(BF16)
    kv_spread = spread(n, me, rows, kv_low, kv_full, s5, r5)
    grad = grad + lax.dot_general(
        kv_low, w_kv[...], (((1,), (1,)), ((), ())), preferred_element_type=F32
    )
    out, gain_grad[...] = norm_back_rows(grad, base[...], gain[...], up[...])
    low = out.astype(BF16)
    res[...] = low.astype(F32)
    finish(spread(n, me, rows, low, full, s2, r2))
    finish(kv_spread)
    drain(sent + kv_sent + z_sent)
    wait_weights(own, (b_in, b_out), sems)
    mlp_backward_part(full, gate_up, (b_in, b_out), mine_out, theirs_out, part_next, acc)


def boundary_scratch(n, rows, width):
    return [pltpu.VMEM((n - 1, rows, width), BF16)] + [pltpu.SemaphoreType.DMA((n - 1,))] * 4


def join_forward(kind, part, base, gain, ident):
    n = lax.axis_size("head")
    count, width = part.shape
    rows = base.shape[0]
    return pl.pallas_call(
        functools.partial(forward_body, n, kind),
        out_shape=(
            jax.ShapeDtypeStruct((rows, width), F32),
            jax.ShapeDtypeStruct((count, width), BF16),
        ),
        in_specs=[vmem()] * 3,
        out_specs=(vmem(), vmem()),
        scratch_shapes=boundary_scratch(n, rows, width),
        compiler_params=pltpu.CompilerParams(collective_id=ident, has_side_effects=True),
    )(part, base, gain)


def join_keys(part, base, gain, w_kv, reach, ident):
    n, blocks = lax.axis_size("head"), lax.axis_size("seq")
    count, width = part.shape
    rows = base.shape[0]
    both = w_kv.shape[1]
    slots = (reach + 1) * n
    return pl.pallas_call(
        functools.partial(keys_body, n, blocks, reach),
        name="join_keys",
        out_shape=(
            jax.ShapeDtypeStruct((rows, width), F32),
            jax.ShapeDtypeStruct((count, width), BF16),
            jax.ShapeDtypeStruct(((reach + 1) * count, both), BF16),
        ),
        in_specs=[vmem()] * 4,
        out_specs=(vmem(), vmem(), vmem()),
        scratch_shapes=boundary_scratch(n, rows, width)
        + [
            pltpu.VMEM((rows, both), BF16),
            pltpu.SemaphoreType.DMA((slots,)),
            pltpu.SemaphoreType.DMA((slots,)),
        ],
        compiler_params=pltpu.CompilerParams(collective_id=ident, has_side_effects=True),
    )(part, base, gain, w_kv)


def join_backward(part, base, gain, up, ident):
    n = lax.axis_size("head")
    count, width = part.shape
    rows = count // n
    return pl.pallas_call(
        functools.partial(backward_body, n),
        out_shape=(
            jax.ShapeDtypeStruct((rows, width), F32),
            jax.ShapeDtypeStruct((1, width), F32),
            jax.ShapeDtypeStruct((count, width), BF16),
        ),
        in_specs=[vmem()] * 4,
        out_specs=(vmem(), vmem(), vmem()),
        scratch_shapes=boundary_scratch(n, rows, width),
        compiler_params=pltpu.CompilerParams(collective_id=ident, has_side_effects=True),
    )(part, base, gain, up)


def join_keys_back(part, base, gain, up, grad_kv, w_kv, gate_up, weights, ident):
    n, blocks = lax.axis_size("head"), lax.axis_size("seq")
    count, width = part.shape
    rows = base.shape[0]
    reach, both = grad_kv.shape[0] - 1, grad_kv.shape[2]
    units = weights[1].shape[0]
    dma = pltpu.SemaphoreType.DMA
    return pl.pallas_call(
        functools.partial(keys_back_body, n, blocks, reach),
        name="join_keys_back",
        out_shape=(
            jax.ShapeDtypeStruct((rows, width), F32),
            jax.ShapeDtypeStruct((1, width), F32),
            jax.ShapeDtypeStruct((count, width), BF16),
            jax.ShapeDtypeStruct((count, both), BF16),
            jax.ShapeDtypeStruct((count, units), BF16),
            jax.ShapeDtypeStruct((count, units), BF16),
            jax.ShapeDtypeStruct((count, width), BF16),
        ),
        in_specs=[vmem()] * 7 + [pl.BlockSpec(memory_space=pl.ANY)] * 4,
        out_specs=tuple([vmem()] * 7),
        scratch_shapes=boundary_scratch(n, rows, width)
        + [
            pltpu.VMEM((n - 1, reach + 1, rows, both), BF16),
            dma((n - 1,)),
            dma((n - 1,)),
            pltpu.VMEM((reach + 1, rows, both), BF16),
            pltpu.VMEM((reach, rows, both), BF16),
            dma((reach,)),
            dma((reach,)),
            dma((n - 1,)),
            dma((n - 1,)),
        ]
        + mlp_scratch(count, width, units, 1),
        compiler_params=pltpu.CompilerParams(collective_id=ident, has_side_effects=True),
    )(part, base, gain, up, grad_kv, w_kv, gate_up, *weights)


def totals_body(heads, blocks, gains, chan, gates, gain_out, chan_out, gate_out, *scratch):
    g1, g2, g3, sum_one, sum_two, c2, c3, csum, w2, sems = scratch
    head, place, core = lax.axis_index("head"), lax.axis_index("seq"), lax.axis_index("section")
    barrier = pltpu.get_barrier_semaphore()
    for axis, me, n in (("head", head, heads), ("seq", place, blocks), ("section", core, 2)):
        for k in range(1, n):
            pl.semaphore_signal(
                barrier, inc=1, device_id={axis: lax.rem(me + k, n)}, device_id_type=MESH
            )
    pl.semaphore_wait(barrier, heads + blocks - 1)
    used = 0

    def exchange(src, slots, axis, me, n, split=False):
        nonlocal used
        copies = []
        for k in range(1, n):
            peer = lax.rem(me + k, n)
            copies.append(
                remote(
                    src.at[peer] if split else src,
                    slots.at[k - 1],
                    sems.at[0, used],
                    sems.at[1, used],
                    axis,
                    peer,
                )
            )
            used += 1
        for copy in copies:
            copy.start()
        return copies

    def collect(copies, src, slots):
        total = src[...]
        for k, copy in enumerate(copies):
            copy.wait_recv()
            total = total + slots[k]
        return total

    by_head = exchange(gains, g1, "head", head, heads)
    chan_seq = exchange(chan, c2, "seq", place, blocks)
    gate_seq = exchange(gates, w2, "seq", place, blocks, True)
    sum_one[...] = collect(by_head, gains, g1)
    gain_seq = exchange(sum_one, g2, "seq", place, blocks)
    csum[...] = collect(chan_seq, chan, c2)
    chan_core = exchange(csum, c3, "section", core, 2)
    sum_two[...] = collect(gain_seq, sum_one, g2)
    gain_core = exchange(sum_two, g3, "section", core, 2)
    chan_out[...] = collect(chan_core, csum, c3)
    gain_out[...] = collect(gain_core, sum_two, g3)
    gate_total = gates[place].astype(F32)
    for k, copy in enumerate(gate_seq):
        copy.wait_recv()
        gate_total = gate_total + w2[k].astype(F32)
    gate_out[...] = gate_total.astype(BF16)
    for copy in by_head + chan_seq + gate_seq + gain_seq + chan_core + gain_core:
        copy.wait_send()


def totals(gains, chan, gates, ident):
    heads, blocks = lax.axis_size("head"), lax.axis_size("seq")
    gs, cs, ws = gains.shape, chan.shape, gates.shape[1:]
    return pl.pallas_call(
        functools.partial(totals_body, heads, blocks),
        name="totals",
        out_shape=(
            jax.ShapeDtypeStruct(gs, F32),
            jax.ShapeDtypeStruct(cs, F32),
            jax.ShapeDtypeStruct(ws, BF16),
        ),
        in_specs=[vmem(), vmem(), vmem()],
        out_specs=(vmem(), vmem(), vmem()),
        scratch_shapes=[
            pltpu.VMEM((heads - 1,) + gs, F32),
            pltpu.VMEM((blocks - 1,) + gs, F32),
            pltpu.VMEM((1,) + gs, F32),
            pltpu.VMEM(gs, F32),
            pltpu.VMEM(gs, F32),
            pltpu.VMEM((blocks - 1,) + cs, F32),
            pltpu.VMEM((1,) + cs, F32),
            pltpu.VMEM(cs, F32),
            pltpu.VMEM((blocks - 1,) + ws, BF16),
            pltpu.SemaphoreType.DMA((2, heads + 3 * blocks)),
        ],
        compiler_params=pltpu.CompilerParams(collective_id=ident, has_side_effects=True),
    )(gains, chan, gates)


OVER_LAST = (((1,), (1,)), ((), ()))
TILES = 3


def weight_copies(own, buffers, sems):
    tile = buffers[1].shape[1]
    copies = []
    for t in range(TILES):
        units = pl.ds(t * tile, tile)
        for k in range(2):
            copies.append(
                pltpu.make_async_copy(
                    own[0].at[k, :, units],
                    buffers[0].at[t, :, pl.ds(k * tile, tile)],
                    sems.at[k, t],
                )
            )
        copies.append(pltpu.make_async_copy(own[1].at[units], buffers[1].at[t], sems.at[2, t]))
    return copies


def fetch_weights(layer, own, other, buffers, sems):
    core = lax.axis_index("section")
    for near, use in ((own, core == layer), (other, core != layer)):

        @pl.when(use)
        def _(near=near):
            for copy in weight_copies(near, buffers, sems):
                copy.start()


def wait_weights(own, buffers, sems):
    for copy in weight_copies(own, buffers, sems):
        copy.wait()


def tile_columns(t, tile):
    return pl.ds(pl.multiple_of(t * tile, 128), tile)


def grad_tile(low, gate, up, w_in, w_out, mine, theirs, columns_at, acc):
    grad_hidden = lax.dot_general(low, w_out, OVER_LAST, preferred_element_type=F32)
    act, slope = gelu_parts(gate)
    grad_gate = (grad_hidden * up * slope).astype(BF16)
    grad_up = (grad_hidden * act).astype(BF16)
    swap = lax.axis_index("section") == 0
    mine[:, columns_at] = jnp.where(swap, grad_gate, grad_up)
    theirs[:, columns_at] = jnp.where(swap, grad_up, grad_gate)
    both = jnp.concatenate([grad_gate, grad_up], axis=1)
    acc[...] += lax.dot_general(both, w_in, OVER_LAST, preferred_element_type=F32)
    return act


def mlp_forward_part(x, buffers, gate_up, hidden, part, acc):
    tile = buffers[1].shape[1]
    acc[...] = jnp.zeros_like(acc)

    @pl.loop(0, TILES)
    def _(t):
        both = jnp.dot(x[...], buffers[0][t], preferred_element_type=F32)
        gate_up[t] = both
        low = (gelu_parts(both[:, :tile])[0] * both[:, tile:]).astype(BF16)
        hidden[:, tile_columns(t, tile)] = low
        acc[...] += jnp.dot(low, buffers[1][t], preferred_element_type=F32)

    part[...] = acc[...].astype(BF16)


def mlp_backward_part(low, gate_up, buffers, mine, theirs, part, acc):
    tile = buffers[1].shape[1]
    acc[...] = jnp.zeros_like(acc)

    @pl.loop(0, TILES)
    def _(t):
        grad_tile(
            low[...], gate_up[t, :, :tile], gate_up[t, :, tile:], buffers[0][t], buffers[1][t],
            mine, theirs, tile_columns(t, tile), acc,
        )

    part[...] = acc[...].astype(BF16)


def mlp_scratch(count, width, units, accs):
    tile = units // TILES
    return [pltpu.VMEM((count, width), F32)] * accs + [
        pltpu.VMEM((TILES, width, 2 * tile), BF16),
        pltpu.VMEM((TILES, tile, width), BF16),
        pltpu.SemaphoreType.DMA((3, TILES)),
    ]


def weight_grad_body(sizes, core, *refs):
    out = refs[-1]
    over = (((0,), (0,)), ((), ()))
    start = 0
    for t, size in enumerate(sizes):
        left, left_other, right, right_other = refs[4 * t : 4 * t + 4]
        spare = right.shape[1] - size
        if spare:
            window = pl.ds(pl.multiple_of(core[0] * spare, 128), size)
            near, far = right[:, window], right_other[:, window]
        else:
            near, far = right[...], right_other[...]
        left, left_other = (
            ref[0] if len(ref.shape) == 3 else ref[...] for ref in (left, left_other)
        )
        total = lax.dot_general(left, near, over, preferred_element_type=F32)
        total += lax.dot_general(left_other, far, over, preferred_element_type=F32)
        out[:, start : start + size] = total.astype(BF16)
        start += size


def weight_grad(core, terms, half):
    count, width = terms[0][0].shape
    tile = 256
    steps = width // tile // (2 if half else 1)
    sizes = [term[4] for term in terms]
    in_specs, operands = [], []
    for left, left_other, right, right_other, _ in terms:
        if half:
            rows = pl.BlockSpec((count, tile), lambda i, core: (0, core[0] * steps + i))
        else:
            rows = pl.BlockSpec((count, tile), lambda i, core: (0, i))
        full = pl.BlockSpec(right.shape, lambda i, core: (0, 0))
        if left.ndim == 3:
            in_specs += [
                pl.BlockSpec((1, count, tile), lambda i, core: (core[0], 0, i)),
                pl.BlockSpec((1, count, tile), lambda i, core: (1 - core[0], 0, i)),
            ]
        else:
            in_specs += [rows, rows]
        in_specs += [full, full]
        operands += [left, left_other, right, right_other]
    return pl.pallas_call(
        functools.partial(weight_grad_body, sizes),
        grid_spec=pltpu.PrefetchScalarGridSpec(
            num_scalar_prefetch=1,
            grid=(steps,),
            in_specs=in_specs,
            out_specs=pl.BlockSpec((tile, sum(sizes)), lambda i, core: (i, 0)),
        ),
        out_shape=jax.ShapeDtypeStruct((steps * tile, sum(sizes)), BF16),
    )(core, *operands)


def carry_start(n, me, edge, every, send_sem, recv_sem):
    copies = []
    for k in range(1, n):
        peer = lax.rem(me + k, n)
        copies.append(
            remote(edge, every.at[k - 1], send_sem.at[k - 1], recv_sem.at[k - 1], "seq", peer)
        )
    for copy in copies:
        copy.start()
    return copies


def carry_state(n, me, reverse, every, width):
    state = jnp.zeros((1, width), F32)
    for k in range(1, n) if reverse else range(n - 1, 0, -1):
        inside = me + n - k < n if reverse else me - k >= 0
        slot = every[k - 1]
        state = jnp.where(inside, slot[0:1] * state + slot[1:2], state)
    return state


def carry_body(n, edge, out, every, send_sem, recv_sem):
    me = lax.axis_index("seq")
    meet("seq", me, n)
    finish(carry_start(n, me, edge, every, send_sem, recv_sem))
    out[...] = jnp.broadcast_to(carry_state(n, me, True, every, edge.shape[1]), out.shape)


def carry_back(edge, ident):
    n = lax.axis_size("seq")
    dma = pltpu.SemaphoreType.DMA((n - 1,))
    return pl.pallas_call(
        functools.partial(carry_body, n),
        name="carry_back",
        out_shape=jax.ShapeDtypeStruct(edge.shape, F32),
        in_specs=[vmem()],
        out_specs=vmem(),
        scratch_shapes=[pltpu.VMEM((n - 1,) + edge.shape, F32), dma, dma],
        compiler_params=pltpu.CompilerParams(collective_id=ident, has_side_effects=True),
    )(edge)


def shifted(x, by, row, fill):
    count = x.shape[0]
    if by > 0:
        return jnp.where(row >= by, pltpu.roll(x, by, 0), fill)
    return jnp.where(row < count + by, pltpu.roll(x, count + by, 0), fill)


def scan_rows(a, b, row, sign):
    step = 1
    while step < a.shape[0]:
        b = b + a * shifted(b, sign * step, row, 0.0)
        a = a * shifted(a, sign * step, row, 1.0)
        step *= 2
    return a, b


def minus_expm1(y):
    series = jnp.full_like(y, 1.0)
    for k in range(9, 1, -1):
        series = 1.0 + y * series * (1.0 / k)
    return jnp.where(y > -0.5, -y * series, 1.0 - jnp.exp(y))


def gelu_parts(x):
    c = 0.7978845608028654
    inner = c * (x + 0.044715 * x * x * x)
    t = jnp.tanh(inner)
    act = 0.5 * x * (1.0 + t)
    slope = 0.5 * (1.0 + t) + 0.5 * x * (1.0 - t * t) * c * (1.0 + 3.0 * 0.044715 * x * x)
    return act, slope


def same_rows(ids, k):
    return (pltpu.roll(ids, k, 0)[16:] == ids[16:]).astype(F32)


def soft_plus(x):
    e = jnp.exp(-jnp.abs(x))
    series = jnp.full_like(e, 1.0 / 8.0)
    for k in range(7, 0, -1):
        series = 1.0 / k - e * series
    return jnp.maximum(x, 0.0) + jnp.where(e < 0.05, e * series, jnp.log(1.0 + e))


def id_columns(row):
    return jnp.broadcast_to(row.astype(F32), (128, row.shape[1])).T


def rec_forward_body(
    spot, x, before, gain, w_in, segments, before_ids, chan, gates,
    normed, ids, gate_pre, ext, conv_out, pre_out, through, local, edge, low_x,
):
    count, block = conv_out.shape

    @pl.when(pl.program_id(0) == 0)
    def _():
        for v, at in ((before[0], slice(0, 16)), (x[0], slice(16, count + 16))):
            v = v.astype(F32)
            out = v * lax.rsqrt(jnp.mean(v * v, axis=-1, keepdims=True) + EPSILON) * gain[...]
            low_x[at] = out.astype(BF16)
        normed[...] = low_x[16:]
        earlier = id_columns(before_ids[pl.ds(spot[0], 1)])[count - 16 :]
        ids[0:16] = jnp.where(spot[1] == 0, -1.0, earlier)
        ids[16:] = id_columns(segments[pl.ds(spot[0], 1)])

    values = jnp.dot(low_x[...], w_in[0], preferred_element_type=F32).astype(BF16)
    gate_pre[...] = jnp.dot(low_x[16:], w_in[1], preferred_element_type=F32)
    ext[...] = values
    wide = values.astype(F32)
    total = chan[4:5] + chan[0:1] * wide[16:]
    for k in range(1, 4):
        total = total + chan[k : k + 1] * pltpu.roll(wide, k, 0)[16:] * same_rows(ids[...], k)
    low = total.astype(BF16)
    conv_out[...] = low
    pre = jnp.dot(low, gates[0], preferred_element_type=F32)
    rate = pre[:, :block] + chan[5:6]
    gate = pre[:, block:] + chan[6:7]
    pre_out[0] = rate
    pre_out[1] = gate
    log_decay = -8.0 * jax.nn.sigmoid(rate) * soft_plus(chan[7:8])
    decay = jnp.exp(log_decay) * same_rows(ids[...], 1)
    drive = jnp.sqrt(minus_expm1(2.0 * log_decay)) * jax.nn.sigmoid(gate) * low.astype(F32)
    row = lax.broadcasted_iota(jnp.int32, (count, block), 0)
    a, b = scan_rows(decay, drive, row, 1)
    through[...] = a
    local[...] = b
    edge[0:1] = a[count - 1 :]
    edge[1:2] = b[count - 1 :]
    edge[2:8] = jnp.zeros((6, block), F32)


def rec_forward(spot, inputs, before, gain, w_in, segments, before_ids, chan, gates):
    _, count, width = inputs.shape
    chans = w_in.shape[2]
    blocks, block = gates.shape[:2]
    wide = pl.BlockSpec((count, block), lambda i, spot: (0, i))
    row8 = pl.BlockSpec((8, block), lambda i, spot: (0, i))
    tall = pl.BlockSpec((count + 16, block), lambda i, spot: (0, i))
    flat = pl.BlockSpec(segments.shape, lambda i, spot: (0, 0))
    f32 = jax.ShapeDtypeStruct((count, chans), F32)
    return pl.pallas_call(
        rec_forward_body,
        name="rec_forward",
        grid_spec=pltpu.PrefetchScalarGridSpec(
            num_scalar_prefetch=1,
            grid=(blocks,),
            in_specs=[
                pl.BlockSpec((1, count, width), lambda i, spot: (spot[0], 0, 0)),
                pl.BlockSpec((1, 16, width), lambda i, spot: (spot[0], 0, 0)),
                pl.BlockSpec((1, width), lambda i, spot: (0, 0)),
                pl.BlockSpec((2, width, block), lambda i, spot: (0, 0, i)),
                flat,
                flat,
                row8,
                pl.BlockSpec((1, block, 2 * block), lambda i, spot: (i, 0, 0)),
            ],
            out_specs=(
                pl.BlockSpec((count, width), lambda i, spot: (0, 0)),
                pl.BlockSpec((count + 16, 128), lambda i, spot: (0, 0)),
                wide,
                tall,
                wide,
                pl.BlockSpec((2, count, block), lambda i, spot: (0, 0, i)),
                wide,
                wide,
                row8,
            ),
            scratch_shapes=[pltpu.VMEM((count + 16, width), BF16)],
        ),
        out_shape=(
            jax.ShapeDtypeStruct((count, width), BF16),
            jax.ShapeDtypeStruct((count + 16, 128), F32),
            f32,
            jax.ShapeDtypeStruct((count + 16, chans), BF16),
            jax.ShapeDtypeStruct((count, chans), BF16),
            jax.ShapeDtypeStruct((2, count, chans), F32),
            f32,
            f32,
            jax.ShapeDtypeStruct((8, chans), F32),
        ),
    )(spot, inputs, before, gain, w_in, segments, before_ids, chan, gates)


def rec_back_first_body(gm, gate_pre, hidden, rate, chan, ids, grad_gate, beyond, local, edge):
    count, block = gm.shape
    act, slope = gelu_parts(gate_pre[...])
    up = gm[...]
    grad_gate[...] = (up * hidden[...] * slope).astype(BF16)
    decay = jnp.exp(-8.0 * jax.nn.sigmoid(rate[0]) * soft_plus(chan[7:8])) * same_rows(ids[...], 1)
    row = lax.broadcasted_iota(jnp.int32, (count, block), 0)
    a, b = scan_rows(shifted(decay, -1, row, 1.0), up * act, row, -1)
    beyond[...] = a
    local[...] = b
    edge[0:1] = decay[0:1] * a[0:1]
    edge[1:2] = decay[0:1] * b[0:1]
    edge[2:8] = jnp.zeros((6, block), F32)


def rec_back_first(gm, gate_pre, hidden, pre, chan, ids, block):
    count, chans = gm.shape
    wide = pl.BlockSpec((count, block), lambda i: (0, i))
    row8 = pl.BlockSpec((8, block), lambda i: (0, i))
    return pl.pallas_call(
        rec_back_first_body,
        name="rec_back_first",
        grid=(chans // block,),
        out_shape=(
            jax.ShapeDtypeStruct((count, chans), BF16),
            jax.ShapeDtypeStruct((count, chans), F32),
            jax.ShapeDtypeStruct((count, chans), F32),
            jax.ShapeDtypeStruct((8, chans), F32),
        ),
        in_specs=[
            wide,
            wide,
            wide,
            pl.BlockSpec((1, count, block), lambda i: (0, 0, i)),
            row8,
            pl.BlockSpec((count + 16, 128), lambda i: (0, 0)),
        ],
        out_specs=(wide, wide, wide, row8),
    )(gm, gate_pre, hidden, pre, chan, ids)


def rec_back_second_body(
    core, beyond, local, arriving, hidden, entering, pre, conv, chan, gates, ids, ext,
    mine, theirs, grad_values, edge, chan_grad,
):
    count, block = local.shape
    row = lax.broadcasted_iota(jnp.int32, (count, block), 0)
    state = local[...] + beyond[...] * arriving[0:1]
    earlier = jnp.where(row >= 1, pltpu.roll(hidden[...], 1, 0), entering[0:1])
    low = conv[...].astype(F32)
    soft = soft_plus(chan[7:8])
    keep_rate = jax.nn.sigmoid(pre[0])
    log_decay = -8.0 * keep_rate * soft
    decay = jnp.exp(log_decay)
    size = jnp.sqrt(minus_expm1(2.0 * log_decay))
    gate = jax.nn.sigmoid(pre[1])
    grad_decay = state * earlier * same_rows(ids[...], 1)
    grad_log = grad_decay * decay - state * gate * low * (decay * decay / size)
    grad_rate = grad_log * (-8.0 * soft) * keep_rate * (1.0 - keep_rate)
    grad_gate = state * size * low * gate * (1.0 - gate)
    rate_low = grad_rate.astype(BF16)
    gate_low_part = grad_gate.astype(BF16)
    swap = core[0] == 0
    mine[...] = jnp.where(swap, rate_low, gate_low_part)
    theirs[...] = jnp.where(swap, gate_low_part, rate_low)
    weights = gates[0]
    over = (((1,), (1,)), ((), ()))
    grad_conv = (
        state * size * gate
        + lax.dot_general(rate_low, weights[:, :block], over, preferred_element_type=F32)
        + lax.dot_general(gate_low_part, weights[:, block:], over, preferred_element_type=F32)
    )
    wide = ext[...].astype(F32)
    total = chan[0:1] * grad_conv
    chan_grad[0:1] = jnp.sum(grad_conv * wide[16:], axis=0, keepdims=True)
    row8 = lax.broadcasted_iota(jnp.int32, (8, block), 0)
    over_edge = jnp.zeros((8, block), F32)
    for k in range(1, 4):
        masked = grad_conv * same_rows(ids[...], k)
        chan_grad[k : k + 1] = jnp.sum(masked * pltpu.roll(wide, k, 0)[16:], axis=0, keepdims=True)
        back = chan[k : k + 1] * masked
        total = total + shifted(back, -k, row, 0.0)
        first = back[0:8]
        if k < 3:
            first = pltpu.roll(first, 3 - k, 0)
        over_edge = over_edge + jnp.where((row8 >= 3 - k) & (row8 < 3), first, 0.0)
    grad_values[...] = total
    edge[...] = over_edge
    chan_grad[4:5] = jnp.sum(grad_conv, axis=0, keepdims=True)
    chan_grad[5:6] = jnp.sum(grad_rate, axis=0, keepdims=True)
    chan_grad[6:7] = jnp.sum(grad_gate, axis=0, keepdims=True)
    chan_grad[7:8] = jnp.sum(grad_log * keep_rate, axis=0, keepdims=True) * (
        -8.0 * jax.nn.sigmoid(chan[7:8])
    )


def rec_back_second(core, beyond, local, arriving, hidden, entering, pre, conv, chan, gates, ids, ext):
    count, chans = local.shape
    blocks, block = gates.shape[:2]
    wide = pl.BlockSpec((count, block), lambda i, core: (0, i))
    row8 = pl.BlockSpec((8, block), lambda i, core: (0, i))
    pair = pl.BlockSpec((2, count, block), lambda i, core: (0, 0, i))
    low = jax.ShapeDtypeStruct((count, chans), BF16)
    return pl.pallas_call(
        rec_back_second_body,
        name="rec_back_second",
        grid_spec=pltpu.PrefetchScalarGridSpec(
            num_scalar_prefetch=1,
            grid=(blocks,),
            in_specs=[
                wide,
                wide,
                row8,
                wide,
                row8,
                pair,
                wide,
                row8,
                pl.BlockSpec((1, block, 2 * block), lambda i, core: (i, 0, 0)),
                pl.BlockSpec((count + 16, 128), lambda i, core: (0, 0)),
                pl.BlockSpec((count + 16, block), lambda i, core: (0, i)),
            ],
            out_specs=(wide, wide, wide, row8, row8),
        ),
        out_shape=(
            low,
            low,
            jax.ShapeDtypeStruct((count, chans), F32),
            jax.ShapeDtypeStruct((8, chans), F32),
            jax.ShapeDtypeStruct((8, chans), F32),
        ),
    )(core, beyond, local, arriving, hidden, entering, pre, conv, chan, gates, ids, ext)


def from_behind(array, axis, by):
    devices = lax.axis_size(axis)
    pairs = [(i, i + by) for i in range(devices) if 0 <= i + by < devices]
    return lax.ppermute(array, axis, pairs)


def swapped(array):
    return lax.ppermute(array, "section", SWAP)


def attend(query_rows, key_rows, allowed):
    head_dim = query_rows.shape[2]
    scores = jnp.einsum(
        "qhd,kd->hqk", query_rows, key_rows[:, :head_dim], preferred_element_type=F32
    ) * head_dim ** (-0.5)
    masked = jnp.where(allowed[None], scores, -1e30)
    row_max = jnp.max(masked, axis=-1, keepdims=True)
    lifted = jnp.exp(masked - row_max)
    row_total = jnp.sum(lifted, axis=-1, keepdims=True)
    weights = (lifted / row_total).astype(BF16)
    attended = jnp.einsum(
        "hqk,kd->qhd", weights, key_rows[:, head_dim:], preferred_element_type=F32
    ).astype(BF16)
    return (attended, row_max[:, :, 0] + jnp.log(row_total[:, :, 0]))


def attend_back(query_rows, key_rows, allowed, log_total, grad_rows):
    head_dim = query_rows.shape[2]
    factor = head_dim ** (-0.5)
    scores = (
        jnp.einsum("qhd,kd->hqk", query_rows, key_rows[:, :head_dim], preferred_element_type=F32)
        * factor
    )
    probs = jnp.exp(jnp.where(allowed[None], scores, -1e30) - log_total[:, :, None])
    weights = probs.astype(BF16)
    grad_probs = jnp.einsum(
        "qhd,kd->hqk", grad_rows, key_rows[:, head_dim:], preferred_element_type=F32
    )
    grad_values = jnp.einsum("hqk,qhd->kd", weights, grad_rows, preferred_element_type=F32)
    grad_scores = (
        probs * (grad_probs - jnp.sum(grad_probs * probs, axis=-1, keepdims=True))
    ).astype(BF16)
    grad_query = (
        jnp.einsum("hqk,kd->qhd", grad_scores, key_rows[:, :head_dim], preferred_element_type=F32)
        * factor
    )
    grad_keys = (
        jnp.einsum("hqk,qhd->kd", grad_scores, query_rows, preferred_element_type=F32) * factor
    )
    return (grad_query, jnp.concatenate([grad_keys, grad_values], axis=-1))


def seq_scatter(grad):
    return lax.psum_scatter(grad, "seq", scatter_dimension=0, tiled=True)


def on_device(
    inputs,
    segments,
    norms,
    rec_in,
    rec_gates,
    rec_chan,
    rec_out,
    attn_q,
    attn_kv,
    attn_out,
    mlp_in,
    mlp_out,
    cotangent,
):
    core = lax.axis_index("section")
    first = core == 0
    place = lax.axis_index("seq")
    blocks_seq = lax.axis_size("seq")
    _, count, width = inputs.shape
    chans = rec_in.shape[2]
    blocks, block = rec_gates.shape[:2]

    def pick(array, index):
        return lax.dynamic_index_in_dim(array, index, 0, keepdims=False)

    core_ref = core[None].astype(jnp.int32)
    spot = jnp.stack([core, place]).astype(jnp.int32)
    before = from_behind(inputs[:, -16:], "seq", 1)
    before_ids = from_behind(segments, "seq", 1)
    ids = pick(segments, core)
    reach = min(max(1, WINDOW // count), blocks_seq - 1)

    own_in = jnp.swapaxes(mlp_in[0], 0, 1)
    own_out = mlp_out[0]
    other_in, other_out, other_norms = swapped(own_in), swapped(own_out), swapped(norms[0])
    gains = [
        jnp.where(first, norms[0], other_norms),
        jnp.where(first, other_norms, norms[0]),
    ]
    gain = [[gains[l][k][None] for k in range(2)] for l in range(2)]
    weights = (own_in, own_out, other_in, other_out)
    rec_in_wide = jnp.swapaxes(rec_in, 0, 1)

    gates_flat = rec_gates.reshape(blocks, block, 2 * block)
    normed_one, ext_ids, gate_pre, ext, conv_low, pre, through, local, edge = rec_forward(
        spot, inputs, before, gain[0][0], rec_in_wide, segments, before_ids, rec_chan, gates_flat
    )
    entering, every_id, hidden_state, mixed, res_one, normed_a, gate_up_a, hidden_a, part = mixing(
        edge, segments, local, through, gate_pre, rec_out, inputs, gain[0][1], weights, 1
    )
    passed, normed_two, all_keys = join_keys(part, res_one, gain[1][0], attn_kv, reach, 2)

    head_dim = attn_kv.shape[1] // 2
    heads_here = attn_q.shape[1] // head_dim
    queries = dot(normed_two, attn_q, (1, 0), BF16).reshape(count, heads_here, head_dim)
    key_ids = jnp.concatenate(
        [
            pick(pick(every_id, lax.rem(place - distance + blocks_seq, blocks_seq)), core)
            for distance in range(reach, 0, -1)
        ]
        + [ids]
    )
    key_spots = (place - reach) * count + jnp.arange((reach + 1) * count, dtype=jnp.int32)
    query_spots = place * count + jnp.arange(count, dtype=jnp.int32)
    distance_q = query_spots[:, None] - key_spots[None, :]
    inside = (distance_q >= 0) & (distance_q < WINDOW) & (key_spots >= 0)[None, :]
    allowed = inside & (ids[:, None] == key_ids[None, :])
    attended, log_totals = attend(queries, all_keys, allowed)
    attended = attended.reshape(count, heads_here * head_dim)
    part = dot(attended, attn_out, (1, 0), BF16)
    (
        res_two, normed_b, hidden_b, mine_b, part_last, part_b, normed_b_other, hidden_b_other,
        mine_b_other,
    ) = last_layer(part, passed, gain[1][1], cotangent, weights, 3)

    units = hidden_b.shape[1]
    window = (units // 2 + 127) // 128 * 128

    def mlp_term(mine, theirs, normed, hidden, out_low, out_other):
        return [
            (normed, swapped(normed), mine, swapped(theirs), units),
            (out_low, out_other, hidden, swapped(hidden), window),
        ]

    terms = [
        (normed_b, normed_b_other, mine_b, mine_b_other, units),
        (cotangent, cotangent, hidden_b, hidden_b_other, window),
    ]
    part, sum_b = lax.optimization_barrier((part_b, weight_grad(core_ref, terms, False)))
    sum_b = seq_scatter(sum_b)
    grad_res_two, gain_b, low_two = join_backward(
        part, res_two, gain[1][1], cotangent, 5
    )

    grad_att = dot(low_two, attn_out, (1, 1), BF16)
    grad_query, grad_kv = attend_back(
        queries, all_keys, allowed, log_totals, grad_att.reshape(count, heads_here, head_dim)
    )
    query_low = grad_query.reshape(count, heads_here * head_dim).astype(BF16)
    part = dot(query_low, attn_q, (1, 1), BF16)
    grad_passed, gain_two, low_passed, kv_low, mine_a, theirs_a, part = join_keys_back(
        part,
        passed,
        gain[1][0],
        grad_res_two,
        grad_kv.astype(BF16).reshape(reach + 1, count, 2 * head_dim),
        attn_kv,
        gate_up_a,
        weights,
        6,
    )

    normed_two_other = swapped(normed_two)
    width_q, width_kv = query_low.shape[1], kv_low.shape[1]
    attn_terms = [
        (normed_two, normed_two_other, query_low, swapped(query_low), width_q),
        (normed_two, normed_two_other, kv_low, swapped(kv_low), width_kv),
        (low_two, swapped(low_two), attended, swapped(attended), width_q),
    ]
    terms = mlp_term(mine_a, theirs_a, normed_a, hidden_a, low_passed, swapped(low_passed))
    part, sum_a = lax.optimization_barrier((part, weight_grad(core_ref, terms, False)))
    sum_a = seq_scatter(sum_a)
    grad_res_one, gain_a, mix_low = join_backward(part, res_one, gain[0][1], grad_passed, 7)

    grad_mixed = dot(mix_low, rec_out, (1, 1))
    grad_branch, beyond, local_grad, edge = rec_back_first(
        grad_mixed, gate_pre, hidden_state, pre, rec_chan, ext_ids, block
    )
    arriving = carry_back(edge, 9)
    gate_mine, gate_theirs, grad_values, over_edge, chan_grad = rec_back_second(
        core_ref, beyond, local_grad, arriving, hidden_state, entering, pre, conv_low, rec_chan,
        gates_flat, ext_ids, ext,
    )
    from_next = from_behind(over_edge[:3], "seq", -1)
    grad_values = jnp.concatenate([grad_values[:-3], grad_values[-3:] + from_next]).astype(BF16)
    part = (
        dot(grad_values, rec_in_wide[0], (1, 1)) + dot(grad_branch, rec_in_wide[1], (1, 1))
    ).astype(BF16)
    normed_one_other = swapped(normed_one)
    rec_sum = weight_grad(
        core_ref,
        [
            (normed_one, normed_one_other, grad_values, swapped(grad_values), chans),
            (normed_one, normed_one_other, grad_branch, swapped(grad_branch), chans),
            (mix_low, swapped(mix_low), mixed, swapped(mixed), chans),
        ]
        + attn_terms,
        True,
    )
    part, rec_sum = lax.optimization_barrier((part, rec_sum))
    rec_sum = seq_scatter(rec_sum)
    _, gain_one, grad_inputs = join_backward(part, inputs, gain[0][0], grad_res_one, 8)

    def gate_grad(left, right):
        return jnp.einsum(
            "tnb,tnc->bnc",
            left.reshape(count, blocks, block),
            right.reshape(count, blocks, block),
            preferred_element_type=F32,
        )

    gate_sum = gate_grad(conv_low, gate_mine) + gate_grad(swapped(conv_low), swapped(gate_theirs))
    share = block // (2 * blocks_seq)
    gate_sum = jnp.swapaxes(
        gate_sum.astype(BF16).reshape(2, blocks_seq, share, chans), 0, 1
    ).reshape(blocks_seq, 2 * share, chans)
    gain_rows = jnp.concatenate([gain_one, gain_a, gain_two, gain_b], axis=0)
    gain_total, chan_total, gate_sum = totals(gain_rows, chan_grad, gate_sum, 11)
    gate_sum = gate_sum.reshape(2, share, chans)
    share_norm = width // blocks_seq
    grad_norms = lax.dynamic_slice_in_dim(
        pick(gain_total.reshape(2, 2, width), core), place * share_norm, share_norm, axis=1
    )
    grad_chan = jnp.where(first, chan_total[:4], chan_total[4:])

    own_part = jnp.where(first, sum_a, sum_b)
    other_part = swapped(jnp.where(first, sum_b, sum_a))
    lower = jnp.where(first, own_part, other_part).astype(F32)
    upper = jnp.where(first, other_part, own_part).astype(F32)
    grad_mlp_in = jnp.stack([lower[:, :units], upper[:, :units]], axis=1)
    grad_mlp_out = jnp.concatenate(
        [lower[:, units:].T, upper[:, 2 * window :].T], axis=0
    )
    part_last, grad_mlp_in, grad_mlp_out, grad_norms = lax.optimization_barrier(
        (part_last, grad_mlp_in, grad_mlp_out, grad_norms)
    )
    _, final = join_forward("last", part_last, res_two, gain[1][1], 4)

    chans_q = attn_q.shape[1]
    rec_sum = rec_sum.astype(F32)
    attn_sum = rec_sum[:, 3 * chans :]
    grad_q = attn_sum[:, :chans_q]
    grad_kv_out = attn_sum[:, chans_q : chans_q + 2 * head_dim]
    grad_attn_out = attn_sum[:, chans_q + 2 * head_dim :].T
    grad_in = rec_sum[:, : 2 * chans].reshape(-1, 2, chans)
    grad_rec_out = rec_sum[:, 2 * chans : 3 * chans].T
    own_gate = pick(gate_sum, core)
    other_gate = swapped(pick(gate_sum, 1 - core))
    grad_gates = jnp.transpose(
        jnp.stack([jnp.where(first, own_gate, other_gate), jnp.where(first, other_gate, own_gate)])
        .astype(F32)
        .reshape(2, share, blocks, block),
        (2, 1, 0, 3),
    )
    return (
        final[None],
        grad_inputs.astype(F32)[None],
        grad_norms[None],
        grad_in,
        grad_gates,
        grad_chan,
        grad_rec_out,
        grad_q,
        grad_kv_out,
        grad_attn_out,
        grad_mlp_in[None],
        grad_mlp_out[None],
    )


def solution(mesh):
    in_specs = (
        P(None, "seq", None),
        P(None, "seq"),
        P("section", None, None),
        P(None, None, "head"),
        P("head", None, None, None),
        P(None, "head"),
        P("head", None),
        P(None, "head"),
        P(),
        P("head", None),
        P("section", None, None, "head"),
        P("section", "head", None),
        P(None, "seq", None),
    )
    out_specs = (
        P("section", "seq", None),
        P("section", "seq", None),
        P("section", None, "seq"),
        P(("section", "seq"), None, "head"),
        P("head", ("section", "seq"), None, None),
        P("section", "head"),
        P("head", ("section", "seq")),
        P(("section", "seq"), "head"),
        P(("section", "seq"), None),
        P("head", ("section", "seq")),
        P("section", "seq", None, "head"),
        P("section", "head", "seq"),
    )

    return jax.shard_map(
        on_device, mesh=mesh, in_specs=in_specs, out_specs=out_specs, check_vma=False
    )
```
